768 devices in a mesh: grp: 16 (over y, core), sub: 48 (over z, x).
Axes of the slice: x: 4, y: 8, z: 12, core: 2. Of those that a mesh axis runs over, the one named last changes fastest.
Arguments:
- fields: float32 [4, 35, 196608], P(None, None, ('grp', 'sub')), may hold values from -6 to 6
- section_store: float32 [4, 35, 196608], P(None, None, ('grp', 'sub')), may hold values from -6 to 6
- metric_terms: float32 [9, 196608], P(None, ('grp', 'sub')), may hold values from -6 to 6
- normals: float32 [4, 3, 196608], P(None, None, ('grp', 'sub')), may hold values from -3 to 3
- face_scale: float32 [4, 196608], P(None, ('grp', 'sub')), may hold values from 1 to 4
- damping: float32 [196608], P(('grp', 'sub')), may hold values from 1 to 10
- absorb_mask: int32 [196608], P(('grp', 'sub')), may hold values from 0 to 1
- refine_level: int32 [196608], P(('grp', 'sub')), may hold values from 0 to 2
- face_source: int32 [4, 196608], P(None, ('grp', 'sub')), may hold values from -1 to 2623, as said below
- orientation: int32 [4, 196608], P(None, ('grp', 'sub')), may hold values from 0 to 5, as said below
- derivative: float32 [3, 35, 35], replicated, may hold values from -1 to 1
- lift_matrix: float32 [35, 60], replicated, may hold values from -0.75 to 0.75
Outputs:
- fields_next: float32 [4, 35, 196608], P(None, None, ('grp', 'sub'))
- store_next: float32 [4, 35, 196608], P(None, None, ('grp', 'sub'))
- absorbed_energy: float32 [], replicated
The draws below stay inside these ranges and needn't reach their ends.
Inputs may be any that keep to these rules, and one draw needn't show every extreme that they name: `face_source`: the neighbour relation is symmetric: the neighbour of a face's neighbour is the face itself, every code at or above 1024 names a slot used by exactly one face of its device, and a face's neighbour on device d holds the matching slot as in the reference program. A device uses the slots of a block from rank 0 on without gaps; it never uses block s (its own sub index), nor block 48 at the first grp index or block 49 at the last. For a sub peer b with |b - s| <= 4 at most 32 ranks are used, for other peers at most 8, and across grp at most 32; in every draw some near pair uses all 32, some farther pair all 8, and some pair across grp all 32. Local neighbours lie on the same device. `orientation`: paired faces have inverse orientations: 1 and 2 swap, 0, 3, 4 and 5 stay.
All inputs are finite; a program needn't handle non-finite values.
Results may differ from the reference program's by a relative error of at most 0.0003.
Values sent between devices are 32-bit elements; how exact they have to be, the bound alone decides.
A program may use at most 32 MiB of HBM per device.

```python
import math
import jax
import jax.numpy as jnp
import numpy as np
from jax import lax

VOLUME_NODES = 35
FACE_NODES = 15
NEAR_PEERS = 4
LOCAL_ELEMENTS = 256
PEER_SLOTS = 32
ELEMENTS = 196608
N_GRP = 16
N_SUB = 48


def link_tables(key):
    devices = N_GRP * N_SUB
    per_device = LOCAL_ELEMENTS
    slot_width = PEER_SLOTS
    narrow = slot_width // 4
    block_total = N_SUB + 2
    box_size = block_total * slot_width
    face_total = 4 * per_device
    subkeys = jax.random.split(jax.random.fold_in(key, 7301), 10)
    member_ids = jnp.arange(N_SUB, dtype=jnp.int32)
    spread = jnp.abs(member_ids[:, None] - member_ids[None, :])
    near_draw = jax.random.randint(subkeys[0], (N_GRP, N_SUB, N_SUB), slot_width // 2, slot_width + 1)
    far_draw = jax.random.randint(subkeys[1], (N_GRP, N_SUB, N_SUB), 0, narrow + 1)
    upper_part = jnp.triu(jnp.where(spread[None] <= NEAR_PEERS, near_draw, far_draw), 1)
    counts = upper_part + jnp.transpose(upper_part, (0, 2, 1))
    start_at = jax.random.randint(subkeys[2], (N_GRP,), 0, N_SUB - NEAR_PEERS - 1)
    group_ids = jnp.arange(N_GRP, dtype=jnp.int32)
    counts = counts.at[group_ids, start_at, start_at + 1].set(slot_width)
    counts = counts.at[group_ids, start_at + 1, start_at].set(slot_width)
    counts = counts.at[group_ids, start_at, start_at + NEAR_PEERS + 1].set(narrow)
    counts = counts.at[group_ids, start_at + NEAR_PEERS + 1, start_at].set(narrow)
    slab_counts = jax.random.randint(subkeys[3], (N_GRP - 1, N_SUB), slot_width // 2, slot_width + 1)
    slab_group = jax.random.randint(subkeys[4], (), 0, N_GRP - 1)
    slab_member = jax.random.randint(subkeys[5], (), 0, N_SUB)
    slab_counts = slab_counts.at[slab_group, slab_member].set(slot_width)
    zero_row = jnp.zeros((1, N_SUB), jnp.int32)
    down_counts = jnp.concatenate([zero_row, slab_counts], 0).reshape(devices)
    upward = jnp.concatenate([slab_counts, zero_row], 0).reshape(devices)
    block_counts = jnp.concatenate([counts.reshape(devices, N_SUB), down_counts[:, None], upward[:, None]], 1)
    block_ends = jnp.cumsum(block_counts, 1)
    begins = block_ends - block_counts
    remote_total = block_ends[:, -1]
    leftover = face_total - remote_total
    wall_draw = jax.random.randint(subkeys[6], (devices,), 0, 1 << 20)
    wall_count = leftover % 2 + 2 * (wall_draw % (leftover // 16 + 1))
    pair_start = remote_total + wall_count
    position = jnp.arange(face_total, dtype=jnp.int32)
    block_index = jax.vmap(lambda row: jnp.searchsorted(row, position, side='right'))(block_ends).astype(jnp.int32)
    block_index = jnp.minimum(block_index, block_total - 1)
    rank = position[None, :] - jnp.take_along_axis(begins, block_index, 1)
    is_remote = position[None, :] < remote_total[:, None]
    is_pair = position[None, :] >= pair_start[:, None]
    offset_pair = position[None, :] - pair_start[:, None]
    partner_pos = jnp.clip(pair_start[:, None] + jnp.bitwise_xor(offset_pair, 1), 0, face_total - 1)
    orders = jax.vmap(lambda sub_key: jax.random.permutation(sub_key, face_total))(jax.random.split(subkeys[7], devices)).astype(jnp.int32)
    partner_face = jnp.take_along_axis(orders, partner_pos, 1)
    code_pos = jnp.where(is_remote, face_total + block_index * slot_width + rank, jnp.where(is_pair, partner_face, -1))
    inverse = jnp.array([0, 2, 1, 3, 4, 5], jnp.int32)
    own_turn = jax.random.randint(subkeys[8], (devices, face_total), 0, 6)
    pair_lead = offset_pair % 2 == 0
    local_turn = jnp.where(pair_lead, own_turn, inverse[jnp.take_along_axis(own_turn, partner_pos, 1)])
    link_turn = jax.random.randint(subkeys[9], (devices * box_size,), 0, 6)
    device = jnp.arange(devices, dtype=jnp.int32)[:, None]
    group_index = device // N_SUB
    member = device % N_SUB
    peer_dev = jnp.where(block_index < N_SUB, group_index * N_SUB + block_index, jnp.where(block_index == N_SUB, device - N_SUB, device + N_SUB))
    peer_slot = jnp.where(block_index < N_SUB, member * slot_width + rank, jnp.where(block_index == N_SUB, (N_SUB + 1) * slot_width + rank, N_SUB * slot_width + rank))
    own_slot = block_index * slot_width + rank
    mine = link_turn[jnp.clip(device * box_size + own_slot, 0, devices * box_size - 1)]
    theirs = inverse[link_turn[jnp.clip(peer_dev * box_size + peer_slot, 0, devices * box_size - 1)]]
    remote_turn = jnp.where(device < peer_dev, mine, theirs)
    turn_pos = jnp.where(is_remote, remote_turn, jnp.where(is_pair, local_turn, own_turn))
    device_rows = jnp.broadcast_to(device, (devices, face_total))
    source_faces = jnp.zeros((devices, face_total), jnp.int32).at[device_rows, orders].set(code_pos)
    turn_faces = jnp.zeros((devices, face_total), jnp.int32).at[device_rows, orders].set(turn_pos)
    source_out = jnp.transpose(source_faces.reshape(devices, 4, per_device), (1, 0, 2)).reshape(4, devices * per_device)
    turn_out = jnp.transpose(turn_faces.reshape(devices, 4, per_device), (1, 0, 2)).reshape(4, devices * per_device)
    return (source_out, turn_out)


def draw_face_source(key, part):
    return link_tables(key)[0]


def draw_orientation(key, part):
    return link_tables(key)[1]


def draw_absorb_mask(key, part):
    total_elements = LOCAL_ELEMENTS * N_GRP * N_SUB
    element = jnp.arange(total_elements, dtype=jnp.int32)
    limit = 150 + 300 * element // total_elements
    picks = jax.random.randint(jax.random.fold_in(key, 4409), (total_elements,), 0, 1000)
    return (picks < limit).astype(jnp.int32)


def plant(result, rng, least, high):
    extent = result.shape
    place = [jax.random.randint(jax.random.fold_in(rng, axis), (), 0, extent[axis]) for axis in range(len(extent))]
    result = result.at[tuple(place)].set(least)
    longest = extent.index(max(extent))
    place[longest] = (place[longest] + 1) % extent[longest]
    return result.at[tuple(place)].set(high)


def block_scale(key, dims, shards, smallest, high):
    loudness, own = 1.0, jax.random.fold_in(key, 6)
    for axis_at, parts in shards:
        heights = jnp.exp(jax.random.uniform(jax.random.fold_in(own, axis_at), (parts,), jnp.float32, smallest / len(shards), high / len(shards)))
        loudness = loudness * jnp.repeat(heights, dims[axis_at] // parts).reshape([-1 if axis == axis_at else 1 for axis in range(len(dims))])
    return loudness


def centred(key, extent, scale, reach, shards=(), kind=jnp.bfloat16):
    values = jax.random.normal(key, extent, jnp.float32) * scale
    if len(shards) > 0:
        values = block_scale(key, extent, shards, -0.22, 0.18) * values
    return jnp.clip(values, min=-reach, max=reach).astype(kind)


def setup_inputs(seed: int = 0) -> dict:
    key_list = jax.random.split(jax.random.key(seed), 13)
    fields = centred(key_list[0], (4, VOLUME_NODES, ELEMENTS), 1.0, 6.0, ((2, 768),), jnp.float32)
    section_store = centred(key_list[1], (4, VOLUME_NODES, ELEMENTS), 1.0, 6.0, ((2, 768),), jnp.float32)
    metric_terms = centred(key_list[2], (9, ELEMENTS), 1.0, 6.0, ((1, 768),), jnp.float32)
    normals = centred(key_list[3], (4, 3, ELEMENTS), 0.577, 3.0, ((2, 768),), jnp.float32)
    face_scale = jnp.clip(jnp.exp(math.log(4.0) - 1.3862944 * jax.random.uniform(key_list[4], (4, ELEMENTS), jnp.float32) ** block_scale(key_list[4], (4, ELEMENTS), ((1, 768),), -0.2, 0.2)), 1.0, 4.0)
    damping = jnp.clip(jnp.exp(math.log(10.0) - 2.3025851 * jax.random.uniform(key_list[5], (ELEMENTS,), jnp.float32) ** block_scale(key_list[5], (ELEMENTS,), ((0, 768),), -0.2, 0.2)), 1.0, 10.0)
    absorb_mask = draw_absorb_mask(jax.random.fold_in(key_list[12], 71), 0)
    refine_level = plant(jax.random.randint(key_list[7], (ELEMENTS,), 0, 3), jax.random.fold_in(key_list[7], 1), 0, 2).astype(jnp.int32)
    face_source = draw_face_source(jax.random.fold_in(key_list[12], 71), 0)
    orientation = draw_orientation(jax.random.fold_in(key_list[12], 71), 0)
    derivative = centred(key_list[10], (3, VOLUME_NODES, VOLUME_NODES), VOLUME_NODES ** -0.5, 1.0, (), jnp.float32)
    lift_matrix = centred(key_list[11], (VOLUME_NODES, 4 * FACE_NODES), (4 * FACE_NODES) ** -0.5, 0.75, (), jnp.float32)
    return dict(fields=fields, section_store=section_store, metric_terms=metric_terms, normals=normals, face_scale=face_scale, damping=damping, absorb_mask=absorb_mask, refine_level=refine_level, face_source=face_source, orientation=orientation, derivative=derivative, lift_matrix=lift_matrix)


RUNGE_CARRY = -567301805773.0 / 1357537059087.0
RUNGE_ADVANCE = 5161836677717.0 / 13612068292357.0
TIME_STEP = 0.02


def node_tables():
    volume_list = [(first_part, second_part, third_part, 4 - first_part - second_part - third_part)
                   for first_part in range(5) for second_part in range(5 - first_part)
                   for third_part in range(5 - first_part - second_part)]
    triples = [(first_part, second_part, 4 - first_part - second_part)
               for first_part in range(5) for second_part in range(5 - first_part)]
    face_index = np.zeros((4, 15), np.int32)
    for facet in range(4):
        others = [corner for corner in range(4) if corner != facet]
        for node_pos in range(15):
            corners = [0, 0, 0, 0]
            for place_pos in range(3):
                corners[others[place_pos]] = triples[node_pos][place_pos]
            face_index[facet, node_pos] = volume_list.index(tuple(corners))
    vertex_orders = [(0, 1, 2), (1, 2, 0), (2, 0, 1), (0, 2, 1), (2, 1, 0), (1, 0, 2)]
    turn_index = np.zeros((6, 15), np.int32)
    for option in range(6):
        vertex_order = vertex_orders[option]
        for node_pos in range(15):
            triple = triples[node_pos]
            turned = (triple[vertex_order[0]], triple[vertex_order[1]], triple[vertex_order[2]])
            turn_index[option, node_pos] = triples.index(turned)
    return face_index, turn_index


def turn_matrices():
    face_index, turn_index = node_tables()
    table = np.zeros((6, 15, 15), np.float32)
    for option in range(6):
        for node_pos in range(15):
            table[option, node_pos, turn_index[option, node_pos]] = 1.0
    return jnp.asarray(table, jnp.float32)


def advance(fields, section_store, metric_terms, normals, face_scale, damping, absorb_mask, refine_level,
            face_codes, orient_flat, inner_cols, outer_cols, derivative, lift_matrix):
    elements_here = fields.shape[2]
    total_faces = 4 * elements_here
    turning = turn_matrices()
    inside = inner_cols.reshape(4, FACE_NODES, total_faces)
    gathered = outer_cols.reshape(4, FACE_NODES, total_faces)
    outside = gathered
    for option in range(1, 6):
        turned = jnp.einsum("jk,ckx->cjx", turning[option], gathered, precision=lax.Precision.HIGHEST)
        outside = jnp.where(orient_flat[None, None, :] == option, turned, outside)
    normal_flat = jnp.transpose(normals, (1, 0, 2)).reshape(3, total_faces)
    on_wall = (face_codes < 0)[None, :]
    press_in = inside[0]
    veloc_in = inside[1:]
    normal_in = jnp.sum(normal_flat[:, None, :] * veloc_in, 0)
    press_out = jnp.where(on_wall, press_in, outside[0])
    veloc_out = jnp.where(on_wall[None], veloc_in - 2.0 * normal_flat[:, None, :] * normal_in[None], outside[1:])
    press_jump = press_in - press_out
    normal_jump = jnp.sum(normal_flat[:, None, :] * (veloc_in - veloc_out), 0)
    growth = jnp.exp2(refine_level.astype(jnp.float32))
    weight_face = (face_scale * growth[None, :]).reshape(total_faces)
    flux_press = 0.5 * weight_face[None, :] * (normal_jump - press_jump)
    flux_veloc = 0.5 * weight_face[None, None, :] * normal_flat[:, None, :] * (press_jump - normal_jump)[None]
    flux_all = jnp.concatenate([flux_press[None], flux_veloc], 0).reshape(4, FACE_NODES, 4, elements_here)
    lifted = jnp.einsum("nfj,cjfe->cne", lift_matrix.reshape(VOLUME_NODES, 4, FACE_NODES), flux_all,
                        precision=lax.Precision.HIGHEST)
    slopes = jnp.einsum("dnm,cme->dcne", derivative, fields, precision=lax.Precision.HIGHEST)
    metric = metric_terms.reshape(3, 3, elements_here) * growth[None, None, :]
    physical = jnp.einsum("ide,dcne->icne", metric, slopes, precision=lax.Precision.HIGHEST)
    absorb = damping * absorb_mask.astype(jnp.float32)
    diverge = physical[0, 1] + physical[1, 2] + physical[2, 3]
    volume = jnp.concatenate([-diverge[None], -physical[:, 0]], 0)
    change = volume + lifted - absorb[None, None, :] * fields
    store_next = RUNGE_CARRY * section_store + TIME_STEP * change
    fields_next = fields + RUNGE_ADVANCE * store_next
    energy = jnp.sum(absorb * jnp.sum(fields_next * fields_next, (0, 1)))
    return fields_next, store_next, energy


def reference(fields, section_store, metric_terms, normals, face_scale, damping, absorb_mask, refine_level,
              face_source, orientation, derivative, lift_matrix):
    face_index, turn_index = node_tables()
    devices = N_GRP * N_SUB
    per_device = LOCAL_ELEMENTS
    slot_width = PEER_SLOTS
    box_size = (N_SUB + 2) * slot_width
    traces = fields[:, face_index, :]
    own_cols = jnp.transpose(traces.reshape(4, 4, FACE_NODES, devices, per_device), (0, 2, 3, 1, 4))
    own_cols = own_cols.reshape(4 * FACE_NODES, 4 * ELEMENTS)
    element = jnp.arange(ELEMENTS, dtype=jnp.int32)
    device = jnp.broadcast_to((element // per_device)[None, :], (4, ELEMENTS))
    within = jnp.broadcast_to((element % per_device)[None, :], (4, ELEMENTS))
    facet = jnp.arange(4, dtype=jnp.int32)[:, None]
    column = device * (4 * per_device) + facet * per_device + within
    face_codes = face_source
    is_local = (face_codes >= 0) & (face_codes < 4 * per_device)
    is_remote = face_codes >= 4 * per_device
    local_col = device * (4 * per_device) + jnp.clip(face_codes, 0, 4 * per_device - 1)
    slot_index = jnp.where(is_remote, face_codes - 4 * per_device, 0)
    block_index = slot_index // slot_width
    rank = slot_index % slot_width
    group_index = device // N_SUB
    member = device % N_SUB
    peer_dev = jnp.where(block_index < N_SUB, group_index * N_SUB + block_index,
                         jnp.where(block_index == N_SUB, device - N_SUB, device + N_SUB))
    peer_slot = jnp.where(block_index < N_SUB, member * slot_width + rank,
                          jnp.where(block_index == N_SUB, (N_SUB + 1) * slot_width + rank, N_SUB * slot_width + rank))
    owner_place = jnp.where(is_remote, device * box_size + slot_index, devices * box_size).astype(jnp.int32)
    slot_owner = jnp.zeros((devices * box_size,), jnp.int32).at[owner_place.reshape(-1)].set(
        column.reshape(-1), mode="drop")
    remote_col = slot_owner[jnp.clip(peer_dev * box_size + peer_slot, 0, devices * box_size - 1).astype(jnp.int32)]
    partner = jnp.where(is_local, local_col, jnp.where(is_remote, remote_col, 0)).astype(jnp.int32)

    def by_device(array):
        return jnp.transpose(array.reshape(array.shape[:-1] + (devices, per_device)),
                             (array.ndim - 1,) + tuple(range(array.ndim - 1)) + (array.ndim,))

    fields_d = by_device(fields)
    store_d = by_device(section_store)
    metric_d = by_device(metric_terms)
    normals_d = by_device(normals)
    scale_d = by_device(face_scale)
    damping_d = damping.reshape(devices, per_device)
    mask_d = absorb_mask.reshape(devices, per_device)
    level_d = refine_level.reshape(devices, per_device)
    codes_d = by_device(face_source).reshape(devices, 4 * per_device)
    orient_d = by_device(orientation).reshape(devices, 4 * per_device)
    partner_d = by_device(partner).reshape(devices, 4 * per_device)
    inner_d = jnp.transpose(own_cols.reshape(4 * FACE_NODES, devices, 4 * per_device), (1, 0, 2))

    def one_device(pieces):
        (fields_p, store_p, metric_p, normals_p, scale_p, damping_p, mask_p, level_p,
         codes_p, orient_p, inner_p, partner_p) = pieces
        outer_p = jnp.take(own_cols, partner_p, axis=1)
        return advance(fields_p, store_p, metric_p, normals_p, scale_p, damping_p, mask_p, level_p,
                       codes_p, orient_p, inner_p, outer_p, derivative, lift_matrix)

    fields_out, store_out, energies = lax.map(one_device, (fields_d, store_d, metric_d, normals_d, scale_d,
                                                          damping_d, mask_d, level_d, codes_d, orient_d,
                                                          inner_d, partner_d))
    fields_next = jnp.transpose(fields_out, (1, 2, 0, 3)).reshape(4, VOLUME_NODES, ELEMENTS)
    store_next = jnp.transpose(store_out, (1, 2, 0, 3)).reshape(4, VOLUME_NODES, ELEMENTS)
    absorbed_energy = jnp.sum(energies) / (ELEMENTS * VOLUME_NODES)
    return (fields_next, store_next, absorbed_energy)
```

```python
import functools

import jax
import jax.numpy as jnp
import numpy as np
from jax import lax
from jax.experimental import pallas as pl
from jax.experimental.pallas import tpu as pltpu
from jax.sharding import PartitionSpec as P

MESH = pl.DeviceIdType.MESH
F32 = jnp.float32
BF16 = jnp.bfloat16

RUNGE_CARRY = -567301805773.0 / 1357537059087.0
RUNGE_ADVANCE = 5161836677717.0 / 13612068292357.0
TIME_STEP = 0.02

NODES = 35
ELEMS = 256
FACES = 4 * ELEMS
NEAR = 4
NEAR_ROWS = 9 * 16
RING = 4


def pick_table():
    volume = [(a, b, c, 4 - a - b - c) for a in range(5) for b in range(5 - a) for c in range(5 - a - b)]
    triples = [(a, b, 4 - a - b) for a in range(5) for b in range(5 - a)]
    orders = [(0, 1, 2), (1, 2, 0), (2, 0, 1), (0, 2, 1), (2, 1, 0), (1, 0, 2)]
    inverse = [0, 2, 1, 3, 4, 5]
    table = np.zeros((4, 6, 16, 2, 48), np.float32)
    for facet in range(4):
        others = [corner for corner in range(4) if corner != facet]
        for option in range(6):
            order = orders[inverse[option]]
            for node in range(15):
                triple = triples[node]
                turned = tuple(triple[q] for q in order)
                corners = [0, 0, 0, 0]
                for place in range(3):
                    corners[others[place]] = turned[place]
                table[facet, option, node, :, volume.index(tuple(corners))] = 1.0
    return table.reshape(4, 96, 96)


def split(value):
    high = value.astype(BF16)
    low = (value - high.astype(F32)).astype(BF16)
    return high, low


def kernel(
    ng,
    ns,
    half,
    fields,
    store,
    metric,
    normals,
    scale,
    damping,
    mask,
    level,
    source,
    orient,
    deriv,
    lift,
    picks,
    fields_out,
    store_out,
    energy_out,
    stacked,
    inner,
    turned,
    place,
    local,
    base,
    lifts,
    near_box,
    far_box,
    grp_box,
    near_in,
    far_in,
    grp_in,
    stage,
    row_own,
    row_sub,
    sum_own,
    row_grp,
    send_sem,
    recv_sem,
    grp_send,
    grp_recv,
    esend_sub,
    erecv_sub,
    esend_grp,
    erecv_grp,
):
    g = lax.axis_index("grp")
    s = lax.axis_index("sub")
    nz = ns // RING
    far_at = NEAR_ROWS
    grp_at = NEAR_ROWS + 4 * ns
    rows = grp_at + 32

    def peer_of(m):
        i = m // RING
        j = RING - 1 - m % RING
        off = nz // 2 + (1 - 2 * (i % 2)) * ((i + 1) // 2)
        z = (s // RING + off) % nz
        x = (s % RING + j) % RING
        return z * RING + x

    near_in[...] = jnp.zeros_like(near_in)
    far_in[...] = jnp.zeros_like(far_in)
    grp_in[...] = jnp.zeros_like(grp_in)

    barrier = pltpu.get_barrier_semaphore()

    def greet_sub(m, carry):
        pl.semaphore_signal(barrier, inc=1, device_id=(g, peer_of(m)), device_id_type=MESH)
        return carry

    def greet_grp(k, carry):
        pl.semaphore_signal(barrier, inc=1, device_id=((g + k) % ng, s), device_id_type=MESH)
        return carry

    lax.fori_loop(0, ns - 1, greet_sub, 0)
    lax.fori_loop(1, ng, greet_grp, 0)

    stacked[...] = jnp.zeros_like(stacked)
    for c in range(4):
        high, low = split(fields[c])
        stacked[c, 0:NODES, :] = high
        stacked[c, 48 : 48 + NODES, :] = low
    for f in range(4):
        option_of = orient[f : f + 1, :]
        at = slice(f * ELEMS, (f + 1) * ELEMS)
        for c in range(4):
            found = jnp.dot(picks[f], stacked[c], preferred_element_type=F32)
            inner[c * 16 : (c + 1) * 16, at] = found[0:16]
            chosen = found[0:16]
            for option in range(1, 6):
                chosen = jnp.where(option_of == option, found[option * 16 : (option + 1) * 16], chosen)
            high, low = split(chosen)
            turned[c * 16 : (c + 1) * 16, at] = high
            turned[64 + c * 16 : 64 + (c + 1) * 16, at] = low

    codes = jnp.concatenate([source[f : f + 1, :] for f in range(4)], axis=1)
    slot = codes - FACES
    block = slot >> 5
    rank = slot & 31
    delta = block - s
    beside = (block < ns) & (delta >= -NEAR) & (delta <= NEAR)
    apart = (block < ns) & jnp.logical_not(beside)
    row = jnp.where(
        apart,
        far_at + block * 4 + (rank & 3),
        jnp.where(beside, (delta + NEAR) * 16, grp_at + (block - ns) * 16) + (rank & 15),
    )
    row = row + half * jnp.where(apart, (rank >> 2) & 1, rank >> 4)
    row = jnp.where(codes >= FACES, row, -1)

    def build_place(i, carry):
        at = lax.broadcasted_iota(jnp.int32, (32, FACES), 0) + i * 32
        place[pl.ds(i * 32, 32), :] = jnp.where(at == row, 1.0, 0.0).astype(BF16)
        return carry

    lax.fori_loop(0, 2 * half // 32, build_place, 0)

    packed = lax.dot_general(place[...], turned[...], (((1,), (1,)), ((), ())), preferred_element_type=F32)
    left, right = packed[:half], packed[half:]
    left = left + pltpu.roll(left, 64, 1)
    right = right + pltpu.roll(right, 64, 1)
    lane = lax.broadcasted_iota(jnp.int32, (half, 128), 1)
    out = jnp.where(lane < 64, left, right)
    near_box[...] = out[:far_at].reshape(9, 16, 128)
    for b in range(ns):
        far_box[b] = out[far_at + 4 * b : far_at + 4 * b + 4]
    grp_box[...] = out[grp_at:rows].reshape(2, 16, 128)

    pl.semaphore_wait(barrier, ns - 1 + ng - 1)

    def near_copy(b):
        return pltpu.make_async_remote_copy(
            src_ref=near_box.at[b - s + NEAR],
            dst_ref=near_in.at[s - b + NEAR],
            send_sem=send_sem.at[b],
            recv_sem=recv_sem.at[s],
            device_id=(g, b),
            device_id_type=MESH,
        )

    def far_copy(b):
        return pltpu.make_async_remote_copy(
            src_ref=far_box.at[b],
            dst_ref=far_in.at[s],
            send_sem=send_sem.at[b],
            recv_sem=recv_sem.at[s],
            device_id=(g, b),
            device_id_type=MESH,
        )

    def near_arrival(b):
        return pltpu.make_async_remote_copy(
            src_ref=near_box.at[b - s + NEAR],
            dst_ref=near_in.at[b - s + NEAR],
            send_sem=send_sem.at[b],
            recv_sem=recv_sem.at[b],
            device_id=(g, b),
            device_id_type=MESH,
        )

    def far_arrival(b):
        return pltpu.make_async_remote_copy(
            src_ref=far_box.at[b],
            dst_ref=far_in.at[b],
            send_sem=send_sem.at[b],
            recv_sem=recv_sem.at[b],
            device_id=(g, b),
            device_id_type=MESH,
        )

    def is_near(b):
        return (b - s <= NEAR) & (s - b <= NEAR)

    def grp_copy(up):
        return pltpu.make_async_remote_copy(
            src_ref=grp_box.at[up],
            dst_ref=grp_in.at[1 - up],
            send_sem=grp_send.at[up],
            recv_sem=grp_recv.at[1 - up],
            device_id=(g + 2 * up - 1, s),
            device_id_type=MESH,
        )

    def send_sub(m, carry):
        b = peer_of(m)

        @pl.when(is_near(b))
        def _():
            near_copy(b).start()

        @pl.when(jnp.logical_not(is_near(b)))
        def _():
            far_copy(b).start()

        return carry

    lax.fori_loop(0, ns - 1, send_sub, 0)

    @pl.when(g < ng - 1)
    def _():
        grp_copy(1).start()

    @pl.when(g > 0)
    def _():
        grp_copy(0).start()

    growth = jnp.exp2(level[...].astype(F32))
    absorb = damping[...] * mask[...].astype(F32)

    def build_local(i, carry):
        at = lax.broadcasted_iota(jnp.int32, (32, FACES), 0) + i * 32
        local[pl.ds(i * 32, 32), :] = jnp.where(at == codes, 1.0, 0.0).astype(BF16)
        return carry

    lax.fori_loop(0, FACES // 32, build_local, 0)
    outer_own = jnp.dot(turned[...], local[...], preferred_element_type=F32)

    lifts[...] = jnp.zeros_like(lifts)
    for f in range(4):
        lifts[0:NODES, f * 16 : f * 16 + 15] = lift[:, f * 15 : (f + 1) * 15]

    slopes = [
        [jnp.dot(deriv[d], fields[c], precision=lax.Precision.HIGHEST, preferred_element_type=F32) for c in range(4)]
        for d in range(3)
    ]

    def physical(x, c):
        total = metric[3 * x : 3 * x + 1, :] * slopes[0][c]
        for y in range(1, 3):
            total = total + metric[3 * x + y : 3 * x + y + 1, :] * slopes[y][c]
        return growth * total

    volume = [-(physical(0, 1) + physical(1, 2) + physical(2, 3))]
    volume += [-physical(x, 0) for x in range(3)]
    for c in range(4):
        base[c] = RUNGE_CARRY * store[c] + TIME_STEP * (volume[c] - absorb * fields[c])

    def arrive(m, carry):
        b = peer_of(m)

        @pl.when(is_near(b))
        def _():
            near_arrival(b).wait_recv()

        @pl.when(jnp.logical_not(is_near(b)))
        def _():
            far_arrival(b).wait_recv()

        return carry

    lax.fori_loop(0, ns - 1, arrive, 0)

    def grp_arrival(down):
        return pltpu.make_async_remote_copy(
            src_ref=grp_box.at[down],
            dst_ref=grp_in.at[down],
            send_sem=grp_send.at[down],
            recv_sem=grp_recv.at[down],
            device_id=(g + 2 * down - 1, s),
            device_id_type=MESH,
        )

    @pl.when(g > 0)
    def _():
        grp_arrival(0).wait_recv()

    @pl.when(g < ng - 1)
    def _():
        grp_arrival(1).wait_recv()

    stage[0:far_at, :] = near_in[...].reshape(far_at, 128)
    for b in range(ns):
        stage[far_at + 4 * b : far_at + 4 * b + 4, :] = far_in[b]
    stage[grp_at:rows, :] = grp_in[...].reshape(32, 128)
    if half > rows:
        stage[rows:half, :] = jnp.zeros((half - rows, 128), F32)
    came = stage[...].T
    came_high, came_low = split(came)
    left = jnp.concatenate([came_high[0:64], came_low[0:64]], axis=0)
    right = jnp.concatenate([came_high[64:128], came_low[64:128]], axis=0)
    outer_all = (
        outer_own
        + jnp.dot(left, place[0:half, :], preferred_element_type=F32)
        + jnp.dot(right, place[half : 2 * half, :], preferred_element_type=F32)
    )
    outer = outer_all[0:64] + outer_all[64:128]

    flux = [[None] * 4 for _ in range(4)]
    for f in range(4):
        at = slice(f * ELEMS, (f + 1) * ELEMS)
        wall = source[f : f + 1, :] < 0
        norm = [normals[f, x : x + 1, :] for x in range(3)]
        press_in = inner[0:16, at]
        veloc_in = [inner[(1 + x) * 16 : (2 + x) * 16, at] for x in range(3)]
        along = norm[0] * veloc_in[0] + norm[1] * veloc_in[1] + norm[2] * veloc_in[2]
        press_jump = jnp.where(wall, 0.0, press_in - outer[0:16, at])
        normal_jump = jnp.zeros_like(along)
        for x in range(3):
            met = jnp.where(wall, veloc_in[x] - 2.0 * norm[x] * along, outer[(1 + x) * 16 : (2 + x) * 16, at])
            normal_jump = normal_jump + norm[x] * (veloc_in[x] - met)
        weight = 0.5 * scale[f : f + 1, :] * growth
        flux[0][f] = weight * (normal_jump - press_jump)
        for x in range(3):
            flux[1 + x][f] = -norm[x] * flux[0][f]

    energy = jnp.zeros((1, ELEMS), F32)
    for c in range(4):
        lifted = jnp.dot(
            lifts[0:40, :],
            jnp.concatenate(flux[c], axis=0),
            precision=lax.Precision.HIGHEST,
            preferred_element_type=F32,
        )
        store_next = base[c] + TIME_STEP * lifted[0:NODES]
        fields_next = fields[c] + RUNGE_ADVANCE * store_next
        store_out[c] = store_next
        fields_out[c] = fields_next
        energy = energy + jnp.sum(fields_next * fields_next, axis=0, keepdims=True)
    energy = absorb * energy
    row_own[...] = energy[:, 0:128] + energy[:, 128:256]

    def sub_row(b, at):
        return pltpu.make_async_remote_copy(
            src_ref=row_own,
            dst_ref=row_sub.at[at],
            send_sem=esend_sub.at[b],
            recv_sem=erecv_sub.at[at],
            device_id=(g, b),
            device_id_type=MESH,
        )

    def send_row(m, carry):
        sub_row(peer_of(m), s).start()
        return carry

    lax.fori_loop(0, ns - 1, send_row, 0)
    row_sub[s] = row_own[...]

    def take_row(m, carry):
        b = peer_of(m)
        sub_row(b, b).wait_recv()
        return carry

    lax.fori_loop(0, ns - 1, take_row, 0)
    sum_own[...] = jnp.sum(row_sub[...], axis=0)

    def grp_row(b, at):
        return pltpu.make_async_remote_copy(
            src_ref=sum_own,
            dst_ref=row_grp.at[at],
            send_sem=esend_grp.at[b],
            recv_sem=erecv_grp.at[at],
            device_id=(b, s),
            device_id_type=MESH,
        )

    def send_sum(k, carry):
        grp_row((g + k) % ng, g).start()
        return carry

    lax.fori_loop(1, ng, send_sum, 0)
    row_grp[g] = sum_own[...]

    def sent_sub(m, carry):
        b = peer_of(m)

        @pl.when(is_near(b))
        def _():
            near_copy(b).wait_send()

        @pl.when(jnp.logical_not(is_near(b)))
        def _():
            far_copy(b).wait_send()

        sub_row(b, s).wait_send()
        return carry

    lax.fori_loop(0, ns - 1, sent_sub, 0)

    @pl.when(g < ng - 1)
    def _():
        grp_copy(1).wait_send()

    @pl.when(g > 0)
    def _():
        grp_copy(0).wait_send()

    def take_sum(k, carry):
        b = (g + k) % ng
        grp_row(b, b).wait_recv()
        return carry

    lax.fori_loop(1, ng, take_sum, 0)
    total = jnp.sum(jnp.sum(row_grp[...], axis=0))
    energy_out[0, 0] = total * (1.0 / (ELEMS * NODES * ng * ns))

    def sent_sum(k, carry):
        grp_row((g + k) % ng, g).wait_send()
        return carry

    lax.fori_loop(1, ng, sent_sum, 0)


def solution(mesh):
    ng, ns = mesh.shape["grp"], mesh.shape["sub"]
    rows = NEAR_ROWS + 4 * ns + 32
    half = -(-rows // 128) * 128
    both = ("grp", "sub")
    vmem = pl.BlockSpec(memory_space=pltpu.VMEM)
    dma = pltpu.SemaphoreType.DMA

    call = pl.pallas_call(
        functools.partial(kernel, ng, ns, half),
        out_shape=(
            jax.ShapeDtypeStruct((4, NODES, ELEMS), F32),
            jax.ShapeDtypeStruct((4, NODES, ELEMS), F32),
            jax.ShapeDtypeStruct((1, 1), F32),
        ),
        in_specs=[vmem] * 13,
        out_specs=(vmem, vmem, pl.BlockSpec(memory_space=pltpu.SMEM)),
        scratch_shapes=[
            pltpu.VMEM((4, 96, ELEMS), BF16),
            pltpu.VMEM((64, FACES), F32),
            pltpu.VMEM((128, FACES), BF16),
            pltpu.VMEM((2 * half, FACES), BF16),
            pltpu.VMEM((FACES, FACES), BF16),
            pltpu.VMEM((4, NODES, ELEMS), F32),
            pltpu.VMEM((40, 64), F32),
            pltpu.VMEM((9, 16, 128), F32),
            pltpu.VMEM((ns, 4, 128), F32),
            pltpu.VMEM((2, 16, 128), F32),
            pltpu.VMEM((9, 16, 128), F32),
            pltpu.VMEM((ns, 4, 128), F32),
            pltpu.VMEM((2, 16, 128), F32),
            pltpu.VMEM((half, 128), F32),
            pltpu.VMEM((1, 128), F32),
            pltpu.VMEM((ns, 1, 128), F32),
            pltpu.VMEM((1, 128), F32),
            pltpu.VMEM((ng, 1, 128), F32),
            dma((ns,)),
            dma((ns,)),
            dma((2,)),
            dma((2,)),
            dma((ns,)),
            dma((ns,)),
            dma((ng,)),
            dma((ng,)),
        ],
        compiler_params=pltpu.CompilerParams(collective_id=0, has_side_effects=True),
        name="section",
    )

    def local(
        fields,
        section_store,
        metric_terms,
        normals,
        face_scale,
        damping,
        absorb_mask,
        refine_level,
        face_source,
        orientation,
        derivative,
        lift_matrix,
    ):
        fields_next, store_next, energy = call(
            fields,
            section_store,
            metric_terms,
            normals,
            face_scale,
            damping.reshape(1, ELEMS),
            absorb_mask.reshape(1, ELEMS),
            refine_level.reshape(1, ELEMS),
            face_source,
            orientation,
            derivative,
            lift_matrix,
            jnp.asarray(pick_table(), BF16),
        )
        return fields_next, store_next, energy.reshape(())

    in_specs = (
        P(None, None, both),
        P(None, None, both),
        P(None, both),
        P(None, None, both),
        P(None, both),
        P(both),
        P(both),
        P(both),
        P(None, both),
        P(None, both),
        P(),
        P(),
    )
    out_specs = (P(None, None, both), P(None, None, both), P())
    return jax.shard_map(local, mesh=mesh, in_specs=in_specs, out_specs=out_specs, check_vma=False)
```

```python
import functools

import jax
import jax.numpy as jnp
import numpy as np
from jax import lax
from jax.experimental import pallas as pl
from jax.experimental.pallas import tpu as pltpu
from jax.sharding import PartitionSpec as P

MESH = pl.DeviceIdType.MESH
F32 = jnp.float32
BF16 = jnp.bfloat16

RUNGE_CARRY = -567301805773.0 / 1357537059087.0
RUNGE_ADVANCE = 5161836677717.0 / 13612068292357.0
TIME_STEP = 0.02

NODES = 35
ELEMS = 256
FACES = 4 * ELEMS
NEAR = 4
NEAR_ROWS = 8 * 16


def pick_table():
    volume = [(a, b, c, 4 - a - b - c) for a in range(5) for b in range(5 - a) for c in range(5 - a - b)]
    triples = [(a, b, 4 - a - b) for a in range(5) for b in range(5 - a)]
    orders = [(0, 1, 2), (1, 2, 0), (2, 0, 1), (0, 2, 1), (2, 1, 0), (1, 0, 2)]
    inverse = [0, 2, 1, 3, 4, 5]
    table = np.zeros((4, 6, 16, 2, 48), np.float32)
    for facet in range(4):
        others = [corner for corner in range(4) if corner != facet]
        for option in range(6):
            order = orders[inverse[option]]
            for node in range(15):
                triple = triples[node]
                turned = tuple(triple[q] for q in order)
                corners = [0, 0, 0, 0]
                for place in range(3):
                    corners[others[place]] = turned[place]
                table[facet, option, node, :, volume.index(tuple(corners))] = 1.0
    return table.reshape(4, 96, 96)


def split(value):
    high = value.astype(BF16)
    low = (value - high.astype(F32)).astype(BF16)
    return high, low


def kernel(
    ng,
    ns,
    half,
    fields_hbm,
    store_hbm,
    metric_hbm,
    normals_hbm,
    scale_hbm,
    damping_hbm,
    mask_hbm,
    level_hbm,
    source_hbm,
    orient_hbm,
    deriv_hbm,
    lift_hbm,
    picks_hbm,
    fields_out,
    store_out,
    energy_out,
    fields,
    store,
    metric,
    normals,
    scale,
    damping,
    mask,
    level,
    source,
    orient,
    deriv,
    lift,
    picks,
    fields_new,
    store_new,
    stacked,
    inner,
    turned,
    place,
    local,
    base,
    lifts,
    near_box,
    far_box,
    grp_box,
    near_in,
    far_in,
    grp_in,
    stage,
    row_own,
    row_sub,
    sum_own,
    row_grp,
    load_sem,
    out_sem,
    near_sems,
    far_sems,
    grp_send,
    grp_recv,
    sub_sems,
    top_sems,
):
    g = lax.axis_index("grp")
    s = lax.axis_index("sub")
    far_at = NEAR_ROWS
    grp_at = NEAR_ROWS + 4 * (ns - 9)
    rows = grp_at + 32

    def load(at, src, dst):
        return pltpu.make_async_copy(src, dst, load_sem.at[at])

    load_source = load(0, source_hbm, source)
    load_orient = load(1, orient_hbm, orient)
    load_fields = [load(2 + c, fields_hbm.at[:, c, :], fields.at[c]) for c in range(4)]
    load_picks = load(6, picks_hbm, picks)
    load_store = [load(7 + c, store_hbm.at[:, c, :], store.at[c]) for c in range(4)]
    load_rest = [
        load(11, metric_hbm, metric),
        load(12, normals_hbm, normals),
        load(13, scale_hbm, scale),
        load(14, damping_hbm, damping),
        load(15, mask_hbm, mask),
        load(16, level_hbm, level),
        load(17, deriv_hbm, deriv),
        load(18, lift_hbm, lift),
    ]
    for copy in [load_source, load_orient, *load_fields, load_picks, *load_rest, *load_store]:
        copy.start()

    def peer(k):
        return lax.rem(s + k, ns)

    near_in[...] = jnp.zeros_like(near_in)
    far_in[...] = jnp.zeros_like(far_in)
    grp_in[...] = jnp.zeros_like(grp_in)

    order = sorted(range(1, ns), key=lambda k: -min(k, ns - k))

    barrier = pltpu.get_barrier_semaphore()
    for k in order:
        pl.semaphore_signal(barrier, inc=1, device_id=(g, peer(k)), device_id_type=MESH)
    for k in range(1, ng):
        pl.semaphore_signal(barrier, inc=1, device_id=(lax.rem(g + k, ng), s), device_id_type=MESH)

    load_source.wait()
    codes = jnp.concatenate([source[f : f + 1, :] for f in range(4)], axis=1)
    slot = codes - FACES
    block = slot >> 5
    rank = slot & 31
    delta = block - s
    delta = jnp.where(delta < 0, delta + ns, delta)
    in_sub = block < ns
    after = in_sub & (delta <= NEAR)
    before = in_sub & (delta >= ns - NEAR)
    apart = in_sub & (delta > NEAR) & (delta < ns - NEAR)
    box = jnp.where(after, (delta - 1) * 16, jnp.where(before, (delta - ns + 8) * 16, grp_at + (block - ns) * 16))
    row = jnp.where(apart, far_at + (delta - NEAR - 1) * 4 + (rank & 3), box + (rank & 15))
    row = row + half * jnp.where(apart, (rank >> 2) & 1, rank >> 4)
    row = jnp.where(codes >= FACES, row, -1)

    def build_place(i, carry):
        at = lax.broadcasted_iota(jnp.int32, (32, FACES), 0) + i * 32
        place[pl.ds(i * 32, 32), :] = jnp.where(at == row, 1.0, 0.0).astype(BF16)
        return carry

    lax.fori_loop(0, 2 * half // 32, build_place, 0)

    stacked[...] = jnp.zeros_like(stacked)
    load_orient.wait()
    load_picks.wait()
    for c in range(4):
        load_fields[c].wait()
        high, low = split(fields[c])
        stacked[c, 0:NODES, :] = high
        stacked[c, 48 : 48 + NODES, :] = low
    for f in range(4):
        option_of = orient[f : f + 1, :]
        at = slice(f * ELEMS, (f + 1) * ELEMS)
        for c in range(4):
            found = jnp.dot(picks[f], stacked[c], preferred_element_type=F32)
            inner[c * 16 : (c + 1) * 16, at] = found[0:16]
            chosen = found[0:16]
            for option in range(1, 6):
                chosen = jnp.where(option_of == option, found[option * 16 : (option + 1) * 16], chosen)
            high, low = split(chosen)
            turned[c * 16 : (c + 1) * 16, at] = high
            turned[64 + c * 16 : 64 + (c + 1) * 16, at] = low

    packed = lax.dot_general(place[...], turned[...], (((1,), (1,)), ((), ())), preferred_element_type=F32)
    left, right = packed[:half], packed[half:]
    left = left + pltpu.roll(left, 64, 1)
    right = right + pltpu.roll(right, 64, 1)
    lane = lax.broadcasted_iota(jnp.int32, (half, 128), 1)
    out = jnp.where(lane < 64, left, right)
    near_box[...] = out[:far_at].reshape(8, 16, 128)
    for b in range(ns - 9):
        far_box[b] = out[far_at + 4 * b : far_at + 4 * b + 4]
    grp_box[...] = out[grp_at:rows].reshape(2, 16, 128)

    pl.semaphore_wait(barrier, ns - 1 + ng - 1)

    def near_at(k):
        return k - 1 if k <= NEAR else k - ns + 8

    def sub_copy(k):
        if NEAR < k < ns - NEAR:
            src, dst, sems = far_box.at[k - NEAR - 1], far_in.at[ns - k - NEAR - 1], far_sems
        else:
            src, dst, sems = near_box.at[near_at(k)], near_in.at[near_at(ns - k)], near_sems
        return pltpu.make_async_remote_copy(
            src_ref=src,
            dst_ref=dst,
            send_sem=sems.at[0],
            recv_sem=sems.at[1],
            device_id=(g, peer(k)),
            device_id_type=MESH,
        )

    def grp_copy(up):
        return pltpu.make_async_remote_copy(
            src_ref=grp_box.at[up],
            dst_ref=grp_in.at[1 - up],
            send_sem=grp_send.at[up],
            recv_sem=grp_recv.at[1 - up],
            device_id=(g + 2 * up - 1, s),
            device_id_type=MESH,
        )

    for k in order:
        sub_copy(k).start()

    @pl.when(g < ng - 1)
    def _():
        grp_copy(1).start()

    @pl.when(g > 0)
    def _():
        grp_copy(0).start()

    for copy in [*load_rest, *load_store]:
        copy.wait()
    growth = jnp.exp2(level[...].astype(F32))
    absorb = damping[...] * mask[...].astype(F32)

    def build_local(i, carry):
        at = lax.broadcasted_iota(jnp.int32, (32, FACES), 0) + i * 32
        local[pl.ds(i * 32, 32), :] = jnp.where(at == codes, 1.0, 0.0).astype(BF16)
        return carry

    lax.fori_loop(0, FACES // 32, build_local, 0)
    outer_own = jnp.dot(turned[...], local[...], preferred_element_type=F32)

    lifts[...] = jnp.zeros_like(lifts)
    for f in range(4):
        lifts[0:NODES, f * 16 : f * 16 + 15] = lift[:, f * 15 : (f + 1) * 15]
    lift_high, lift_low = split(lifts[...])
    lift_cat = jnp.concatenate([lift_high, lift_high, lift_low], axis=1)

    slopes = [
        [jnp.dot(deriv[d], fields[c], precision=lax.Precision.HIGHEST, preferred_element_type=F32) for c in range(4)]
        for d in range(3)
    ]

    def physical(x, c):
        total = metric[3 * x : 3 * x + 1, :] * slopes[0][c]
        for y in range(1, 3):
            total = total + metric[3 * x + y : 3 * x + y + 1, :] * slopes[y][c]
        return growth * total

    volume = [-(physical(0, 1) + physical(1, 2) + physical(2, 3))]
    volume += [-physical(x, 0) for x in range(3)]
    for c in range(4):
        base[c] = RUNGE_CARRY * store[c] + TIME_STEP * (volume[c] - absorb * fields[c])

    def arrival(ref, sems):
        return pltpu.make_async_copy(ref, ref, sems.at[1])

    arrival(near_in, near_sems).wait()
    arrival(far_in, far_sems).wait()

    @pl.when(g > 0)
    def _():
        pltpu.make_async_copy(grp_in.at[0], grp_in.at[0], grp_recv.at[0]).wait()

    @pl.when(g < ng - 1)
    def _():
        pltpu.make_async_copy(grp_in.at[1], grp_in.at[1], grp_recv.at[1]).wait()

    stage[0:far_at, :] = near_in[...].reshape(far_at, 128)
    for b in range(ns - 9):
        stage[far_at + 4 * b : far_at + 4 * b + 4, :] = far_in[b]
    stage[grp_at:rows, :] = grp_in[...].reshape(32, 128)
    if stage.shape[0] > rows:
        stage[rows:, :] = jnp.zeros((stage.shape[0] - rows, 128), F32)
    came = stage[...].T
    came_high, came_low = split(came)
    left = jnp.concatenate([came_high[0:64], came_low[0:64]], axis=0)[:, :half]
    right = jnp.concatenate([came_high[64:128], came_low[64:128]], axis=0)[:, :half]
    outer_all = (
        outer_own
        + jnp.dot(left, place[0:half, :], preferred_element_type=F32)
        + jnp.dot(right, place[half : 2 * half, :], preferred_element_type=F32)
    )
    outer = outer_all[0:64] + outer_all[64:128]

    flux = [[None] * 4 for _ in range(4)]
    for f in range(4):
        at = slice(f * ELEMS, (f + 1) * ELEMS)
        wall = source[f : f + 1, :] < 0
        norm = [normals[x, f : f + 1, :] for x in range(3)]
        press_in = inner[0:16, at]
        veloc_in = [inner[(1 + x) * 16 : (2 + x) * 16, at] for x in range(3)]
        along = norm[0] * veloc_in[0] + norm[1] * veloc_in[1] + norm[2] * veloc_in[2]
        press_jump = jnp.where(wall, 0.0, press_in - outer[0:16, at])
        normal_jump = jnp.zeros_like(along)
        for x in range(3):
            met = jnp.where(wall, veloc_in[x] - 2.0 * norm[x] * along, outer[(1 + x) * 16 : (2 + x) * 16, at])
            normal_jump = normal_jump + norm[x] * (veloc_in[x] - met)
        weight = 0.5 * scale[f : f + 1, :] * growth
        flux[0][f] = weight * (normal_jump - press_jump)
        for x in range(3):
            flux[1 + x][f] = -norm[x] * flux[0][f]

    energy = jnp.zeros((1, ELEMS), F32)
    for c in range(4):
        high, low = split(jnp.concatenate(flux[c], axis=0))
        lifted = jnp.dot(lift_cat, jnp.concatenate([high, low, high], axis=0), preferred_element_type=F32)
        store_next = base[c] + TIME_STEP * lifted[0:NODES]
        fields_next = fields[c] + RUNGE_ADVANCE * store_next
        store_new[c] = store_next
        fields_new[c] = fields_next
        energy = energy + jnp.sum(fields_next * fields_next, axis=0, keepdims=True)
    energy = absorb * energy
    row_own[...] = energy[:, 0:128] + energy[:, 128:256]

    def sub_row(k):
        return pltpu.make_async_remote_copy(
            src_ref=row_own,
            dst_ref=row_sub.at[s],
            send_sem=sub_sems.at[0],
            recv_sem=sub_sems.at[1],
            device_id=(g, peer(k)),
            device_id_type=MESH,
        )

    for k in order:
        sub_row(k).start()
    row_sub[s] = row_own[...]

    outs = [pltpu.make_async_copy(fields_new.at[c], fields_out.at[:, c, :], out_sem.at[c]) for c in range(4)]
    outs += [pltpu.make_async_copy(store_new.at[c], store_out.at[:, c, :], out_sem.at[4 + c]) for c in range(4)]
    for copy in outs:
        copy.start()

    many = row_sub.at[0 : ns - 1]
    arrival(many, sub_sems).wait()
    sum_own[...] = jnp.sum(row_sub[...], axis=0)

    def top_row(k):
        return pltpu.make_async_remote_copy(
            src_ref=sum_own,
            dst_ref=row_grp.at[g],
            send_sem=top_sems.at[0],
            recv_sem=top_sems.at[1],
            device_id=(lax.rem(g + k, ng), s),
            device_id_type=MESH,
        )

    for k in sorted(range(1, ng), key=lambda k: -min(k, ng - k)):
        top_row(k).start()
    row_grp[g] = sum_own[...]

    def left_here(ref, sem):
        pltpu.make_async_copy(ref, ref, sem).wait()

    left_here(near_box, near_sems.at[0])
    left_here(far_box, far_sems.at[0])
    left_here(many, sub_sems.at[0])

    @pl.when(g < ng - 1)
    def _():
        grp_copy(1).wait_send()

    @pl.when(g > 0)
    def _():
        grp_copy(0).wait_send()

    for copy in outs:
        copy.wait()

    few = row_grp.at[0 : ng - 1]
    arrival(few, top_sems).wait()
    total = jnp.sum(jnp.sum(row_grp[...], axis=0))
    energy_out[0, 0] = total * (1.0 / (ELEMS * NODES * ng * ns))
    left_here(few, top_sems.at[0])


def solution(mesh):
    ng, ns = mesh.shape["grp"], mesh.shape["sub"]
    rows = NEAR_ROWS + 4 * (ns - 9) + 32
    half = -(-rows // 32) * 32
    both = ("grp", "sub")
    hbm = pl.BlockSpec(memory_space=pl.ANY)
    dma = pltpu.SemaphoreType.DMA
    volume = (4, NODES, ELEMS)
    state = jax.ShapeDtypeStruct((NODES, 4, ELEMS), F32)

    call = pl.pallas_call(
        functools.partial(kernel, ng, ns, half),
        out_shape=(state, state, jax.ShapeDtypeStruct((1, 1), F32)),
        in_specs=[hbm] * 13,
        out_specs=(hbm, hbm, pl.BlockSpec(memory_space=pltpu.SMEM)),
        scratch_shapes=[
            pltpu.VMEM(volume, F32),
            pltpu.VMEM(volume, F32),
            pltpu.VMEM((9, ELEMS), F32),
            pltpu.VMEM((3, 4, ELEMS), F32),
            pltpu.VMEM((4, ELEMS), F32),
            pltpu.VMEM((1, ELEMS), F32),
            pltpu.VMEM((1, ELEMS), jnp.int32),
            pltpu.VMEM((1, ELEMS), jnp.int32),
            pltpu.VMEM((4, ELEMS), jnp.int32),
            pltpu.VMEM((4, ELEMS), jnp.int32),
            pltpu.VMEM((3, NODES, NODES), F32),
            pltpu.VMEM((NODES, 60), F32),
            pltpu.VMEM((4, 96, 96), BF16),
            pltpu.VMEM(volume, F32),
            pltpu.VMEM(volume, F32),
            pltpu.VMEM((4, 96, ELEMS), BF16),
            pltpu.VMEM((64, FACES), F32),
            pltpu.VMEM((128, FACES), BF16),
            pltpu.VMEM((2 * half, FACES), BF16),
            pltpu.VMEM((FACES, FACES), BF16),
            pltpu.VMEM(volume, F32),
            pltpu.VMEM((48, 64), F32),
            pltpu.VMEM((8, 16, 128), F32),
            pltpu.VMEM((ns - 9, 4, 128), F32),
            pltpu.VMEM((2, 16, 128), F32),
            pltpu.VMEM((8, 16, 128), F32),
            pltpu.VMEM((ns - 9, 4, 128), F32),
            pltpu.VMEM((2, 16, 128), F32),
            pltpu.VMEM((-(-half // 128) * 128, 128), F32),
            pltpu.VMEM((1, 128), F32),
            pltpu.VMEM((ns, 1, 128), F32),
            pltpu.VMEM((1, 128), F32),
            pltpu.VMEM((ng, 1, 128), F32),
            dma((19,)),
            dma((8,)),
            dma((2,)),
            dma((2,)),
            dma((2,)),
            dma((2,)),
            dma((2,)),
            dma((2,)),
        ],
        compiler_params=pltpu.CompilerParams(collective_id=0, has_side_effects=True),
        name="section",
    )

    def local(
        fields,
        section_store,
        metric_terms,
        normals,
        face_scale,
        damping,
        absorb_mask,
        refine_level,
        face_source,
        orientation,
        derivative,
        lift_matrix,
    ):
        fields_next, store_next, energy = call(
            jnp.transpose(fields, (1, 0, 2)),
            jnp.transpose(section_store, (1, 0, 2)),
            metric_terms,
            jnp.transpose(normals, (1, 0, 2)),
            face_scale,
            damping.reshape(1, ELEMS),
            absorb_mask.reshape(1, ELEMS),
            refine_level.reshape(1, ELEMS),
            face_source,
            orientation,
            derivative,
            lift_matrix,
            jnp.asarray(pick_table(), BF16),
        )
        return (
            jnp.transpose(fields_next, (1, 0, 2)),
            jnp.transpose(store_next, (1, 0, 2)),
            energy.reshape(()),
        )

    in_specs = (
        P(None, None, both),
        P(None, None, both),
        P(None, both),
        P(None, None, both),
        P(None, both),
        P(both),
        P(both),
        P(both),
        P(None, both),
        P(None, both),
        P(),
        P(),
    )
    out_specs = (P(None, None, both), P(None, None, both), P())
    return jax.shard_map(local, mesh=mesh, in_specs=in_specs, out_specs=out_specs, check_vma=False)
```

```python
import functools

import jax
import jax.numpy as jnp
import numpy as np
from jax import lax
from jax.experimental import pallas as pl
from jax.experimental.pallas import tpu as pltpu
from jax.sharding import PartitionSpec as P

MESH = pl.DeviceIdType.MESH
F32 = jnp.float32
BF16 = jnp.bfloat16

RUNGE_CARRY = -567301805773.0 / 1357537059087.0
RUNGE_ADVANCE = 5161836677717.0 / 13612068292357.0
TIME_STEP = 0.02

NODES = 35
ELEMS = 256
FACES = 4 * ELEMS
NEAR = 4
NEAR_ROWS = 8 * 16


def pick_table():
    volume = [(a, b, c, 4 - a - b - c) for a in range(5) for b in range(5 - a) for c in range(5 - a - b)]
    triples = [(a, b, 4 - a - b) for a in range(5) for b in range(5 - a)]
    orders = [(0, 1, 2), (1, 2, 0), (2, 0, 1), (0, 2, 1), (2, 1, 0), (1, 0, 2)]
    inverse = [0, 2, 1, 3, 4, 5]
    table = np.zeros((4, 6, 16, 2, 48), np.float32)
    for facet in range(4):
        others = [corner for corner in range(4) if corner != facet]
        for option in range(6):
            order = orders[inverse[option]]
            for node in range(15):
                triple = triples[node]
                turned = tuple(triple[q] for q in order)
                corners = [0, 0, 0, 0]
                for place in range(3):
                    corners[others[place]] = turned[place]
                table[facet, option, node, :, volume.index(tuple(corners))] = 1.0
    return table.reshape(4, 96, 96)


def split(value):
    high = value.astype(BF16)
    low = (value - high.astype(F32)).astype(BF16)
    return high, low


def kernel(
    ng,
    ns,
    half,
    fields_hbm,
    store_hbm,
    metric_hbm,
    normals_hbm,
    scale_hbm,
    damping_hbm,
    mask_hbm,
    level_hbm,
    source_hbm,
    orient_hbm,
    deriv_hbm,
    lift_hbm,
    picks_hbm,
    fields_new,
    store_new,
    energy_row,
    fields,
    store,
    metric,
    normals,
    scale,
    damping,
    mask,
    level,
    source,
    orient,
    deriv,
    lift,
    picks,
    stacked,
    inner,
    turned,
    place,
    local,
    base,
    lifts,
    near_box,
    far_box,
    grp_box,
    near_in,
    far_in,
    grp_in,
    near_stage,
    far_stage,
    row_own,
    row_sub,
    sum_own,
    row_grp,
    load_sem,
    near_sems,
    far_sems,
    grp_send,
    grp_recv,
    sub_sems,
    top_sems,
):
    g = lax.axis_index("grp")
    s = lax.axis_index("sub")
    grp_at = NEAR_ROWS
    far_at = NEAR_ROWS + 32
    rows = far_at + 4 * (ns - 9)

    def load(at, src, dst):
        return pltpu.make_async_copy(src, dst, load_sem.at[at])

    load_source = load(0, source_hbm, source)
    load_orient = load(1, orient_hbm, orient)
    load_fields = [load(2 + c, fields_hbm.at[:, c, :], fields.at[c]) for c in range(4)]
    load_picks = load(6, picks_hbm, picks)
    load_store = [load(7 + c, store_hbm.at[:, c, :], store.at[c]) for c in range(4)]
    load_rest = [
        load(11, metric_hbm, metric),
        load(12, normals_hbm, normals),
        load(13, scale_hbm, scale),
        load(14, damping_hbm, damping),
        load(15, mask_hbm, mask),
        load(16, level_hbm, level),
        load(17, deriv_hbm, deriv),
        load(18, lift_hbm, lift),
    ]
    for copy in [load_source, load_orient, *load_fields, load_picks, *load_rest, *load_store]:
        copy.start()

    def peer(k):
        other = s + k
        return jnp.where(other >= ns, other - ns, other)

    def peer_grp(k):
        other = g + k
        return jnp.where(other >= ng, other - ng, other)

    near_in[...] = jnp.zeros_like(near_in)
    far_in[...] = jnp.zeros_like(far_in)
    grp_in[...] = jnp.zeros_like(grp_in)

    order = sorted(range(1, ns), key=lambda k: -min(k, ns - k))

    barrier = pltpu.get_barrier_semaphore()
    for k in order:
        pl.semaphore_signal(barrier, inc=1, device_id=(g, peer(k)), device_id_type=MESH)
    for k in range(1, ng):
        pl.semaphore_signal(barrier, inc=1, device_id=(peer_grp(k), s), device_id_type=MESH)

    load_source.wait()
    codes = jnp.concatenate([source[f : f + 1, :] for f in range(4)], axis=1)
    slot = codes - FACES
    block = slot >> 5
    rank = slot & 31
    delta = block - s
    delta = jnp.where(delta < 0, delta + ns, delta)
    in_sub = block < ns
    after = in_sub & (delta <= NEAR)
    before = in_sub & (delta >= ns - NEAR)
    apart = in_sub & (delta > NEAR) & (delta < ns - NEAR)
    box = jnp.where(after, (delta - 1) * 16, jnp.where(before, (delta - ns + 8) * 16, grp_at + (block - ns) * 16))
    row = jnp.where(apart, far_at + (delta - NEAR - 1) * 4 + (rank & 3), box + (rank & 15))
    row = row + half * jnp.where(apart, (rank >> 2) & 1, rank >> 4)
    row = jnp.where(codes >= FACES, row, -1)

    def build_place(i, carry):
        at = lax.broadcasted_iota(jnp.int32, (32, FACES), 0) + i * 32
        place[pl.ds(i * 32, 32), :] = jnp.where(at == row, 1.0, 0.0).astype(BF16)
        return carry

    lax.fori_loop(0, 2 * half // 32, build_place, 0)

    stacked[...] = jnp.zeros_like(stacked)
    load_orient.wait()
    load_picks.wait()
    for c in range(4):
        load_fields[c].wait()
        high, low = split(fields[c])
        stacked[c, 0:NODES, :] = high
        stacked[c, 48 : 48 + NODES, :] = low
    for f in range(4):
        option_of = orient[f : f + 1, :]
        at = slice(f * ELEMS, (f + 1) * ELEMS)
        for c in range(4):
            found = jnp.dot(picks[f], stacked[c], preferred_element_type=F32)
            inner[c * 16 : (c + 1) * 16, at] = found[0:16]
            chosen = found[0:16]
            for option in range(1, 6):
                chosen = jnp.where(option_of == option, found[option * 16 : (option + 1) * 16], chosen)
            high, low = split(chosen)
            turned[c * 16 : (c + 1) * 16, at] = high
            turned[64 + c * 16 : 64 + (c + 1) * 16, at] = low

    packed = lax.dot_general(place[...], turned[...], (((1,), (1,)), ((), ())), preferred_element_type=F32)
    left, right = packed[:half], packed[half:]
    left = left + pltpu.roll(left, 64, 1)
    right = right + pltpu.roll(right, 64, 1)
    lane = lax.broadcasted_iota(jnp.int32, (half, 128), 1)
    out = jnp.where(lane < 64, left, right)
    near_box[...] = out[:grp_at].reshape(8, 16, 128)
    for b in range(ns - 9):
        far_box[b] = out[far_at + 4 * b : far_at + 4 * b + 4]
    grp_box[...] = out[grp_at:far_at].reshape(2, 16, 128)

    pl.semaphore_wait(barrier, ns - 1 + ng - 1)

    def near_at(k):
        return k - 1 if k <= NEAR else k - ns + 8

    def sub_copy(k):
        if NEAR < k < ns - NEAR:
            src, dst, sems = far_box.at[k - NEAR - 1], far_in.at[ns - k - NEAR - 1], far_sems
        else:
            src, dst, sems = near_box.at[near_at(k)], near_in.at[near_at(ns - k)], near_sems
        return pltpu.make_async_remote_copy(
            src_ref=src,
            dst_ref=dst,
            send_sem=sems.at[0],
            recv_sem=sems.at[1],
            device_id=(g, peer(k)),
            device_id_type=MESH,
        )

    def grp_copy(up):
        return pltpu.make_async_remote_copy(
            src_ref=grp_box.at[up],
            dst_ref=grp_in.at[1 - up],
            send_sem=grp_send.at[up],
            recv_sem=grp_recv.at[1 - up],
            device_id=(g + 2 * up - 1, s),
            device_id_type=MESH,
        )

    for k in order:
        sub_copy(k).start()

    @pl.when(g < ng - 1)
    def _():
        grp_copy(1).start()

    @pl.when(g > 0)
    def _():
        grp_copy(0).start()

    for copy in [*load_rest, *load_store]:
        copy.wait()
    growth = jnp.exp2(level[...].astype(F32))
    absorb = damping[...] * mask[...].astype(F32)

    def build_local(i, carry):
        at = lax.broadcasted_iota(jnp.int32, (32, FACES), 0) + i * 32
        local[pl.ds(i * 32, 32), :] = jnp.where(at == codes, 1.0, 0.0).astype(BF16)
        return carry

    lax.fori_loop(0, FACES // 32, build_local, 0)
    outer_own = jnp.dot(turned[...], local[...], preferred_element_type=F32)

    lifts[...] = jnp.zeros_like(lifts)
    for f in range(4):
        lifts[0:NODES, f * 16 : f * 16 + 15] = lift[:, f * 15 : (f + 1) * 15]
    lift_high, lift_low = split(lifts[...])
    lift_cat = jnp.concatenate([lift_high, lift_high, lift_low], axis=1)

    slopes = [
        [jnp.dot(deriv[d], fields[c], precision=lax.Precision.HIGHEST, preferred_element_type=F32) for c in range(4)]
        for d in range(3)
    ]

    def physical(x, c):
        total = metric[3 * x : 3 * x + 1, :] * slopes[0][c]
        for y in range(1, 3):
            total = total + metric[3 * x + y : 3 * x + y + 1, :] * slopes[y][c]
        return growth * total

    volume = [-(physical(0, 1) + physical(1, 2) + physical(2, 3))]
    volume += [-physical(x, 0) for x in range(3)]
    for c in range(4):
        base[c] = RUNGE_CARRY * store[c] + TIME_STEP * (volume[c] - absorb * fields[c])

    def arrival(ref, sems):
        return pltpu.make_async_copy(ref, ref, sems.at[1])

    def picked(stage, at):
        came = stage[...].T
        high, low = split(came)
        deep = stage.shape[0]
        left = jnp.concatenate([high[0:64], low[0:64]], axis=0)
        right = jnp.concatenate([high[64:128], low[64:128]], axis=0)
        return jnp.dot(left, place[at : at + deep, :], preferred_element_type=F32) + jnp.dot(
            right, place[half + at : half + at + deep, :], preferred_element_type=F32
        )

    far_stage[...] = jnp.zeros_like(far_stage)
    arrival(near_in, near_sems).wait()

    @pl.when(g > 0)
    def _():
        pltpu.make_async_copy(grp_in.at[0], grp_in.at[0], grp_recv.at[0]).wait()

    @pl.when(g < ng - 1)
    def _():
        pltpu.make_async_copy(grp_in.at[1], grp_in.at[1], grp_recv.at[1]).wait()

    near_stage[0:grp_at, :] = near_in[...].reshape(grp_at, 128)
    near_stage[grp_at:far_at, :] = grp_in[...].reshape(32, 128)
    outer_near = outer_own + picked(near_stage, 0)

    arrival(far_in, far_sems).wait()
    for b in range(ns - 9):
        far_stage[4 * b : 4 * b + 4, :] = far_in[b]
    outer_all = outer_near + picked(far_stage, far_at)
    outer = outer_all[0:64] + outer_all[64:128]

    flux = [[None] * 4 for _ in range(4)]
    for f in range(4):
        at = slice(f * ELEMS, (f + 1) * ELEMS)
        wall = source[f : f + 1, :] < 0
        norm = [normals[x, f : f + 1, :] for x in range(3)]
        press_in = inner[0:16, at]
        veloc_in = [inner[(1 + x) * 16 : (2 + x) * 16, at] for x in range(3)]
        along = norm[0] * veloc_in[0] + norm[1] * veloc_in[1] + norm[2] * veloc_in[2]
        press_jump = jnp.where(wall, 0.0, press_in - outer[0:16, at])
        normal_jump = jnp.zeros_like(along)
        for x in range(3):
            met = jnp.where(wall, veloc_in[x] - 2.0 * norm[x] * along, outer[(1 + x) * 16 : (2 + x) * 16, at])
            normal_jump = normal_jump + norm[x] * (veloc_in[x] - met)
        weight = 0.5 * scale[f : f + 1, :] * growth
        flux[0][f] = weight * (normal_jump - press_jump)
        for x in range(3):
            flux[1 + x][f] = -norm[x] * flux[0][f]

    energy = jnp.zeros((1, ELEMS), F32)
    for c in range(4):
        high, low = split(jnp.concatenate(flux[c], axis=0))
        lifted = jnp.dot(lift_cat, jnp.concatenate([high, low, high], axis=0), preferred_element_type=F32)
        store_next = base[c] + TIME_STEP * lifted[0:NODES]
        fields_next = fields[c] + RUNGE_ADVANCE * store_next
        store_new[c] = store_next
        fields_new[c] = fields_next
        energy = energy + jnp.sum(fields_next * fields_next, axis=0, keepdims=True)
    energy = absorb * energy
    row_own[...] = energy[:, 0:128] + energy[:, 128:256]

    def sub_row(k):
        return pltpu.make_async_remote_copy(
            src_ref=row_own,
            dst_ref=row_sub.at[s],
            send_sem=sub_sems.at[0],
            recv_sem=sub_sems.at[1],
            device_id=(g, peer(k)),
            device_id_type=MESH,
        )

    for k in order:
        sub_row(k).start()
    row_sub[s] = row_own[...]

    many = row_sub.at[0 : ns - 1]
    arrival(many, sub_sems).wait()
    sum_own[...] = jnp.sum(row_sub[...], axis=0)

    def top_row(k):
        return pltpu.make_async_remote_copy(
            src_ref=sum_own,
            dst_ref=row_grp.at[g],
            send_sem=top_sems.at[0],
            recv_sem=top_sems.at[1],
            device_id=(peer_grp(k), s),
            device_id_type=MESH,
        )

    for k in sorted(range(1, ng), key=lambda k: -min(k, ng - k)):
        top_row(k).start()
    row_grp[g] = sum_own[...]

    def left_here(ref, sem):
        pltpu.make_async_copy(ref, ref, sem).wait()

    left_here(near_box, near_sems.at[0])
    left_here(far_box, far_sems.at[0])
    left_here(many, sub_sems.at[0])

    @pl.when(g < ng - 1)
    def _():
        grp_copy(1).wait_send()

    @pl.when(g > 0)
    def _():
        grp_copy(0).wait_send()

    few = row_grp.at[0 : ng - 1]
    arrival(few, top_sems).wait()
    energy_row[...] = jnp.sum(row_grp[...], axis=0)
    left_here(few, top_sems.at[0])


def finish(count, fields_new, store_new, energy_row, fields_out, store_out, energy_out, out_sem):
    outs = [pltpu.make_async_copy(fields_new.at[c], fields_out.at[:, c, :], out_sem.at[c]) for c in range(4)]
    outs += [pltpu.make_async_copy(store_new.at[c], store_out.at[:, c, :], out_sem.at[4 + c]) for c in range(4)]
    for copy in outs:
        copy.start()
    energy_out[0, 0] = jnp.sum(energy_row[...]) * (1.0 / count)
    for copy in outs:
        copy.wait()


def solution(mesh):
    ng, ns = mesh.shape["grp"], mesh.shape["sub"]
    rows = NEAR_ROWS + 4 * (ns - 9) + 32
    half = -(-rows // 16) * 16
    both = ("grp", "sub")
    hbm = pl.BlockSpec(memory_space=pltpu.HBM)
    vmem = pl.BlockSpec(memory_space=pltpu.VMEM)
    dma = pltpu.SemaphoreType.DMA
    volume = (4, NODES, ELEMS)
    state = jax.ShapeDtypeStruct((NODES, 4, ELEMS), F32)

    call = pl.pallas_call(
        functools.partial(kernel, ng, ns, half),
        out_shape=(
            jax.ShapeDtypeStruct(volume, F32),
            jax.ShapeDtypeStruct(volume, F32),
            jax.ShapeDtypeStruct((1, 128), F32),
        ),
        in_specs=[hbm] * 13,
        out_specs=(vmem, vmem, vmem),
        scratch_shapes=[
            pltpu.VMEM(volume, F32),
            pltpu.VMEM(volume, F32),
            pltpu.VMEM((9, ELEMS), F32),
            pltpu.VMEM((3, 4, ELEMS), F32),
            pltpu.VMEM((4, ELEMS), F32),
            pltpu.VMEM((1, ELEMS), F32),
            pltpu.VMEM((1, ELEMS), jnp.int32),
            pltpu.VMEM((1, ELEMS), jnp.int32),
            pltpu.VMEM((4, ELEMS), jnp.int32),
            pltpu.VMEM((4, ELEMS), jnp.int32),
            pltpu.VMEM((3, NODES, NODES), F32),
            pltpu.VMEM((NODES, 60), F32),
            pltpu.VMEM((4, 96, 96), BF16),
            pltpu.VMEM((4, 96, ELEMS), BF16),
            pltpu.VMEM((64, FACES), F32),
            pltpu.VMEM((128, FACES), BF16),
            pltpu.VMEM((2 * half, FACES), BF16),
            pltpu.VMEM((FACES, FACES), BF16),
            pltpu.VMEM(volume, F32),
            pltpu.VMEM((48, 64), F32),
            pltpu.VMEM((8, 16, 128), F32),
            pltpu.VMEM((ns - 9, 4, 128), F32),
            pltpu.VMEM((2, 16, 128), F32),
            pltpu.VMEM((8, 16, 128), F32),
            pltpu.VMEM((ns - 9, 4, 128), F32),
            pltpu.VMEM((2, 16, 128), F32),
            pltpu.VMEM((NEAR_ROWS + 32, 128), F32),
            pltpu.VMEM((half - NEAR_ROWS - 32, 128), F32),
            pltpu.VMEM((1, 128), F32),
            pltpu.VMEM((ns, 1, 128), F32),
            pltpu.VMEM((1, 128), F32),
            pltpu.VMEM((ng, 1, 128), F32),
            dma((19,)),
            dma((2,)),
            dma((2,)),
            dma((2,)),
            dma((2,)),
            dma((2,)),
            dma((2,)),
        ],
        compiler_params=pltpu.CompilerParams(collective_id=0, has_side_effects=True, vmem_limit_bytes=24 << 20),
        name="section",
    )
    write = pl.pallas_call(
        functools.partial(finish, ELEMS * NODES * ng * ns),
        out_shape=(state, state, jax.ShapeDtypeStruct((1, 1), F32)),
        in_specs=[vmem] * 3,
        out_specs=(hbm, hbm, pl.BlockSpec(memory_space=pltpu.SMEM)),
        scratch_shapes=[dma((8,))],
        compiler_params=pltpu.CompilerParams(vmem_limit_bytes=8 << 20),
        name="finish",
    )

    def keep(x):
        return pltpu.with_memory_space_constraint(x, pltpu.HBM)

    def local(
        fields,
        section_store,
        metric_terms,
        normals,
        face_scale,
        damping,
        absorb_mask,
        refine_level,
        face_source,
        orientation,
        derivative,
        lift_matrix,
    ):
        fields_new, store_new, energy_row = call(*map(keep,(
            jnp.transpose(fields, (1, 0, 2)),
            jnp.transpose(section_store, (1, 0, 2)),
            metric_terms,
            jnp.transpose(normals, (1, 0, 2)),
            face_scale,
            damping.reshape(1, ELEMS),
            absorb_mask.reshape(1, ELEMS),
            refine_level.reshape(1, ELEMS),
            face_source,
            orientation,
            derivative,
            lift_matrix,
            jnp.asarray(pick_table(), BF16),
        )))
        fields_next, store_next, energy = write(fields_new, store_new, energy_row)
        return (
            jnp.transpose(fields_next, (1, 0, 2)),
            jnp.transpose(store_next, (1, 0, 2)),
            energy.reshape(()),
        )

    in_specs = (
        P(None, None, both),
        P(None, None, both),
        P(None, both),
        P(None, None, both),
        P(None, both),
        P(both),
        P(both),
        P(both),
        P(None, both),
        P(None, both),
        P(),
        P(),
    )
    out_specs = (P(None, None, both), P(None, None, both), P())
    return jax.shard_map(local, mesh=mesh, in_specs=in_specs, out_specs=out_specs, check_vma=False)
```

```python
import functools

import jax
import jax.numpy as jnp
import numpy as np
from jax import lax
from jax.experimental import pallas as pl
from jax.experimental.pallas import tpu as pltpu
from jax.sharding import PartitionSpec as P

MESH = pl.DeviceIdType.MESH
F32 = jnp.float32
BF16 = jnp.bfloat16

RUNGE_CARRY = -567301805773.0 / 1357537059087.0
RUNGE_ADVANCE = 5161836677717.0 / 13612068292357.0
TIME_STEP = 0.02

NODES = 35
ELEMS = 256
FACES = 4 * ELEMS
RING = 4
NEAR_BOXES = 11
NEAR_ROWS = NEAR_BOXES * 16


def pick_table():
    volume = [(a, b, c, 4 - a - b - c) for a in range(5) for b in range(5 - a) for c in range(5 - a - b)]
    triples = [(a, b, 4 - a - b) for a in range(5) for b in range(5 - a)]
    orders = [(0, 1, 2), (1, 2, 0), (2, 0, 1), (0, 2, 1), (2, 1, 0), (1, 0, 2)]
    inverse = [0, 2, 1, 3, 4, 5]
    table = np.zeros((4, 6, 16, 2, 48), np.float32)
    for facet in range(4):
        others = [corner for corner in range(4) if corner != facet]
        for option in range(6):
            order = orders[inverse[option]]
            for node in range(15):
                triple = triples[node]
                turned = tuple(triple[q] for q in order)
                corners = [0, 0, 0, 0]
                for place in range(3):
                    corners[others[place]] = turned[place]
                table[facet, option, node, :, volume.index(tuple(corners))] = 1.0
    return table.reshape(4, 96, 96)


def split(value):
    high = value.astype(BF16)
    low = (value - high.astype(F32)).astype(BF16)
    return high, low


def kernel(
    ng,
    ns,
    half,
    fields_hbm,
    store_hbm,
    metric_hbm,
    normals_hbm,
    scale_hbm,
    damping_hbm,
    mask_hbm,
    level_hbm,
    source_hbm,
    orient_hbm,
    deriv_hbm,
    lift_hbm,
    picks_hbm,
    fields_new,
    store_new,
    energy_row,
    fields,
    store,
    metric,
    normals,
    scale,
    damping,
    mask,
    level,
    source,
    orient,
    deriv,
    lift,
    picks,
    stacked,
    inner,
    turned,
    place,
    local,
    base,
    lifts,
    near_box,
    far_box,
    grp_box,
    near_in,
    far_in,
    grp_in,
    relay_in,
    near_stage,
    far_stage,
    row_own,
    row_sub,
    sum_own,
    row_grp,
    load_sem,
    near_sems,
    far_sems,
    grp_send,
    grp_recv,
    sub_sems,
    top_sems,
    relay_sems,
    pass_sem,
):
    g = lax.axis_index("grp")
    s = lax.axis_index("sub")
    grp_at = NEAR_ROWS
    far_at = NEAR_ROWS + 32
    far_count = ns - 3 * RING
    nz = ns // RING
    z = s // RING
    x = s % RING

    def load(at, src, dst):
        return pltpu.make_async_copy(src, dst, load_sem.at[at])

    load_source = load(0, source_hbm, source)
    load_orient = load(1, orient_hbm, orient)
    load_fields = [load(2 + c, fields_hbm.at[:, c, :], fields.at[c]) for c in range(4)]
    load_picks = load(6, picks_hbm, picks)
    load_store = [load(7 + c, store_hbm.at[:, c, :], store.at[c]) for c in range(4)]
    load_rest = [
        load(11, metric_hbm, metric),
        load(12, normals_hbm, normals),
        load(13, scale_hbm, scale),
        load(14, damping_hbm, damping),
        load(15, mask_hbm, mask),
        load(16, level_hbm, level),
        load(17, deriv_hbm, deriv),
        load(18, lift_hbm, lift),
    ]
    for copy in [load_source, load_orient, *load_fields, load_picks]:
        copy.start()

    def wrapped(value, count):
        return jnp.where(value >= count, value - count, value)

    z_at = [wrapped(z + dz, nz) for dz in range(nz)]
    x_at = [(x + dx) % RING for dx in range(RING)]

    def peer(dz, dx):
        return z_at[dz % nz] * RING + x_at[dx % RING]

    def peer_grp(k):
        return wrapped(g + k, ng)

    def hops(dz, dx):
        return min(dz % nz, -dz % nz) + min(dx % RING, -dx % RING)

    def farthest(pairs):
        return sorted(pairs, key=lambda pair: -hops(*pair))

    everyone = farthest([(dz, dx) for dz in range(nz) for dx in range(RING) if (dz, dx) != (0, 0)])
    close = [(dz, dx) for dz, dx in everyone if min(dz, nz - dz) <= 3]

    barrier = pltpu.get_barrier_semaphore()
    greeted = [(hops(dz, dx), (g, peer(dz, dx))) for dz, dx in close]
    greeted += [(min(k, ng - k) // 2, (peer_grp(k), s)) for k in range(1, ng)]
    near_in[...] = jnp.zeros_like(near_in)
    grp_in[...] = jnp.zeros_like(grp_in)
    for _, device in sorted(greeted, key=lambda entry: -entry[0]):
        pl.semaphore_signal(barrier, inc=1, device_id=device, device_id_type=MESH)
    for copy in [*load_rest, *load_store]:
        copy.start()

    load_source.wait()
    codes = jnp.concatenate([source[f : f + 1, :] for f in range(4)], axis=1)
    slot = codes - FACES
    block = slot >> 5
    rank = slot & 31
    in_sub = block < ns
    dz = (block >> 2) - z
    dz = jnp.where(dz < 0, dz + nz, dz)
    dx = ((block & 3) - x) & 3
    apart = in_sub & (dz > 1) & (dz < nz - 1)
    box = jnp.where(dz == 0, dx - 1, jnp.where(dz == 1, 3 + dx, 7 + dx))
    box = jnp.where(in_sub, box * 16, grp_at + (block - ns) * 16)
    row = jnp.where(apart, far_at + ((dz - 2) * RING + dx) * 4 + (rank & 3), box + (rank & 15))
    row = row + half * jnp.where(apart, (rank >> 2) & 1, rank >> 4)
    row = jnp.where(codes >= FACES, row, -1)

    def build_place(i, carry):
        at = lax.broadcasted_iota(jnp.int32, (32, FACES), 0) + i * 32
        place[pl.ds(i * 32, 32), :] = jnp.where(at == row, 1.0, 0.0).astype(BF16)
        return carry

    lax.fori_loop(0, 2 * half // 32, build_place, 0)

    stacked[...] = jnp.zeros_like(stacked)
    load_orient.wait()
    load_picks.wait()
    for c in range(4):
        load_fields[c].wait()
        high, low = split(fields[c])
        stacked[c, 0:NODES, :] = high
        stacked[c, 48 : 48 + NODES, :] = low
    for f in range(4):
        option_of = orient[f : f + 1, :]
        at = slice(f * ELEMS, (f + 1) * ELEMS)
        for c in range(4):
            found = jnp.dot(picks[f], stacked[c], preferred_element_type=F32)
            inner[c * 16 : (c + 1) * 16, at] = found[0:16]
            chosen = found[0:16]
            for option in range(1, 6):
                chosen = jnp.where(option_of == option, found[option * 16 : (option + 1) * 16], chosen)
            high, low = split(chosen)
            turned[c * 16 : (c + 1) * 16, at] = high
            turned[64 + c * 16 : 64 + (c + 1) * 16, at] = low

    packed = lax.dot_general(place[...], turned[...], (((1,), (1,)), ((), ())), preferred_element_type=F32)
    left, right = packed[:half], packed[half:]
    left = left + pltpu.roll(left, 64, 1)
    right = right + pltpu.roll(right, 64, 1)
    lane = lax.broadcasted_iota(jnp.int32, (half, 128), 1)
    out = jnp.where(lane < 64, left, right)
    near_box[...] = out[:grp_at].reshape(NEAR_BOXES, 16, 128)
    for b in range(far_count):
        far_box[b] = out[far_at + 4 * b : far_at + 4 * b + 4]
    grp_box[...] = out[grp_at:far_at].reshape(2, 16, 128)

    pl.semaphore_wait(barrier, len(greeted))

    def near_at(dz, dx):
        return {0: dx % RING - 1, 1: 3 + dx % RING, nz - 1: 7 + dx % RING}[dz % nz]

    def far_slot(dz, dx):
        return (dz % nz - 2) * RING + dx % RING

    def sub_copy(dz, dx):
        if 1 < dz < nz - 1:
            src, dst, sems = far_box.at[far_slot(dz, dx)], far_in.at[far_slot(-dz, -dx)], far_sems
        else:
            src, dst, sems = near_box.at[near_at(dz, dx)], near_in.at[near_at(-dz, -dx)], near_sems
        return pltpu.make_async_remote_copy(
            src_ref=src,
            dst_ref=dst,
            send_sem=sems.at[0],
            recv_sem=sems.at[1],
            device_id=(g, peer(dz, dx)),
            device_id_type=MESH,
        )

    relays = [(3, (5, 6)), (nz - 3, (7,)), (2, (4,)), (nz - 2, (8,))]

    def relay_part(ref, legs, base):
        return ref.at[far_slot(legs[0], 0) - base : far_slot(legs[-1], 0) + RING - base]

    def relay_copy(n):
        step, legs = relays[n]
        return pltpu.make_async_remote_copy(
            src_ref=relay_part(far_box, legs, 0),
            dst_ref=relay_part(relay_in, legs, far_slot(4, 0)),
            send_sem=far_sems.at[0],
            recv_sem=relay_sems.at[n],
            device_id=(g, peer(step, 0)),
            device_id_type=MESH,
        )

    def forward_copy(step, leg, dx):
        return pltpu.make_async_remote_copy(
            src_ref=relay_in.at[far_slot(leg, dx) - far_slot(4, 0)],
            dst_ref=far_in.at[far_slot(-leg, -dx)],
            send_sem=pass_sem.at[0],
            recv_sem=far_sems.at[1],
            device_id=(g, peer(leg - step, dx)),
            device_id_type=MESH,
        )

    def grp_copy(up):
        return pltpu.make_async_remote_copy(
            src_ref=grp_box.at[up],
            dst_ref=grp_in.at[1 - up],
            send_sem=grp_send.at[up],
            recv_sem=grp_recv.at[1 - up],
            device_id=(g + 2 * up - 1, s),
            device_id_type=MESH,
        )

    for n in range(len(relays)):
        relay_copy(n).start()
    for dz, dx in close:
        sub_copy(dz, dx).start()

    @pl.when(g < ng - 1)
    def _():
        grp_copy(1).start()

    @pl.when(g > 0)
    def _():
        grp_copy(0).start()

    for copy in [*load_rest, *load_store]:
        copy.wait()
    growth = jnp.exp2(level[...].astype(F32))
    absorb = damping[...] * mask[...].astype(F32)

    def build_local(i, carry):
        at = lax.broadcasted_iota(jnp.int32, (32, FACES), 0) + i * 32
        local[pl.ds(i * 32, 32), :] = jnp.where(at == codes, 1.0, 0.0).astype(BF16)
        return carry

    lax.fori_loop(0, FACES // 32, build_local, 0)
    outer_own = jnp.dot(turned[...], local[...], preferred_element_type=F32)

    lifts[...] = jnp.zeros_like(lifts)
    for f in range(4):
        lifts[0:NODES, f * 16 : f * 16 + 15] = lift[:, f * 15 : (f + 1) * 15]
    lift_high, lift_low = split(lifts[...])
    lift_cat = jnp.concatenate([lift_high, lift_high, lift_low], axis=1)

    slopes = [
        [jnp.dot(deriv[d], fields[c], precision=lax.Precision.HIGHEST, preferred_element_type=F32) for c in range(4)]
        for d in range(3)
    ]

    def physical(x, c):
        total = metric[3 * x : 3 * x + 1, :] * slopes[0][c]
        for y in range(1, 3):
            total = total + metric[3 * x + y : 3 * x + y + 1, :] * slopes[y][c]
        return growth * total

    volume = [-(physical(0, 1) + physical(1, 2) + physical(2, 3))]
    volume += [-physical(x, 0) for x in range(3)]
    for c in range(4):
        base[c] = RUNGE_CARRY * store[c] + TIME_STEP * (volume[c] - absorb * fields[c])

    def arrival(ref, sems):
        return pltpu.make_async_copy(ref, ref, sems.at[1])

    for n, (step, legs) in enumerate(relays):
        pltpu.make_async_copy(
            relay_part(relay_in, legs, far_slot(4, 0)),
            relay_part(relay_in, legs, far_slot(4, 0)),
            relay_sems.at[n],
        ).wait()
        for dx in (2, 1, 3, 0):
            for leg in reversed(legs):
                forward_copy(step, leg, dx).start()

    def picked(stage, at):
        came = stage[...].T
        high, low = split(came)
        deep = stage.shape[0]
        left = jnp.concatenate([high[0:64], low[0:64]], axis=0)
        right = jnp.concatenate([high[64:128], low[64:128]], axis=0)
        return jnp.dot(left, place[at : at + deep, :], preferred_element_type=F32) + jnp.dot(
            right, place[half + at : half + at + deep, :], preferred_element_type=F32
        )

    arrival(near_in, near_sems).wait()

    @pl.when(g > 0)
    def _():
        pltpu.make_async_copy(grp_in.at[0], grp_in.at[0], grp_recv.at[0]).wait()

    @pl.when(g < ng - 1)
    def _():
        pltpu.make_async_copy(grp_in.at[1], grp_in.at[1], grp_recv.at[1]).wait()

    near_stage[0:grp_at, :] = near_in[...].reshape(grp_at, 128)
    near_stage[grp_at:far_at, :] = grp_in[...].reshape(32, 128)
    outer_near = outer_own + picked(near_stage, 0)

    arrival(far_in, far_sems).wait()
    for b in range(far_count):
        far_stage[4 * b : 4 * b + 4, :] = far_in[b]
    outer_all = outer_near + picked(far_stage, far_at)
    outer = outer_all[0:64] + outer_all[64:128]

    flux = [[None] * 4 for _ in range(4)]
    for f in range(4):
        at = slice(f * ELEMS, (f + 1) * ELEMS)
        wall = source[f : f + 1, :] < 0
        norm = [normals[x, f : f + 1, :] for x in range(3)]
        press_in = inner[0:16, at]
        veloc_in = [inner[(1 + x) * 16 : (2 + x) * 16, at] for x in range(3)]
        along = norm[0] * veloc_in[0] + norm[1] * veloc_in[1] + norm[2] * veloc_in[2]
        press_jump = jnp.where(wall, 0.0, press_in - outer[0:16, at])
        normal_jump = jnp.zeros_like(along)
        for x in range(3):
            met = jnp.where(wall, veloc_in[x] - 2.0 * norm[x] * along, outer[(1 + x) * 16 : (2 + x) * 16, at])
            normal_jump = normal_jump + norm[x] * (veloc_in[x] - met)
        weight = 0.5 * scale[f : f + 1, :] * growth
        flux[0][f] = weight * (normal_jump - press_jump)
        for x in range(3):
            flux[1 + x][f] = -norm[x] * flux[0][f]

    energy = jnp.zeros((1, ELEMS), F32)
    for c in range(4):
        high, low = split(jnp.concatenate(flux[c], axis=0))
        lifted = jnp.dot(lift_cat, jnp.concatenate([high, low, high], axis=0), preferred_element_type=F32)
        store_next = base[c] + TIME_STEP * lifted[0:NODES]
        fields_next = fields[c] + RUNGE_ADVANCE * store_next
        store_new[c] = store_next
        fields_new[c] = fields_next
        energy = energy + jnp.sum(fields_next * fields_next, axis=0, keepdims=True)
    energy = absorb * energy
    row_own[...] = energy[:, 0:128] + energy[:, 128:256]

    def sub_row(dz, dx):
        return pltpu.make_async_remote_copy(
            src_ref=row_own,
            dst_ref=row_sub.at[s],
            send_sem=sub_sems.at[0],
            recv_sem=sub_sems.at[1],
            device_id=(g, peer(dz, dx)),
            device_id_type=MESH,
        )

    for dz, dx in everyone:
        sub_row(dz, dx).start()
    row_sub[s] = row_own[...]

    many = row_sub.at[0 : ns - 1]
    arrival(many, sub_sems).wait()
    sum_own[...] = jnp.sum(row_sub[...], axis=0)

    def top_row(k):
        return pltpu.make_async_remote_copy(
            src_ref=sum_own,
            dst_ref=row_grp.at[g],
            send_sem=top_sems.at[0],
            recv_sem=top_sems.at[1],
            device_id=(peer_grp(k), s),
            device_id_type=MESH,
        )

    for k in sorted(range(1, ng), key=lambda k: -min(k, ng - k)):
        top_row(k).start()
    row_grp[g] = sum_own[...]

    def left_here(ref, sem):
        pltpu.make_async_copy(ref, ref, sem).wait()

    left_here(near_box, near_sems.at[0])
    left_here(far_box, far_sems.at[0])
    left_here(relay_in, pass_sem.at[0])
    left_here(many, sub_sems.at[0])

    @pl.when(g < ng - 1)
    def _():
        grp_copy(1).wait_send()

    @pl.when(g > 0)
    def _():
        grp_copy(0).wait_send()

    few = row_grp.at[0 : ng - 1]
    arrival(few, top_sems).wait()
    energy_row[...] = jnp.sum(row_grp[...], axis=0)
    left_here(few, top_sems.at[0])


def finish(count, fields_new, store_new, energy_row, fields_out, store_out, energy_out, out_sem):
    outs = [pltpu.make_async_copy(fields_new.at[c], fields_out.at[:, c, :], out_sem.at[c]) for c in range(4)]
    outs += [pltpu.make_async_copy(store_new.at[c], store_out.at[:, c, :], out_sem.at[4 + c]) for c in range(4)]
    for copy in outs:
        copy.start()
    energy_out[0, 0] = jnp.sum(energy_row[...]) * (1.0 / count)
    for copy in outs:
        copy.wait()


def solution(mesh):
    ng, ns = mesh.shape["grp"], mesh.shape["sub"]
    far_count = ns - 3 * RING
    half = NEAR_ROWS + 32 + 4 * far_count
    both = ("grp", "sub")
    hbm = pl.BlockSpec(memory_space=pltpu.HBM)
    vmem = pl.BlockSpec(memory_space=pltpu.VMEM)
    dma = pltpu.SemaphoreType.DMA
    volume = (4, NODES, ELEMS)
    state = jax.ShapeDtypeStruct((NODES, 4, ELEMS), F32)

    call = pl.pallas_call(
        functools.partial(kernel, ng, ns, half),
        out_shape=(
            jax.ShapeDtypeStruct(volume, F32),
            jax.ShapeDtypeStruct(volume, F32),
            jax.ShapeDtypeStruct((1, 128), F32),
        ),
        in_specs=[hbm] * 13,
        out_specs=(vmem, vmem, vmem),
        scratch_shapes=[
            pltpu.VMEM(volume, F32),
            pltpu.VMEM(volume, F32),
            pltpu.VMEM((9, ELEMS), F32),
            pltpu.VMEM((3, 4, ELEMS), F32),
            pltpu.VMEM((4, ELEMS), F32),
            pltpu.VMEM((1, ELEMS), F32),
            pltpu.VMEM((1, ELEMS), jnp.int32),
            pltpu.VMEM((1, ELEMS), jnp.int32),
            pltpu.VMEM((4, ELEMS), jnp.int32),
            pltpu.VMEM((4, ELEMS), jnp.int32),
            pltpu.VMEM((3, NODES, NODES), F32),
            pltpu.VMEM((NODES, 60), F32),
            pltpu.VMEM((4, 96, 96), BF16),
            pltpu.VMEM((4, 96, ELEMS), BF16),
            pltpu.VMEM((64, FACES), F32),
            pltpu.VMEM((128, FACES), BF16),
            pltpu.VMEM((2 * half, FACES), BF16),
            pltpu.VMEM((FACES, FACES), BF16),
            pltpu.VMEM(volume, F32),
            pltpu.VMEM((48, 64), F32),
            pltpu.VMEM((NEAR_BOXES, 16, 128), F32),
            pltpu.VMEM((far_count, 4, 128), F32),
            pltpu.VMEM((2, 16, 128), F32),
            pltpu.VMEM((NEAR_BOXES, 16, 128), F32),
            pltpu.VMEM((far_count, 4, 128), F32),
            pltpu.VMEM((2, 16, 128), F32),
            pltpu.VMEM((5 * RING, 4, 128), F32),
            pltpu.VMEM((NEAR_ROWS + 32, 128), F32),
            pltpu.VMEM((half - NEAR_ROWS - 32, 128), F32),
            pltpu.VMEM((1, 128), F32),
            pltpu.VMEM((ns, 1, 128), F32),
            pltpu.VMEM((1, 128), F32),
            pltpu.VMEM((ng, 1, 128), F32),
            dma((19,)),
            dma((2,)),
            dma((2,)),
            dma((2,)),
            dma((2,)),
            dma((2,)),
            dma((2,)),
            dma((4,)),
            dma((1,)),
        ],
        compiler_params=pltpu.CompilerParams(collective_id=0, has_side_effects=True, vmem_limit_bytes=24 << 20),
        name="section",
    )
    write = pl.pallas_call(
        functools.partial(finish, ELEMS * NODES * ng * ns),
        out_shape=(state, state, jax.ShapeDtypeStruct((1, 1), F32)),
        in_specs=[vmem] * 3,
        out_specs=(hbm, hbm, pl.BlockSpec(memory_space=pltpu.SMEM)),
        scratch_shapes=[dma((8,))],
        compiler_params=pltpu.CompilerParams(vmem_limit_bytes=8 << 20),
        name="finish",
    )

    def keep(x):
        return pltpu.with_memory_space_constraint(x, pltpu.HBM)

    def local(
        fields,
        section_store,
        metric_terms,
        normals,
        face_scale,
        damping,
        absorb_mask,
        refine_level,
        face_source,
        orientation,
        derivative,
        lift_matrix,
    ):
        fields_new, store_new, energy_row = call(*map(keep,(
            jnp.transpose(fields, (1, 0, 2)),
            jnp.transpose(section_store, (1, 0, 2)),
            metric_terms,
            jnp.transpose(normals, (1, 0, 2)),
            face_scale,
            damping.reshape(1, ELEMS),
            absorb_mask.reshape(1, ELEMS),
            refine_level.reshape(1, ELEMS),
            face_source,
            orientation,
            derivative,
            lift_matrix,
            jnp.asarray(pick_table(), BF16),
        )))
        fields_next, store_next, energy = write(fields_new, store_new, energy_row)
        return (
            jnp.transpose(fields_next, (1, 0, 2)),
            jnp.transpose(store_next, (1, 0, 2)),
            energy.reshape(()),
        )

    in_specs = (
        P(None, None, both),
        P(None, None, both),
        P(None, both),
        P(None, None, both),
        P(None, both),
        P(both),
        P(both),
        P(both),
        P(None, both),
        P(None, both),
        P(),
        P(),
    )
    out_specs = (P(None, None, both), P(None, None, both), P())
    return jax.shard_map(local, mesh=mesh, in_specs=in_specs, out_specs=out_specs, check_vma=False)
```

```python
import functools

import jax
import jax.numpy as jnp
import numpy as np
from jax import lax
from jax.experimental import pallas as pl
from jax.experimental.pallas import tpu as pltpu
from jax.sharding import PartitionSpec as P

MESH = pl.DeviceIdType.MESH
F32 = jnp.float32
BF16 = jnp.bfloat16

RUNGE_CARRY = -567301805773.0 / 1357537059087.0
RUNGE_ADVANCE = 5161836677717.0 / 13612068292357.0
TIME_STEP = 0.02

NODES = 35
ELEMS = 256
FACES = 4 * ELEMS
RING = 4
NEAR_BOXES = 11
NEAR_ROWS = NEAR_BOXES * 16


def pick_table():
    volume = [(a, b, c, 4 - a - b - c) for a in range(5) for b in range(5 - a) for c in range(5 - a - b)]
    triples = [(a, b, 4 - a - b) for a in range(5) for b in range(5 - a)]
    orders = [(0, 1, 2), (1, 2, 0), (2, 0, 1), (0, 2, 1), (2, 1, 0), (1, 0, 2)]
    inverse = [0, 2, 1, 3, 4, 5]
    table = np.zeros((4, 6, 16, 2, 48), np.float32)
    for facet in range(4):
        others = [corner for corner in range(4) if corner != facet]
        for option in range(6):
            order = orders[inverse[option]]
            for node in range(15):
                triple = triples[node]
                turned = tuple(triple[q] for q in order)
                corners = [0, 0, 0, 0]
                for place in range(3):
                    corners[others[place]] = turned[place]
                table[facet, option, node, :, volume.index(tuple(corners))] = 1.0
    return table.reshape(4, 96, 96)


def split(value):
    high = value.astype(BF16)
    low = (value - high.astype(F32)).astype(BF16)
    return high, low


def kernel(
    ng,
    ns,
    half,
    fields_hbm,
    store_hbm,
    metric_hbm,
    normals_hbm,
    scale_hbm,
    damping_hbm,
    mask_hbm,
    level_hbm,
    source_hbm,
    orient_hbm,
    deriv_hbm,
    lift_hbm,
    picks_hbm,
    fields_new,
    store_new,
    energy_new,
    fields,
    store,
    metric,
    normals,
    scale,
    damping,
    mask,
    level,
    source,
    orient,
    deriv,
    lift,
    picks,
    stacked,
    inner,
    turned,
    place,
    local,
    base,
    lifts,
    near_box,
    far_box,
    grp_box,
    near_in,
    far_in,
    grp_in,
    relay_in,
    near_stage,
    far_stage,
    row_own,
    row_sub,
    sum_own,
    row_grp,
    load_sem,
    near_sems,
    far_sems,
    grp_send,
    grp_recv,
    sub_sems,
    top_sems,
    relay_sems,
    pass_sems,
):
    g = lax.axis_index("grp")
    s = lax.axis_index("sub")
    grp_at = NEAR_ROWS
    far_at = NEAR_ROWS + 32
    far_count = ns - 3 * RING
    nz = ns // RING
    z = s // RING
    x = s % RING

    def load(at, src, dst):
        return pltpu.make_async_copy(src, dst, load_sem.at[at])

    load_source = load(0, source_hbm, source)
    load_orient = load(1, orient_hbm, orient)
    load_fields = [load(2 + c, fields_hbm.at[:, c, :], fields.at[c]) for c in range(4)]
    load_picks = load(6, picks_hbm, picks)
    load_store = [load(7 + c, store_hbm.at[:, c, :], store.at[c]) for c in range(4)]
    load_rest = [
        load(11, metric_hbm, metric),
        load(12, normals_hbm, normals),
        load(13, scale_hbm, scale),
        load(14, damping_hbm, damping),
        load(15, mask_hbm, mask),
        load(16, level_hbm, level),
        load(17, deriv_hbm, deriv),
        load(18, lift_hbm, lift),
    ]
    for copy in [load_source, load_orient, *load_fields, load_picks]:
        copy.start()

    def wrapped(value, count):
        return jnp.where(value >= count, value - count, value)

    z_at = [wrapped(z + dz, nz) for dz in range(nz)]
    x_at = [(x + dx) % RING for dx in range(RING)]

    def peer(dz, dx):
        return z_at[dz % nz] * RING + x_at[dx % RING]

    def peer_grp(k):
        return wrapped(g + k, ng)

    def hops(dz, dx):
        return min(dz % nz, -dz % nz) + min(dx % RING, -dx % RING)

    def farthest(pairs):
        return sorted(pairs, key=lambda pair: -hops(*pair))

    everyone = farthest([(dz, dx) for dz in range(nz) for dx in range(RING) if (dz, dx) != (0, 0)])
    close = [(dz, dx) for dz, dx in everyone if min(dz, nz - dz) <= 3]

    relays = [(2, 4, 0, nz - 5), (3, 5, 0, nz - 6), (3, 6, 0, nz - 7), (nz - 3, 7, 3, 4), (nz - 2, 8, 2, 3)]

    def relayed(n, step):
        at = z_at[step % nz]
        return (at >= relays[n][2]) & (at <= relays[n][3])

    barrier = pltpu.get_barrier_semaphore()
    greeted = [(hops(dz, dx), (g, peer(dz, dx))) for dz, dx in close]
    greeted += [(min(k, ng - k) // 2, (peer_grp(k), s)) for k in range(1, ng)]
    grp_in[...] = jnp.zeros_like(grp_in)
    for _, device in sorted(greeted, key=lambda entry: -entry[0]):
        pl.semaphore_signal(barrier, inc=1, device_id=device, device_id_type=MESH)
    expected = len(greeted)
    for n, (_, leg, _, _) in enumerate(relays):

        @pl.when(jnp.logical_not(relayed(n, -leg)))
        def _(leg=leg):
            for dx in (2, 1, 3, 0):
                pl.semaphore_signal(barrier, inc=1, device_id=(g, peer(-leg, dx)), device_id_type=MESH)

        expected = expected + jnp.where(relayed(n, 0), 0, RING)
    for copy in [*load_rest, *load_store]:
        copy.start()

    load_source.wait()
    codes = jnp.concatenate([source[f : f + 1, :] for f in range(4)], axis=1)
    slot = codes - FACES
    block = slot >> 5
    rank = slot & 31
    in_sub = block < ns
    dz = (block >> 2) - z
    dz = jnp.where(dz < 0, dz + nz, dz)
    dx = ((block & 3) - x) & 3
    apart = in_sub & (dz > 1) & (dz < nz - 1)
    box = jnp.where(dz == 0, dx - 1, jnp.where(dz == 1, 3 + dx, 7 + dx))
    box = jnp.where(in_sub, box * 16, grp_at + (block - ns) * 16)
    row = jnp.where(apart, far_at + ((dz - 2) * RING + dx) * 4 + (rank & 3), box + (rank & 15))
    row = row + half * jnp.where(apart, (rank >> 2) & 1, rank >> 4)
    row = jnp.where(codes >= FACES, row, -1)

    def build_place(i, carry):
        at = lax.broadcasted_iota(jnp.int32, (32, FACES), 0) + i * 32
        place[pl.ds(i * 32, 32), :] = jnp.where(at == row, 1.0, 0.0).astype(BF16)
        return carry

    lax.fori_loop(0, 2 * half // 32, build_place, 0)

    stacked[...] = jnp.zeros_like(stacked)
    load_orient.wait()
    load_picks.wait()
    for c in range(4):
        load_fields[c].wait()
        high, low = split(fields[c])
        stacked[c, 0:NODES, :] = high
        stacked[c, 48 : 48 + NODES, :] = low
    for f in range(4):
        option_of = orient[f : f + 1, :]
        at = slice(f * ELEMS, (f + 1) * ELEMS)
        for c in range(4):
            found = jnp.dot(picks[f], stacked[c], preferred_element_type=F32)
            inner[c * 16 : (c + 1) * 16, at] = found[0:16]
            chosen = found[0:16]
            for option in range(1, 6):
                chosen = jnp.where(option_of == option, found[option * 16 : (option + 1) * 16], chosen)
            high, low = split(chosen)
            turned[c * 16 : (c + 1) * 16, at] = high
            turned[64 + c * 16 : 64 + (c + 1) * 16, at] = low

    across = (((1,), (1,)), ((), ()))
    left = lax.dot_general(place[:half, :], turned[...], across, preferred_element_type=F32)
    right = lax.dot_general(place[half:, :], turned[...], across, preferred_element_type=F32)
    left = left + pltpu.roll(left, 64, 1)
    right = right + pltpu.roll(right, 64, 1)
    lane = lax.broadcasted_iota(jnp.int32, (half, 128), 1)
    out = jnp.where(lane < 64, left, right)
    near_box[...] = out[:grp_at].reshape(NEAR_BOXES, 16, 128)
    for b in range(far_count):
        far_box[b] = out[far_at + 4 * b : far_at + 4 * b + 4]
    grp_box[...] = out[grp_at:far_at].reshape(2, 16, 128)

    pl.semaphore_wait(barrier, expected)

    def near_at(dz, dx):
        return {0: dx % RING - 1, 1: 3 + dx % RING, nz - 1: 7 + dx % RING}[dz % nz]

    def far_slot(dz, dx):
        return (dz % nz - 2) * RING + dx % RING

    def sub_copy(dz, dx):
        if 1 < dz < nz - 1:
            src, dst, sems = far_box.at[far_slot(dz, dx)], far_in.at[far_slot(-dz, -dx)], far_sems
        else:
            src, dst, sems = near_box.at[near_at(dz, dx)], near_in.at[near_at(-dz, -dx)], near_sems
        return pltpu.make_async_remote_copy(
            src_ref=src,
            dst_ref=dst,
            send_sem=sems.at[0],
            recv_sem=sems.at[1],
            device_id=(g, peer(dz, dx)),
            device_id_type=MESH,
        )

    def relay_part(ref, leg, base):
        return ref.at[far_slot(leg, 0) - base : far_slot(leg, 0) + RING - base]

    def relay_copy(n):
        step, leg, _, _ = relays[n]
        return pltpu.make_async_remote_copy(
            src_ref=relay_part(far_box, leg, 0),
            dst_ref=relay_part(relay_in, leg, far_slot(4, 0)),
            send_sem=far_sems.at[0],
            recv_sem=relay_sems.at[n],
            device_id=(g, peer(step, 0)),
            device_id_type=MESH,
        )

    def forward_copy(n, dx):
        step, leg, _, _ = relays[n]
        return pltpu.make_async_remote_copy(
            src_ref=relay_in.at[far_slot(leg, dx) - far_slot(4, 0)],
            dst_ref=far_in.at[far_slot(-leg, -dx)],
            send_sem=pass_sems.at[n],
            recv_sem=far_sems.at[1],
            device_id=(g, peer(leg - step, dx)),
            device_id_type=MESH,
        )

    def grp_copy(up):
        return pltpu.make_async_remote_copy(
            src_ref=grp_box.at[up],
            dst_ref=grp_in.at[1 - up],
            send_sem=grp_send.at[up],
            recv_sem=grp_recv.at[1 - up],
            device_id=(g + 2 * up - 1, s),
            device_id_type=MESH,
        )

    for n, (_, leg, _, _) in enumerate(relays):

        @pl.when(relayed(n, 0))
        def _(n=n):
            relay_copy(n).start()

        @pl.when(jnp.logical_not(relayed(n, 0)))
        def _(leg=leg):
            for dx in (2, 1, 3, 0):
                sub_copy(leg, dx).start()

    for dz, dx in close:
        sub_copy(dz, dx).start()

    @pl.when(g < ng - 1)
    def _():
        grp_copy(1).start()

    @pl.when(g > 0)
    def _():
        grp_copy(0).start()

    for n, (step, leg, _, _) in enumerate(relays):

        @pl.when(relayed(n, -step))
        def _(n=n, leg=leg):
            part = relay_part(relay_in, leg, far_slot(4, 0))
            pltpu.make_async_copy(part, part, relay_sems.at[n]).wait()
            for dx in (2, 1, 3, 0):
                forward_copy(n, dx).start()

    for copy in [*load_rest, *load_store]:
        copy.wait()
    growth = jnp.exp2(level[...].astype(F32))
    absorb = damping[...] * mask[...].astype(F32)

    def build_local(i, carry):
        at = lax.broadcasted_iota(jnp.int32, (32, FACES), 0) + i * 32
        local[pl.ds(i * 32, 32), :] = jnp.where(at == codes, 1.0, 0.0).astype(BF16)
        return carry

    lax.fori_loop(0, FACES // 32, build_local, 0)
    outer_own = jnp.dot(turned[...], local[...], preferred_element_type=F32)

    lifts[...] = jnp.zeros_like(lifts)
    for f in range(4):
        lifts[0:NODES, f * 16 : f * 16 + 15] = lift[:, f * 15 : (f + 1) * 15]
    lift_high, lift_low = split(lifts[...])
    lift_cat = jnp.concatenate([lift_high, lift_high, lift_low], axis=1)

    slopes = [
        [jnp.dot(deriv[d], fields[c], precision=lax.Precision.HIGHEST, preferred_element_type=F32) for c in range(4)]
        for d in range(3)
    ]

    def physical(x, c):
        total = metric[3 * x : 3 * x + 1, :] * slopes[0][c]
        for y in range(1, 3):
            total = total + metric[3 * x + y : 3 * x + y + 1, :] * slopes[y][c]
        return growth * total

    volume = [-(physical(0, 1) + physical(1, 2) + physical(2, 3))]
    volume += [-physical(x, 0) for x in range(3)]
    for c in range(4):
        base[c] = RUNGE_CARRY * store[c] + TIME_STEP * (volume[c] - absorb * fields[c])

    def arrival(ref, sems):
        return pltpu.make_async_copy(ref, ref, sems.at[1])

    def picked(stage, at):
        came = stage[...].T
        high, low = split(came)
        deep = stage.shape[0]
        left = jnp.concatenate([high[0:64], low[0:64]], axis=0)
        right = jnp.concatenate([high[64:128], low[64:128]], axis=0)
        return jnp.dot(left, place[at : at + deep, :], preferred_element_type=F32) + jnp.dot(
            right, place[half + at : half + at + deep, :], preferred_element_type=F32
        )

    arrival(near_in, near_sems).wait()

    @pl.when(g > 0)
    def _():
        pltpu.make_async_copy(grp_in.at[0], grp_in.at[0], grp_recv.at[0]).wait()

    @pl.when(g < ng - 1)
    def _():
        pltpu.make_async_copy(grp_in.at[1], grp_in.at[1], grp_recv.at[1]).wait()

    near_stage[0:grp_at, :] = near_in[...].reshape(grp_at, 128)
    near_stage[grp_at:far_at, :] = grp_in[...].reshape(32, 128)
    outer_near = outer_own + picked(near_stage, 0)

    arrival(far_in, far_sems).wait()
    for b in range(far_count):
        far_stage[4 * b : 4 * b + 4, :] = far_in[b]
    outer_all = outer_near + picked(far_stage, far_at)
    outer = outer_all[0:64] + outer_all[64:128]

    flux = [[None] * 4 for _ in range(4)]
    for f in range(4):
        at = slice(f * ELEMS, (f + 1) * ELEMS)
        wall = source[f : f + 1, :] < 0
        norm = [normals[x, f : f + 1, :] for x in range(3)]
        press_in = inner[0:16, at]
        veloc_in = [inner[(1 + x) * 16 : (2 + x) * 16, at] for x in range(3)]
        along = norm[0] * veloc_in[0] + norm[1] * veloc_in[1] + norm[2] * veloc_in[2]
        press_jump = jnp.where(wall, 0.0, press_in - outer[0:16, at])
        normal_jump = jnp.zeros_like(along)
        for x in range(3):
            met = jnp.where(wall, veloc_in[x] - 2.0 * norm[x] * along, outer[(1 + x) * 16 : (2 + x) * 16, at])
            normal_jump = normal_jump + norm[x] * (veloc_in[x] - met)
        weight = 0.5 * scale[f : f + 1, :] * growth
        flux[0][f] = weight * (normal_jump - press_jump)
        for x in range(3):
            flux[1 + x][f] = -norm[x] * flux[0][f]

    energy = jnp.zeros((1, ELEMS), F32)
    for c in range(4):
        high, low = split(jnp.concatenate(flux[c], axis=0))
        lifted = jnp.dot(lift_cat, jnp.concatenate([high, low, high], axis=0), preferred_element_type=F32)
        store_next = base[c] + TIME_STEP * lifted[0:NODES]
        fields_next = fields[c] + RUNGE_ADVANCE * store_next
        store_new[c] = store_next
        fields_new[c] = fields_next
        energy = energy + jnp.sum(fields_next * fields_next, axis=0, keepdims=True)
    energy = absorb * energy
    row_own[...] = energy[:, 0:128] + energy[:, 128:256]

    def sub_row(dz, dx):
        return pltpu.make_async_remote_copy(
            src_ref=row_own,
            dst_ref=row_sub.at[s],
            send_sem=sub_sems.at[0],
            recv_sem=sub_sems.at[1],
            device_id=(g, peer(dz, dx)),
            device_id_type=MESH,
        )

    for dz, dx in everyone:
        sub_row(dz, dx).start()
    row_sub[s] = row_own[...]

    many = row_sub.at[0 : ns - 1]
    arrival(many, sub_sems).wait()
    sum_own[...] = jnp.sum(row_sub[...], axis=0)

    def top_row(k):
        return pltpu.make_async_remote_copy(
            src_ref=sum_own,
            dst_ref=row_grp.at[g],
            send_sem=top_sems.at[0],
            recv_sem=top_sems.at[1],
            device_id=(peer_grp(k), s),
            device_id_type=MESH,
        )

    for k in sorted(range(1, ng), key=lambda k: -min(k, ng - k)):
        top_row(k).start()
    row_grp[g] = sum_own[...]

    def left_here(ref, sem):
        pltpu.make_async_copy(ref, ref, sem).wait()

    left_here(near_box, near_sems.at[0])
    left_here(far_box, far_sems.at[0])
    for n, (step, leg, _, _) in enumerate(relays):

        @pl.when(relayed(n, -step))
        def _(n=n, leg=leg):
            left_here(relay_part(relay_in, leg, far_slot(4, 0)), pass_sems.at[n])

    left_here(many, sub_sems.at[0])

    @pl.when(g < ng - 1)
    def _():
        grp_copy(1).wait_send()

    @pl.when(g > 0)
    def _():
        grp_copy(0).wait_send()

    few = row_grp.at[0 : ng - 1]
    arrival(few, top_sems).wait()
    total = jnp.sum(jnp.sum(row_grp[...], axis=0), axis=1, keepdims=True)
    energy_new[...] = jnp.broadcast_to(total * (1.0 / (ELEMS * NODES * ng * ns)), (1, 128))
    left_here(few, top_sems.at[0])


def finish(fields_new, store_new, energy_new, fields_out, store_out, energy_out, single, out_sem):
    single[...] = energy_new[:, 0:1]
    outs = [pltpu.make_async_copy(fields_new.at[c], fields_out.at[:, c, :], out_sem.at[c]) for c in range(4)]
    outs += [pltpu.make_async_copy(store_new.at[c], store_out.at[:, c, :], out_sem.at[4 + c]) for c in range(4)]
    outs += [pltpu.make_async_copy(single, energy_out, out_sem.at[8])]
    for copy in outs:
        copy.start()
    for copy in outs:
        copy.wait()


def solution(mesh):
    ng, ns = mesh.shape["grp"], mesh.shape["sub"]
    far_count = ns - 3 * RING
    half = NEAR_ROWS + 32 + 4 * far_count
    both = ("grp", "sub")
    hbm = pl.BlockSpec(memory_space=pltpu.HBM)
    vmem = pl.BlockSpec(memory_space=pltpu.VMEM)
    dma = pltpu.SemaphoreType.DMA
    volume = (4, NODES, ELEMS)
    state = jax.ShapeDtypeStruct((NODES, 4, ELEMS), F32)

    call = pl.pallas_call(
        functools.partial(kernel, ng, ns, half),
        out_shape=(
            jax.ShapeDtypeStruct(volume, F32),
            jax.ShapeDtypeStruct(volume, F32),
            jax.ShapeDtypeStruct((1, 128), F32),
        ),
        in_specs=[hbm] * 13,
        out_specs=(vmem, vmem, vmem),
        scratch_shapes=[
            pltpu.VMEM(volume, F32),
            pltpu.VMEM(volume, F32),
            pltpu.VMEM((9, ELEMS), F32),
            pltpu.VMEM((3, 4, ELEMS), F32),
            pltpu.VMEM((4, ELEMS), F32),
            pltpu.VMEM((1, ELEMS), F32),
            pltpu.VMEM((1, ELEMS), jnp.int32),
            pltpu.VMEM((1, ELEMS), jnp.int32),
            pltpu.VMEM((4, ELEMS), jnp.int32),
            pltpu.VMEM((4, ELEMS), jnp.int32),
            pltpu.VMEM((3, NODES, NODES), F32),
            pltpu.VMEM((NODES, 60), F32),
            pltpu.VMEM((4, 96, 96), BF16),
            pltpu.VMEM((4, 96, ELEMS), BF16),
            pltpu.VMEM((64, FACES), F32),
            pltpu.VMEM((128, FACES), BF16),
            pltpu.VMEM((2 * half, FACES), BF16),
            pltpu.VMEM((FACES, FACES), BF16),
            pltpu.VMEM(volume, F32),
            pltpu.VMEM((48, 64), F32),
            pltpu.VMEM((NEAR_BOXES, 16, 128), F32),
            pltpu.VMEM((far_count, 4, 128), F32),
            pltpu.VMEM((2, 16, 128), F32),
            pltpu.VMEM((NEAR_BOXES, 16, 128), F32),
            pltpu.VMEM((far_count, 4, 128), F32),
            pltpu.VMEM((2, 16, 128), F32),
            pltpu.VMEM((5 * RING, 4, 128), F32),
            pltpu.VMEM((NEAR_ROWS + 32, 128), F32),
            pltpu.VMEM((half - NEAR_ROWS - 32, 128), F32),
            pltpu.VMEM((1, 128), F32),
            pltpu.VMEM((ns, 1, 128), F32),
            pltpu.VMEM((1, 128), F32),
            pltpu.VMEM((ng, 1, 128), F32),
            dma((19,)),
            dma((2,)),
            dma((2,)),
            dma((2,)),
            dma((2,)),
            dma((2,)),
            dma((2,)),
            dma((5,)),
            dma((5,)),
        ],
        compiler_params=pltpu.CompilerParams(collective_id=0, has_side_effects=True, vmem_limit_bytes=24 << 20),
        name="section",
    )
    write = pl.pallas_call(
        finish,
        out_shape=(state, state, jax.ShapeDtypeStruct((1, 1), F32)),
        in_specs=[vmem] * 3,
        out_specs=(hbm, hbm, hbm),
        scratch_shapes=[pltpu.VMEM((1, 1), F32), dma((9,))],
        compiler_params=pltpu.CompilerParams(vmem_limit_bytes=8 << 20),
        name="finish",
    )

    def keep(x):
        return pltpu.with_memory_space_constraint(x, pltpu.HBM)

    def local(
        fields,
        section_store,
        metric_terms,
        normals,
        face_scale,
        damping,
        absorb_mask,
        refine_level,
        face_source,
        orientation,
        derivative,
        lift_matrix,
    ):
        fields_new, store_new, energy_new = call(*map(keep,(
            jnp.transpose(fields, (1, 0, 2)),
            jnp.transpose(section_store, (1, 0, 2)),
            metric_terms,
            jnp.transpose(normals, (1, 0, 2)),
            face_scale,
            damping.reshape(1, ELEMS),
            absorb_mask.reshape(1, ELEMS),
            refine_level.reshape(1, ELEMS),
            face_source,
            orientation,
            derivative,
            lift_matrix,
            jnp.asarray(pick_table(), BF16),
        )))
        fields_next, store_next, energy = write(fields_new, store_new, energy_new)
        return (
            jnp.transpose(fields_next, (1, 0, 2)),
            jnp.transpose(store_next, (1, 0, 2)),
            energy.reshape(()),
        )

    in_specs = (
        P(None, None, both),
        P(None, None, both),
        P(None, both),
        P(None, None, both),
        P(None, both),
        P(both),
        P(both),
        P(both),
        P(None, both),
        P(None, both),
        P(),
        P(),
    )
    out_specs = (P(None, None, both), P(None, None, both), P())
    return jax.shard_map(local, mesh=mesh, in_specs=in_specs, out_specs=out_specs, check_vma=False)
```

```python
import functools

import jax
import jax.numpy as jnp
import numpy as np
from jax import lax
from jax.experimental import pallas as pl
from jax.experimental.pallas import tpu as pltpu
from jax.sharding import PartitionSpec as P

MESH = pl.DeviceIdType.MESH
F32 = jnp.float32
BF16 = jnp.bfloat16

RUNGE_CARRY = -567301805773.0 / 1357537059087.0
RUNGE_ADVANCE = 5161836677717.0 / 13612068292357.0
TIME_STEP = 0.02

NODES = 35
ELEMS = 256
FACES = 4 * ELEMS
NEAR = 4
NEAR_ROWS = 8 * 16


def pick_table():
    volume = [(a, b, c, 4 - a - b - c) for a in range(5) for b in range(5 - a) for c in range(5 - a - b)]
    triples = [(a, b, 4 - a - b) for a in range(5) for b in range(5 - a)]
    orders = [(0, 1, 2), (1, 2, 0), (2, 0, 1), (0, 2, 1), (2, 1, 0), (1, 0, 2)]
    inverse = [0, 2, 1, 3, 4, 5]
    table = np.zeros((4, 6, 16, 2, 48), np.float32)
    for facet in range(4):
        others = [corner for corner in range(4) if corner != facet]
        for option in range(6):
            order = orders[inverse[option]]
            for node in range(15):
                triple = triples[node]
                turned = tuple(triple[q] for q in order)
                corners = [0, 0, 0, 0]
                for place in range(3):
                    corners[others[place]] = turned[place]
                table[facet, option, node, :, volume.index(tuple(corners))] = 1.0
    return table.reshape(4, 96, 96)


def split(value):
    high = value.astype(BF16)
    low = (value - high.astype(F32)).astype(BF16)
    return high, low


def kernel(
    ng,
    ns,
    half,
    fields_hbm,
    store_hbm,
    metric_hbm,
    normals_hbm,
    scale_hbm,
    damping_hbm,
    mask_hbm,
    level_hbm,
    source_hbm,
    orient_hbm,
    deriv_hbm,
    lift_hbm,
    picks_hbm,
    fields_new,
    store_new,
    energy_new,
    fields,
    store,
    metric,
    normals,
    scale,
    damping,
    mask,
    level,
    source,
    orient,
    deriv,
    lift,
    picks,
    stacked,
    inner,
    turned,
    place,
    local,
    base,
    lifts,
    deriv_pad,
    deriv_cat,
    near_box,
    far_box,
    grp_box,
    near_in,
    far_in,
    grp_in,
    near_stage,
    far_stage,
    row_own,
    row_sub,
    sum_own,
    row_grp,
    total_own,
    total_in,
    load_sem,
    near_sems,
    far_sems,
    grp_send,
    grp_recv,
    sub_sems,
    top_sems,
    up_sems,
    down_sems,
):
    g = lax.axis_index("grp")
    s = lax.axis_index("sub")
    grp_at = NEAR_ROWS
    far_at = NEAR_ROWS + 32
    rows = far_at + 4 * (ns - 9)

    def load(at, src, dst):
        return pltpu.make_async_copy(src, dst, load_sem.at[at])

    load_source = load(0, source_hbm, source)
    load_orient = load(1, orient_hbm, orient)
    load_fields = [load(2 + c, fields_hbm.at[:, c, :], fields.at[c]) for c in range(4)]
    load_picks = load(6, picks_hbm, picks)
    load_store = [load(7 + c, store_hbm.at[:, c, :], store.at[c]) for c in range(4)]
    load_rest = [
        load(11, metric_hbm, metric),
        load(12, normals_hbm, normals),
        load(13, scale_hbm, scale),
        load(14, damping_hbm, damping),
        load(15, mask_hbm, mask),
        load(16, level_hbm, level),
        load(17, deriv_hbm, deriv),
        load(18, lift_hbm, lift),
    ]
    def peer(k):
        other = s + k
        return jnp.where(other >= ns, other - ns, other)

    def peer_grp(k):
        other = g + k
        return jnp.where(other >= ng, other - ng, other)

    grp_in[...] = jnp.zeros_like(grp_in)

    order = sorted(range(1, ns), key=lambda k: -min(k, ns - k))

    barrier = pltpu.get_barrier_semaphore()
    for k in order:
        pl.semaphore_signal(barrier, inc=1, device_id=(g, peer(k)), device_id_type=MESH)
    for k in range(1, ng):
        pl.semaphore_signal(barrier, inc=1, device_id=(peer_grp(k), s), device_id_type=MESH)

    for copy in [load_source, load_orient, *load_fields, load_picks, *load_rest, *load_store]:
        copy.start()

    load_source.wait()
    codes = jnp.concatenate([source[f : f + 1, :] for f in range(4)], axis=1)
    slot = codes - FACES
    block = slot >> 5
    rank = slot & 31
    delta = block - s
    delta = jnp.where(delta < 0, delta + ns, delta)
    in_sub = block < ns
    after = in_sub & (delta <= NEAR)
    before = in_sub & (delta >= ns - NEAR)
    apart = in_sub & (delta > NEAR) & (delta < ns - NEAR)
    box = jnp.where(after, (delta - 1) * 16, jnp.where(before, (delta - ns + 8) * 16, grp_at + (block - ns) * 16))
    row = jnp.where(apart, far_at + (delta - NEAR - 1) * 4 + (rank & 3), box + (rank & 15))
    row = row + half * jnp.where(apart, (rank >> 2) & 1, rank >> 4)
    row = jnp.where(codes >= FACES, row, -1)

    def build_place(i, carry):
        at = lax.broadcasted_iota(jnp.int32, (32, FACES), 0) + i * 32
        place[pl.ds(i * 32, 32), :] = jnp.where(at == row, 1.0, 0.0).astype(BF16)
        return carry

    lax.fori_loop(0, 2 * half // 32, build_place, 0)

    stacked[...] = jnp.zeros_like(stacked)
    load_orient.wait()
    load_picks.wait()
    for c in range(4):
        load_fields[c].wait()
        high, low = split(fields[c])
        stacked[c, 0:NODES, :] = high
        stacked[c, 48 : 48 + NODES, :] = low
    for f in range(4):
        option_of = orient[f : f + 1, :]
        at = slice(f * ELEMS, (f + 1) * ELEMS)
        for c in range(4):
            found = jnp.dot(picks[f], stacked[c], preferred_element_type=F32)
            inner[c * 16 : (c + 1) * 16, at] = found[0:16]
            chosen = found[0:16]
            for option in range(1, 6):
                chosen = jnp.where(option_of == option, found[option * 16 : (option + 1) * 16], chosen)
            high, low = split(chosen)
            turned[c * 16 : (c + 1) * 16, at] = high
            turned[64 + c * 16 : 64 + (c + 1) * 16, at] = low

    across = (((1,), (1,)), ((), ()))
    left = lax.dot_general(place[:half, :], turned[...], across, preferred_element_type=F32)
    right = lax.dot_general(place[half:, :], turned[...], across, preferred_element_type=F32)
    left = left + pltpu.roll(left, 64, 1)
    right = right + pltpu.roll(right, 64, 1)
    lane = lax.broadcasted_iota(jnp.int32, (half, 128), 1)
    out = jnp.where(lane < 64, left, right)
    near_box[...] = out[:grp_at].reshape(8, 16, 128)
    for b in range(ns - 9):
        far_box[b] = out[far_at + 4 * b : far_at + 4 * b + 4]
    grp_box[...] = out[grp_at:far_at].reshape(2, 16, 128)

    pl.semaphore_wait(barrier, ns - 1 + ng - 1)

    def near_at(k):
        return k - 1 if k <= NEAR else k - ns + 8

    def sub_copy(k):
        if NEAR < k < ns - NEAR:
            src, dst, sems = far_box.at[k - NEAR - 1], far_in.at[ns - k - NEAR - 1], far_sems
        else:
            src, dst, sems = near_box.at[near_at(k)], near_in.at[near_at(ns - k)], near_sems
        return pltpu.make_async_remote_copy(
            src_ref=src,
            dst_ref=dst,
            send_sem=sems.at[0],
            recv_sem=sems.at[1],
            device_id=(g, peer(k)),
            device_id_type=MESH,
        )

    def grp_copy(up):
        return pltpu.make_async_remote_copy(
            src_ref=grp_box.at[up],
            dst_ref=grp_in.at[1 - up],
            send_sem=grp_send.at[up],
            recv_sem=grp_recv.at[1 - up],
            device_id=(g + 2 * up - 1, s),
            device_id_type=MESH,
        )

    for k in order:
        sub_copy(k).start()

    @pl.when(g < ng - 1)
    def _():
        grp_copy(1).start()

    @pl.when(g > 0)
    def _():
        grp_copy(0).start()

    for copy in [*load_rest, *load_store]:
        copy.wait()
    growth = jnp.exp2(level[...].astype(F32))
    absorb = damping[...] * mask[...].astype(F32)

    def build_local(i, carry):
        at = lax.broadcasted_iota(jnp.int32, (32, FACES), 0) + i * 32
        local[pl.ds(i * 32, 32), :] = jnp.where(at == codes, 1.0, 0.0).astype(BF16)
        return carry

    lax.fori_loop(0, FACES // 32, build_local, 0)
    outer_own = jnp.dot(turned[...], local[...], preferred_element_type=F32)

    lifts[...] = jnp.zeros_like(lifts)
    for f in range(4):
        lifts[0:NODES, f * 16 : f * 16 + 15] = lift[:, f * 15 : (f + 1) * 15]
    lift_high, lift_low = split(lifts[...])
    lift_cat = jnp.concatenate([lift_high, lift_high, lift_low], axis=1)

    deriv_pad[...] = jnp.zeros_like(deriv_pad)
    for d in range(3):
        deriv_pad[48 * d : 48 * d + NODES, 0:NODES] = deriv[d]
    deriv_high, deriv_low = split(deriv_pad[...])
    deriv_cat[:, 0:48] = deriv_high
    deriv_cat[:, 48:96] = deriv_high
    found = [
        jnp.dot(deriv_cat[...], stacked[c], preferred_element_type=F32)
        + jnp.dot(deriv_low, stacked[c, 0:48, :], preferred_element_type=F32)
        for c in range(4)
    ]
    slopes = [[found[c][48 * d : 48 * d + NODES] for c in range(4)] for d in range(3)]

    def physical(x, c):
        total = metric[3 * x : 3 * x + 1, :] * slopes[0][c]
        for y in range(1, 3):
            total = total + metric[3 * x + y : 3 * x + y + 1, :] * slopes[y][c]
        return growth * total

    volume = [-(physical(0, 1) + physical(1, 2) + physical(2, 3))]
    volume += [-physical(x, 0) for x in range(3)]
    for c in range(4):
        base[c] = RUNGE_CARRY * store[c] + TIME_STEP * (volume[c] - absorb * fields[c])

    def arrival(ref, sems):
        return pltpu.make_async_copy(ref, ref, sems.at[1])

    def picked(stage, at):
        came = stage[...].T
        high, low = split(came)
        deep = stage.shape[0]
        left = jnp.concatenate([high[0:64], low[0:64]], axis=0)
        right = jnp.concatenate([high[64:128], low[64:128]], axis=0)
        return jnp.dot(left, place[at : at + deep, :], preferred_element_type=F32) + jnp.dot(
            right, place[half + at : half + at + deep, :], preferred_element_type=F32
        )

    far_stage[...] = jnp.zeros_like(far_stage)
    arrival(near_in, near_sems).wait()

    @pl.when(g > 0)
    def _():
        pltpu.make_async_copy(grp_in.at[0], grp_in.at[0], grp_recv.at[0]).wait()

    @pl.when(g < ng - 1)
    def _():
        pltpu.make_async_copy(grp_in.at[1], grp_in.at[1], grp_recv.at[1]).wait()

    near_stage[0:grp_at, :] = near_in[...].reshape(grp_at, 128)
    near_stage[grp_at:far_at, :] = grp_in[...].reshape(32, 128)
    outer_near = outer_own + picked(near_stage, 0)

    arrival(far_in, far_sems).wait()
    for b in range(ns - 9):
        far_stage[4 * b : 4 * b + 4, :] = far_in[b]
    outer_all = outer_near + picked(far_stage, far_at)
    outer = outer_all[0:64] + outer_all[64:128]

    flux = [[None] * 4 for _ in range(4)]
    for f in range(4):
        at = slice(f * ELEMS, (f + 1) * ELEMS)
        wall = source[f : f + 1, :] < 0
        norm = [normals[x, f : f + 1, :] for x in range(3)]
        press_in = inner[0:16, at]
        veloc_in = [inner[(1 + x) * 16 : (2 + x) * 16, at] for x in range(3)]
        along = norm[0] * veloc_in[0] + norm[1] * veloc_in[1] + norm[2] * veloc_in[2]
        press_jump = jnp.where(wall, 0.0, press_in - outer[0:16, at])
        normal_jump = jnp.zeros_like(along)
        for x in range(3):
            met = jnp.where(wall, veloc_in[x] - 2.0 * norm[x] * along, outer[(1 + x) * 16 : (2 + x) * 16, at])
            normal_jump = normal_jump + norm[x] * (veloc_in[x] - met)
        weight = 0.5 * scale[f : f + 1, :] * growth
        flux[0][f] = weight * (normal_jump - press_jump)
        for x in range(3):
            flux[1 + x][f] = -norm[x] * flux[0][f]

    energy = jnp.zeros((1, ELEMS), F32)
    for c in range(4):
        high, low = split(jnp.concatenate(flux[c], axis=0))
        lifted = jnp.dot(lift_cat, jnp.concatenate([high, low, high], axis=0), preferred_element_type=F32)
        store_next = base[c] + TIME_STEP * lifted[0:NODES]
        fields_next = fields[c] + RUNGE_ADVANCE * store_next
        store_new[c] = store_next
        fields_new[c] = fields_next
        energy = energy + jnp.sum(fields_next * fields_next, axis=0, keepdims=True)
    energy = absorb * energy
    row_own[...] = energy[:, 0:128] + energy[:, 128:256]

    core = g % 2
    level_y = g // 2
    count_y = ng // 2
    lead = 2 * level_y + 1

    def sub_row(k, sems):
        return pltpu.make_async_remote_copy(
            src_ref=row_own,
            dst_ref=row_sub.at[2 * s + core],
            send_sem=sems.at[0],
            recv_sem=sub_sems.at[1],
            device_id=(lead, peer(k)),
            device_id_type=MESH,
        )

    for k in order:
        sub_row(k, sub_sems).start()

    many = row_sub.at[0 : 2 * ns - 1]
    rest = row_grp.at[0 : count_y - 1]

    def top_row(k):
        other = level_y + k
        return pltpu.make_async_remote_copy(
            src_ref=sum_own,
            dst_ref=row_grp.at[level_y],
            send_sem=top_sems.at[0],
            recv_sem=top_sems.at[1],
            device_id=(2 * jnp.where(other >= count_y, other - count_y, other) + 1, s),
            device_id_type=MESH,
        )

    def down_row():
        return pltpu.make_async_remote_copy(
            src_ref=total_own,
            dst_ref=total_in,
            send_sem=down_sems.at[0],
            recv_sem=down_sems.at[1],
            device_id=(2 * level_y, s),
            device_id_type=MESH,
        )

    @pl.when(core == 0)
    def _():
        sub_row(0, up_sems).start()

    @pl.when(core == 1)
    def _():
        row_sub[2 * s + 1] = row_own[...]
        arrival(many, sub_sems).wait()
        sum_own[...] = jnp.sum(row_sub[...], axis=0)
        for k in sorted(range(1, count_y), key=lambda k: -min(k, count_y - k)):
            top_row(k).start()
        row_grp[level_y] = sum_own[...]

    def left_here(ref, sem):
        pltpu.make_async_copy(ref, ref, sem).wait()

    left_here(near_box, near_sems.at[0])
    left_here(far_box, far_sems.at[0])
    left_here(row_sub.at[0 : ns - 1], sub_sems.at[0])

    @pl.when(g < ng - 1)
    def _():
        grp_copy(1).wait_send()

    @pl.when(g > 0)
    def _():
        grp_copy(0).wait_send()

    @pl.when(core == 1)
    def _():
        arrival(rest, top_sems).wait()
        total = jnp.sum(jnp.sum(row_grp[...], axis=0), axis=1, keepdims=True)
        total_own[...] = jnp.broadcast_to(total * (1.0 / (ELEMS * NODES * ng * ns)), (1, 128))
        down_row().start()
        energy_new[...] = total_own[...]
        left_here(rest, top_sems.at[0])
        down_row().wait_send()

    @pl.when(core == 0)
    def _():
        sub_row(0, up_sems).wait_send()
        down_row().wait_recv()
        energy_new[...] = total_in[...]


def finish(fields_new, store_new, energy_new, fields_out, store_out, energy_out, single, out_sem):
    single[...] = energy_new[:, 0:1]
    outs = [pltpu.make_async_copy(fields_new.at[c], fields_out.at[:, c, :], out_sem.at[c]) for c in range(4)]
    outs += [pltpu.make_async_copy(store_new.at[c], store_out.at[:, c, :], out_sem.at[4 + c]) for c in range(4)]
    outs += [pltpu.make_async_copy(single, energy_out, out_sem.at[8])]
    for copy in outs:
        copy.start()
    for copy in outs:
        copy.wait()


def solution(mesh):
    ng, ns = mesh.shape["grp"], mesh.shape["sub"]
    rows = NEAR_ROWS + 4 * (ns - 9) + 32
    half = -(-rows // 16) * 16
    both = ("grp", "sub")
    hbm = pl.BlockSpec(memory_space=pltpu.HBM)
    vmem = pl.BlockSpec(memory_space=pltpu.VMEM)
    dma = pltpu.SemaphoreType.DMA
    volume = (4, NODES, ELEMS)
    state = jax.ShapeDtypeStruct((NODES, 4, ELEMS), F32)

    call = pl.pallas_call(
        functools.partial(kernel, ng, ns, half),
        out_shape=(
            jax.ShapeDtypeStruct(volume, F32),
            jax.ShapeDtypeStruct(volume, F32),
            jax.ShapeDtypeStruct((1, 128), F32),
        ),
        in_specs=[hbm] * 13,
        out_specs=(vmem, vmem, vmem),
        scratch_shapes=[
            pltpu.VMEM(volume, F32),
            pltpu.VMEM(volume, F32),
            pltpu.VMEM((9, ELEMS), F32),
            pltpu.VMEM((3, 4, ELEMS), F32),
            pltpu.VMEM((4, ELEMS), F32),
            pltpu.VMEM((1, ELEMS), F32),
            pltpu.VMEM((1, ELEMS), jnp.int32),
            pltpu.VMEM((1, ELEMS), jnp.int32),
            pltpu.VMEM((4, ELEMS), jnp.int32),
            pltpu.VMEM((4, ELEMS), jnp.int32),
            pltpu.VMEM((3, NODES, NODES), F32),
            pltpu.VMEM((NODES, 60), F32),
            pltpu.VMEM((4, 96, 96), BF16),
            pltpu.VMEM((4, 96, ELEMS), BF16),
            pltpu.VMEM((64, FACES), F32),
            pltpu.VMEM((128, FACES), BF16),
            pltpu.VMEM((2 * half, FACES), BF16),
            pltpu.VMEM((FACES, FACES), BF16),
            pltpu.VMEM(volume, F32),
            pltpu.VMEM((48, 64), F32),
            pltpu.VMEM((144, 48), F32),
            pltpu.VMEM((144, 96), BF16),
            pltpu.VMEM((8, 16, 128), F32),
            pltpu.VMEM((ns - 9, 4, 128), F32),
            pltpu.VMEM((2, 16, 128), F32),
            pltpu.VMEM((8, 16, 128), F32),
            pltpu.VMEM((ns - 9, 4, 128), F32),
            pltpu.VMEM((2, 16, 128), F32),
            pltpu.VMEM((NEAR_ROWS + 32, 128), F32),
            pltpu.VMEM((half - NEAR_ROWS - 32, 128), F32),
            pltpu.VMEM((1, 128), F32),
            pltpu.VMEM((2 * ns, 1, 128), F32),
            pltpu.VMEM((1, 128), F32),
            pltpu.VMEM((ng // 2, 1, 128), F32),
            pltpu.VMEM((1, 128), F32),
            pltpu.VMEM((1, 128), F32),
            dma((19,)),
            dma((2,)),
            dma((2,)),
            dma((2,)),
            dma((2,)),
            dma((2,)),
            dma((2,)),
            dma((1,)),
            dma((2,)),
        ],
        compiler_params=pltpu.CompilerParams(collective_id=0, has_side_effects=True, vmem_limit_bytes=24 << 20),
        name="section",
    )
    write = pl.pallas_call(
        finish,
        out_shape=(state, state, jax.ShapeDtypeStruct((1, 1), F32)),
        in_specs=[vmem] * 3,
        out_specs=(hbm, hbm, hbm),
        scratch_shapes=[pltpu.VMEM((1, 1), F32), dma((9,))],
        compiler_params=pltpu.CompilerParams(vmem_limit_bytes=8 << 20),
        name="finish",
    )

    def keep(x):
        return pltpu.with_memory_space_constraint(x, pltpu.HBM)

    def local(
        fields,
        section_store,
        metric_terms,
        normals,
        face_scale,
        damping,
        absorb_mask,
        refine_level,
        face_source,
        orientation,
        derivative,
        lift_matrix,
    ):
        fields_new, store_new, energy_new = call(*map(keep,(
            jnp.transpose(fields, (1, 0, 2)),
            jnp.transpose(section_store, (1, 0, 2)),
            metric_terms,
            jnp.transpose(normals, (1, 0, 2)),
            face_scale,
            damping.reshape(1, ELEMS),
            absorb_mask.reshape(1, ELEMS),
            refine_level.reshape(1, ELEMS),
            face_source,
            orientation,
            derivative,
            lift_matrix,
            jnp.asarray(pick_table(), BF16),
        )))
        fields_next, store_next, energy = write(fields_new, store_new, energy_new)
        return (
            jnp.transpose(fields_next, (1, 0, 2)),
            jnp.transpose(store_next, (1, 0, 2)),
            energy.reshape(()),
        )

    in_specs = (
        P(None, None, both),
        P(None, None, both),
        P(None, both),
        P(None, None, both),
        P(None, both),
        P(both),
        P(both),
        P(both),
        P(None, both),
        P(None, both),
        P(),
        P(),
    )
    out_specs = (P(None, None, both), P(None, None, both), P())
    return jax.shard_map(local, mesh=mesh, in_specs=in_specs, out_specs=out_specs, check_vma=False)
```

```python
import functools

import jax
import jax.numpy as jnp
import numpy as np
from jax import lax
from jax.experimental import pallas as pl
from jax.experimental.pallas import tpu as pltpu
from jax.sharding import PartitionSpec as P

MESH = pl.DeviceIdType.MESH
F32 = jnp.float32
BF16 = jnp.bfloat16

RUNGE_CARRY = -567301805773.0 / 1357537059087.0
RUNGE_ADVANCE = 5161836677717.0 / 13612068292357.0
TIME_STEP = 0.02

NODES = 35
ELEMS = 256
FACES = 4 * ELEMS
NEAR = 4
FAR_Y = 2
NEAR_ROWS = 8 * 16


def pick_table():
    volume = [(a, b, c, 4 - a - b - c) for a in range(5) for b in range(5 - a) for c in range(5 - a - b)]
    triples = [(a, b, 4 - a - b) for a in range(5) for b in range(5 - a)]
    orders = [(0, 1, 2), (1, 2, 0), (2, 0, 1), (0, 2, 1), (2, 1, 0), (1, 0, 2)]
    inverse = [0, 2, 1, 3, 4, 5]
    table = np.zeros((4, 6, 16, 2, 48), np.float32)
    for facet in range(4):
        others = [corner for corner in range(4) if corner != facet]
        for option in range(6):
            order = orders[inverse[option]]
            for node in range(15):
                triple = triples[node]
                turned = tuple(triple[q] for q in order)
                corners = [0, 0, 0, 0]
                for place in range(3):
                    corners[others[place]] = turned[place]
                table[facet, option, node, :, volume.index(tuple(corners))] = 1.0
    return table.reshape(4, 96, 96)


def split(value):
    high = value.astype(BF16)
    low = (value - high.astype(F32)).astype(BF16)
    return high, low


def kernel(
    ng,
    ns,
    half,
    fields_hbm,
    store_hbm,
    metric_hbm,
    normals_hbm,
    scale_hbm,
    damping_hbm,
    mask_hbm,
    level_hbm,
    source_hbm,
    orient_hbm,
    deriv_hbm,
    lift_hbm,
    picks_hbm,
    fields_new,
    store_new,
    energy_new,
    fields,
    store,
    metric,
    normals,
    scale,
    damping,
    mask,
    level,
    source,
    orient,
    deriv,
    lift,
    picks,
    stacked,
    inner,
    turned,
    place,
    local,
    base,
    lifts,
    deriv_pad,
    deriv_cat,
    near_box,
    far_box,
    grp_box,
    near_in,
    far_in,
    grp_in,
    near_stage,
    far_stage,
    row_own,
    row_sub,
    sum_own,
    row_grp,
    total_own,
    total_in,
    row_first,
    load_sem,
    near_sems,
    far_sems,
    grp_send,
    grp_recv,
    sub_sems,
    top_sems,
    up_sems,
    down_sems,
    first_send,
    first_recv,
):
    g = lax.axis_index("grp")
    s = lax.axis_index("sub")
    grp_at = NEAR_ROWS
    far_at = NEAR_ROWS + 32
    rows = far_at + 4 * (ns - 9)

    def load(at, src, dst):
        return pltpu.make_async_copy(src, dst, load_sem.at[at])

    load_source = load(0, source_hbm, source)
    load_orient = load(1, orient_hbm, orient)
    load_fields = [load(2 + c, fields_hbm.at[:, c, :], fields.at[c]) for c in range(4)]
    load_picks = load(6, picks_hbm, picks)
    load_store = [load(7 + c, store_hbm.at[:, c, :], store.at[c]) for c in range(4)]
    load_rest = [
        load(11, metric_hbm, metric),
        load(12, normals_hbm, normals),
        load(13, scale_hbm, scale),
        load(14, damping_hbm, damping),
        load(15, mask_hbm, mask),
        load(16, level_hbm, level),
        load(17, deriv_hbm, deriv),
        load(18, lift_hbm, lift),
    ]
    def peer(k):
        other = s + k
        return jnp.where(other >= ns, other - ns, other)

    def peer_grp(k):
        other = g + k
        return jnp.where(other >= ng, other - ng, other)

    grp_in[...] = jnp.zeros_like(grp_in)

    order = sorted(range(1, ns), key=lambda k: -min(k, ns - k))

    barrier = pltpu.get_barrier_semaphore()
    for k in order:
        pl.semaphore_signal(barrier, inc=1, device_id=(g, peer(k)), device_id_type=MESH)
    for k in range(1, ng):
        pl.semaphore_signal(barrier, inc=1, device_id=(peer_grp(k), s), device_id_type=MESH)

    for copy in [load_source, load_orient, *load_fields, load_picks, *load_rest, *load_store]:
        copy.start()

    load_source.wait()
    codes = jnp.concatenate([source[f : f + 1, :] for f in range(4)], axis=1)
    slot = codes - FACES
    block = slot >> 5
    rank = slot & 31
    delta = block - s
    delta = jnp.where(delta < 0, delta + ns, delta)
    in_sub = block < ns
    after = in_sub & (delta <= NEAR)
    before = in_sub & (delta >= ns - NEAR)
    apart = in_sub & (delta > NEAR) & (delta < ns - NEAR)
    box = jnp.where(after, (delta - 1) * 16, jnp.where(before, (delta - ns + 8) * 16, grp_at + (block - ns) * 16))
    row = jnp.where(apart, far_at + (delta - NEAR - 1) * 4 + (rank & 3), box + (rank & 15))
    row = row + half * jnp.where(apart, (rank >> 2) & 1, rank >> 4)
    row = jnp.where(codes >= FACES, row, -1)

    def build_place(i, carry):
        at = lax.broadcasted_iota(jnp.int32, (32, FACES), 0) + i * 32
        place[pl.ds(i * 32, 32), :] = jnp.where(at == row, 1.0, 0.0).astype(BF16)
        return carry

    lax.fori_loop(0, 2 * half // 32, build_place, 0)

    stacked[...] = jnp.zeros_like(stacked)
    load_orient.wait()
    load_picks.wait()
    for c in range(4):
        load_fields[c].wait()
        high, low = split(fields[c])
        stacked[c, 0:NODES, :] = high
        stacked[c, 48 : 48 + NODES, :] = low
    for f in range(4):
        option_of = orient[f : f + 1, :]
        at = slice(f * ELEMS, (f + 1) * ELEMS)
        for c in range(4):
            found = jnp.dot(picks[f], stacked[c], preferred_element_type=F32)
            inner[c * 16 : (c + 1) * 16, at] = found[0:16]
            chosen = found[0:16]
            for option in range(1, 6):
                chosen = jnp.where(option_of == option, found[option * 16 : (option + 1) * 16], chosen)
            high, low = split(chosen)
            turned[c * 16 : (c + 1) * 16, at] = high
            turned[64 + c * 16 : 64 + (c + 1) * 16, at] = low

    across = (((1,), (1,)), ((), ()))
    left = lax.dot_general(place[:half, :], turned[...], across, preferred_element_type=F32)
    right = lax.dot_general(place[half:, :], turned[...], across, preferred_element_type=F32)
    left = left + pltpu.roll(left, 64, 1)
    right = right + pltpu.roll(right, 64, 1)
    lane = lax.broadcasted_iota(jnp.int32, (half, 128), 1)
    out = jnp.where(lane < 64, left, right)
    near_box[...] = out[:grp_at].reshape(8, 16, 128)
    for b in range(ns - 9):
        far_box[b] = out[far_at + 4 * b : far_at + 4 * b + 4]
    grp_box[...] = out[grp_at:far_at].reshape(2, 16, 128)

    pl.semaphore_wait(barrier, ns - 1 + ng - 1)

    def near_at(k):
        return k - 1 if k <= NEAR else k - ns + 8

    def sub_copy(k):
        if NEAR < k < ns - NEAR:
            src, dst, sems = far_box.at[k - NEAR - 1], far_in.at[ns - k - NEAR - 1], far_sems
        else:
            src, dst, sems = near_box.at[near_at(k)], near_in.at[near_at(ns - k)], near_sems
        return pltpu.make_async_remote_copy(
            src_ref=src,
            dst_ref=dst,
            send_sem=sems.at[0],
            recv_sem=sems.at[1],
            device_id=(g, peer(k)),
            device_id_type=MESH,
        )

    def grp_copy(up):
        return pltpu.make_async_remote_copy(
            src_ref=grp_box.at[up],
            dst_ref=grp_in.at[1 - up],
            send_sem=grp_send.at[up],
            recv_sem=grp_recv.at[1 - up],
            device_id=(g + 2 * up - 1, s),
            device_id_type=MESH,
        )

    for k in order:
        sub_copy(k).start()

    @pl.when(g < ng - 1)
    def _():
        grp_copy(1).start()

    @pl.when(g > 0)
    def _():
        grp_copy(0).start()

    for copy in [*load_rest, *load_store]:
        copy.wait()
    growth = jnp.exp2(level[...].astype(F32))
    absorb = damping[...] * mask[...].astype(F32)

    def build_local(i, carry):
        at = lax.broadcasted_iota(jnp.int32, (32, FACES), 0) + i * 32
        local[pl.ds(i * 32, 32), :] = jnp.where(at == codes, 1.0, 0.0).astype(BF16)
        return carry

    lax.fori_loop(0, FACES // 32, build_local, 0)
    outer_own = jnp.dot(turned[...], local[...], preferred_element_type=F32)

    lifts[...] = jnp.zeros_like(lifts)
    for f in range(4):
        lifts[0:NODES, f * 16 : f * 16 + 15] = lift[:, f * 15 : (f + 1) * 15]
    lift_high, lift_low = split(lifts[...])
    lift_cat = jnp.concatenate([lift_high, lift_high, lift_low], axis=1)

    deriv_pad[...] = jnp.zeros_like(deriv_pad)
    for d in range(3):
        deriv_pad[48 * d : 48 * d + NODES, 0:NODES] = deriv[d]
    deriv_high, deriv_low = split(deriv_pad[...])
    deriv_cat[:, 0:48] = deriv_high
    deriv_cat[:, 48:96] = deriv_high
    found = [
        jnp.dot(deriv_cat[...], stacked[c], preferred_element_type=F32)
        + jnp.dot(deriv_low, stacked[c, 0:48, :], preferred_element_type=F32)
        for c in range(4)
    ]
    slopes = [[found[c][48 * d : 48 * d + NODES] for c in range(4)] for d in range(3)]

    def physical(x, c):
        total = metric[3 * x : 3 * x + 1, :] * slopes[0][c]
        for y in range(1, 3):
            total = total + metric[3 * x + y : 3 * x + y + 1, :] * slopes[y][c]
        return growth * total

    volume = [-(physical(0, 1) + physical(1, 2) + physical(2, 3))]
    volume += [-physical(x, 0) for x in range(3)]
    for c in range(4):
        base[c] = RUNGE_CARRY * store[c] + TIME_STEP * (volume[c] - absorb * fields[c])

    def arrival(ref, sems):
        return pltpu.make_async_copy(ref, ref, sems.at[1])

    def picked(stage, at):
        came = stage[...].T
        high, low = split(came)
        deep = stage.shape[0]
        left = jnp.concatenate([high[0:64], low[0:64]], axis=0)
        right = jnp.concatenate([high[64:128], low[64:128]], axis=0)
        return jnp.dot(left, place[at : at + deep, :], preferred_element_type=F32) + jnp.dot(
            right, place[half + at : half + at + deep, :], preferred_element_type=F32
        )

    far_stage[...] = jnp.zeros_like(far_stage)
    arrival(near_in, near_sems).wait()

    @pl.when(g > 0)
    def _():
        pltpu.make_async_copy(grp_in.at[0], grp_in.at[0], grp_recv.at[0]).wait()

    @pl.when(g < ng - 1)
    def _():
        pltpu.make_async_copy(grp_in.at[1], grp_in.at[1], grp_recv.at[1]).wait()

    near_stage[0:grp_at, :] = near_in[...].reshape(grp_at, 128)
    near_stage[grp_at:far_at, :] = grp_in[...].reshape(32, 128)
    outer_near = outer_own + picked(near_stage, 0)

    arrival(far_in, far_sems).wait()
    for b in range(ns - 9):
        far_stage[4 * b : 4 * b + 4, :] = far_in[b]
    outer_all = outer_near + picked(far_stage, far_at)
    outer = outer_all[0:64] + outer_all[64:128]

    flux = [[None] * 4 for _ in range(4)]
    for f in range(4):
        at = slice(f * ELEMS, (f + 1) * ELEMS)
        wall = source[f : f + 1, :] < 0
        norm = [normals[x, f : f + 1, :] for x in range(3)]
        press_in = inner[0:16, at]
        veloc_in = [inner[(1 + x) * 16 : (2 + x) * 16, at] for x in range(3)]
        along = norm[0] * veloc_in[0] + norm[1] * veloc_in[1] + norm[2] * veloc_in[2]
        press_jump = jnp.where(wall, 0.0, press_in - outer[0:16, at])
        normal_jump = jnp.zeros_like(along)
        for x in range(3):
            met = jnp.where(wall, veloc_in[x] - 2.0 * norm[x] * along, outer[(1 + x) * 16 : (2 + x) * 16, at])
            normal_jump = normal_jump + norm[x] * (veloc_in[x] - met)
        weight = 0.5 * scale[f : f + 1, :] * growth
        flux[0][f] = weight * (normal_jump - press_jump)
        for x in range(3):
            flux[1 + x][f] = -norm[x] * flux[0][f]

    energy = jnp.zeros((1, ELEMS), F32)
    for c in range(4):
        high, low = split(jnp.concatenate(flux[c], axis=0))
        lifted = jnp.dot(lift_cat, jnp.concatenate([high, low, high], axis=0), preferred_element_type=F32)
        store_next = base[c] + TIME_STEP * lifted[0:NODES]
        fields_next = fields[c] + RUNGE_ADVANCE * store_next
        store_new[c] = store_next
        fields_new[c] = fields_next
        energy = energy + jnp.sum(fields_next * fields_next, axis=0, keepdims=True)
    energy = absorb * energy
    row_own[...] = energy[:, 0:128] + energy[:, 128:256]

    core = g % 2
    level_y = g // 2
    count_y = ng // 2
    lead = 2 * level_y + 1

    def sub_row(k, sems):
        return pltpu.make_async_remote_copy(
            src_ref=row_own,
            dst_ref=row_sub.at[2 * s + core],
            send_sem=sems.at[0],
            recv_sem=sub_sems.at[1],
            device_id=(lead, peer(k)),
            device_id_type=MESH,
        )

    many = row_sub.at[0 : 2 * ns - 1]
    rest = row_grp.at[0 : count_y - 1]

    def top_row(k):
        other = level_y + k
        return pltpu.make_async_remote_copy(
            src_ref=sum_own,
            dst_ref=row_grp.at[level_y],
            send_sem=top_sems.at[0],
            recv_sem=top_sems.at[1],
            device_id=(2 * jnp.where(other >= count_y, other - count_y, other) + 1, s),
            device_id_type=MESH,
        )

    def down_row():
        return pltpu.make_async_remote_copy(
            src_ref=total_own,
            dst_ref=total_in,
            send_sem=down_sems.at[0],
            recv_sem=down_sems.at[1],
            device_id=(2 * level_y, s),
            device_id_type=MESH,
        )

    first = (g == 1) & (s == 0)
    far_y = (level_y >= FAR_Y) & (level_y <= count_y - FAR_Y)

    def first_row():
        return pltpu.make_async_remote_copy(
            src_ref=row_own,
            dst_ref=row_first.at[level_y, 2 * s + core],
            send_sem=first_send.at[0],
            recv_sem=first_recv.at[level_y],
            device_id=(1, 0),
            device_id_type=MESH,
        )

    @pl.when(far_y)
    def _():
        first_row().start()

    for k in order:
        sub_row(k, sub_sems).start()

    @pl.when(core == 0)
    def _():
        sub_row(0, up_sems).start()

    @pl.when(core == 1)
    def _():
        row_sub[2 * s + 1] = row_own[...]
        arrival(many, sub_sems).wait()
        sum_own[...] = jnp.sum(row_sub[...], axis=0)
        for k in sorted(range(1, count_y), key=lambda k: -min(k, count_y - k)):

            @pl.when(jnp.logical_not((s == 0) & far_y & (level_y + k == count_y)))
            def _(k=k):
                top_row(k).start()

        row_grp[level_y] = sum_own[...]

    def left_here(ref, sem):
        pltpu.make_async_copy(ref, ref, sem).wait()

    left_here(near_box, near_sems.at[0])
    left_here(far_box, far_sems.at[0])
    left_here(row_sub.at[0 : ns - 1], sub_sems.at[0])

    @pl.when(g < ng - 1)
    def _():
        grp_copy(1).wait_send()

    @pl.when(g > 0)
    def _():
        grp_copy(0).wait_send()

    @pl.when(far_y)
    def _():
        first_row().wait_send()

    @pl.when(first)
    def _():
        arrival(row_grp.at[0 : 2 * FAR_Y - 2], top_sems).wait()
        for y in sorted(range(FAR_Y, count_y - FAR_Y + 1), key=lambda y: min(y, count_y - y)):
            pltpu.make_async_copy(row_first.at[y], row_first.at[y], first_recv.at[y]).wait()
            row_grp[y] = jnp.sum(row_first[y], axis=0)

    @pl.when((core == 1) & jnp.logical_not(first))
    def _():
        arrival(rest, top_sems).wait()

    @pl.when(core == 1)
    def _():
        total = jnp.sum(jnp.sum(row_grp[...], axis=0), axis=1, keepdims=True)
        total_own[...] = jnp.broadcast_to(total * (1.0 / (ELEMS * NODES * ng * ns)), (1, 128))
        down_row().start()
        energy_new[...] = total_own[...]
        down_row().wait_send()

        @pl.when((s == 0) & far_y)
        def _():
            left_here(row_grp.at[0 : count_y - 2], top_sems.at[0])

        @pl.when(jnp.logical_not((s == 0) & far_y))
        def _():
            left_here(rest, top_sems.at[0])

    @pl.when(core == 0)
    def _():
        sub_row(0, up_sems).wait_send()
        down_row().wait_recv()
        energy_new[...] = total_in[...]


def finish(fields_new, store_new, energy_new, fields_out, store_out, energy_out, single, out_sem):
    single[...] = energy_new[:, 0:1]
    outs = [pltpu.make_async_copy(fields_new.at[c], fields_out.at[:, c, :], out_sem.at[c]) for c in range(4)]
    outs += [pltpu.make_async_copy(store_new.at[c], store_out.at[:, c, :], out_sem.at[4 + c]) for c in range(4)]
    outs += [pltpu.make_async_copy(single, energy_out, out_sem.at[8])]
    for copy in outs:
        copy.start()
    for copy in outs:
        copy.wait()


def solution(mesh):
    ng, ns = mesh.shape["grp"], mesh.shape["sub"]
    rows = NEAR_ROWS + 4 * (ns - 9) + 32
    half = -(-rows // 16) * 16
    both = ("grp", "sub")
    hbm = pl.BlockSpec(memory_space=pltpu.HBM)
    vmem = pl.BlockSpec(memory_space=pltpu.VMEM)
    dma = pltpu.SemaphoreType.DMA
    volume = (4, NODES, ELEMS)
    state = jax.ShapeDtypeStruct((NODES, 4, ELEMS), F32)

    call = pl.pallas_call(
        functools.partial(kernel, ng, ns, half),
        out_shape=(
            jax.ShapeDtypeStruct(volume, F32),
            jax.ShapeDtypeStruct(volume, F32),
            jax.ShapeDtypeStruct((1, 128), F32),
        ),
        in_specs=[hbm] * 13,
        out_specs=(vmem, vmem, vmem),
        scratch_shapes=[
            pltpu.VMEM(volume, F32),
            pltpu.VMEM(volume, F32),
            pltpu.VMEM((9, ELEMS), F32),
            pltpu.VMEM((3, 4, ELEMS), F32),
            pltpu.VMEM((4, ELEMS), F32),
            pltpu.VMEM((1, ELEMS), F32),
            pltpu.VMEM((1, ELEMS), jnp.int32),
            pltpu.VMEM((1, ELEMS), jnp.int32),
            pltpu.VMEM((4, ELEMS), jnp.int32),
            pltpu.VMEM((4, ELEMS), jnp.int32),
            pltpu.VMEM((3, NODES, NODES), F32),
            pltpu.VMEM((NODES, 60), F32),
            pltpu.VMEM((4, 96, 96), BF16),
            pltpu.VMEM((4, 96, ELEMS), BF16),
            pltpu.VMEM((64, FACES), F32),
            pltpu.VMEM((128, FACES), BF16),
            pltpu.VMEM((2 * half, FACES), BF16),
            pltpu.VMEM((FACES, FACES), BF16),
            pltpu.VMEM(volume, F32),
            pltpu.VMEM((48, 64), F32),
            pltpu.VMEM((144, 48), F32),
            pltpu.VMEM((144, 96), BF16),
            pltpu.VMEM((8, 16, 128), F32),
            pltpu.VMEM((ns - 9, 4, 128), F32),
            pltpu.VMEM((2, 16, 128), F32),
            pltpu.VMEM((8, 16, 128), F32),
            pltpu.VMEM((ns - 9, 4, 128), F32),
            pltpu.VMEM((2, 16, 128), F32),
            pltpu.VMEM((NEAR_ROWS + 32, 128), F32),
            pltpu.VMEM((half - NEAR_ROWS - 32, 128), F32),
            pltpu.VMEM((1, 128), F32),
            pltpu.VMEM((2 * ns, 1, 128), F32),
            pltpu.VMEM((1, 128), F32),
            pltpu.VMEM((ng // 2, 1, 128), F32),
            pltpu.VMEM((1, 128), F32),
            pltpu.VMEM((1, 128), F32),
            pltpu.VMEM((ng // 2, 2 * ns, 1, 128), F32),
            dma((19,)),
            dma((2,)),
            dma((2,)),
            dma((2,)),
            dma((2,)),
            dma((2,)),
            dma((2,)),
            dma((1,)),
            dma((2,)),
            dma((1,)),
            dma((ng // 2,)),
        ],
        compiler_params=pltpu.CompilerParams(collective_id=0, has_side_effects=True, vmem_limit_bytes=24 << 20),
        name="section",
    )
    write = pl.pallas_call(
        finish,
        out_shape=(state, state, jax.ShapeDtypeStruct((1, 1), F32)),
        in_specs=[vmem] * 3,
        out_specs=(hbm, hbm, hbm),
        scratch_shapes=[pltpu.VMEM((1, 1), F32), dma((9,))],
        compiler_params=pltpu.CompilerParams(vmem_limit_bytes=8 << 20),
        name="finish",
    )

    def keep(x):
        return pltpu.with_memory_space_constraint(x, pltpu.HBM)

    def local(
        fields,
        section_store,
        metric_terms,
        normals,
        face_scale,
        damping,
        absorb_mask,
        refine_level,
        face_source,
        orientation,
        derivative,
        lift_matrix,
    ):
        fields_new, store_new, energy_new = call(*map(keep,(
            jnp.transpose(fields, (1, 0, 2)),
            jnp.transpose(section_store, (1, 0, 2)),
            metric_terms,
            jnp.transpose(normals, (1, 0, 2)),
            face_scale,
            damping.reshape(1, ELEMS),
            absorb_mask.reshape(1, ELEMS),
            refine_level.reshape(1, ELEMS),
            face_source,
            orientation,
            derivative,
            lift_matrix,
            jnp.asarray(pick_table(), BF16),
        )))
        fields_next, store_next, energy = write(fields_new, store_new, energy_new)
        return (
            jnp.transpose(fields_next, (1, 0, 2)),
            jnp.transpose(store_next, (1, 0, 2)),
            energy.reshape(()),
        )

    in_specs = (
        P(None, None, both),
        P(None, None, both),
        P(None, both),
        P(None, None, both),
        P(None, both),
        P(both),
        P(both),
        P(both),
        P(None, both),
        P(None, both),
        P(),
        P(),
    )
    out_specs = (P(None, None, both), P(None, None, both), P())
    return jax.shard_map(local, mesh=mesh, in_specs=in_specs, out_specs=out_specs, check_vma=False)
```

```python
import functools

import jax
import jax.numpy as jnp
import numpy as np
from jax import lax
from jax.experimental import pallas as pl
from jax.experimental.pallas import tpu as pltpu
from jax.sharding import PartitionSpec as P

MESH = pl.DeviceIdType.MESH
F32 = jnp.float32
BF16 = jnp.bfloat16

RUNGE_CARRY = -567301805773.0 / 1357537059087.0
RUNGE_ADVANCE = 5161836677717.0 / 13612068292357.0
TIME_STEP = 0.02

NODES = 35
ELEMS = 256
FACES = 4 * ELEMS
NEAR = 4
FAR_Y = 2
NEAR_ROWS = 8 * 16


def pick_table():
    volume = [(a, b, c, 4 - a - b - c) for a in range(5) for b in range(5 - a) for c in range(5 - a - b)]
    triples = [(a, b, 4 - a - b) for a in range(5) for b in range(5 - a)]
    orders = [(0, 1, 2), (1, 2, 0), (2, 0, 1), (0, 2, 1), (2, 1, 0), (1, 0, 2)]
    inverse = [0, 2, 1, 3, 4, 5]
    table = np.zeros((4, 6, 16, 2, 48), np.float32)
    for facet in range(4):
        others = [corner for corner in range(4) if corner != facet]
        for option in range(6):
            order = orders[inverse[option]]
            for node in range(15):
                triple = triples[node]
                turned = tuple(triple[q] for q in order)
                corners = [0, 0, 0, 0]
                for place in range(3):
                    corners[others[place]] = turned[place]
                table[facet, option, node, :, volume.index(tuple(corners))] = 1.0
    return table.reshape(4, 96, 96)


def split(value):
    high = value.astype(BF16)
    low = (value - high.astype(F32)).astype(BF16)
    return high, low


def kernel(
    ng,
    ns,
    half,
    fields_hbm,
    store_hbm,
    metric_hbm,
    normals_hbm,
    scale_hbm,
    damping_hbm,
    mask_hbm,
    level_hbm,
    source_hbm,
    orient_hbm,
    deriv_hbm,
    lift_hbm,
    picks_hbm,
    fields_new,
    store_new,
    energy_new,
    fields,
    store,
    metric,
    normals,
    scale,
    damping,
    mask,
    level,
    source,
    orient,
    deriv,
    lift,
    picks,
    stacked,
    inner,
    turned,
    place,
    local,
    base,
    lifts,
    deriv_pad,
    deriv_cat,
    near_box,
    far_box,
    grp_box,
    near_in,
    far_in,
    grp_in,
    near_stage,
    far_stage,
    row_own,
    row_sub,
    sum_own,
    row_grp,
    total_own,
    total_in,
    row_first,
    load_sem,
    near_sems,
    far_sems,
    grp_send,
    grp_recv,
    sub_sems,
    top_sems,
    up_sems,
    down_sems,
    first_send,
    first_recv,
):
    g = lax.axis_index("grp")
    s = lax.axis_index("sub")
    grp_at = NEAR_ROWS
    far_at = NEAR_ROWS + 32
    rows = far_at + 4 * (ns - 9)

    def load(at, src, dst):
        return pltpu.make_async_copy(src, dst, load_sem.at[at])

    load_source = load(0, source_hbm, source)
    load_orient = load(1, orient_hbm, orient)
    load_fields = [load(2 + c, fields_hbm.at[:, c, :], fields.at[c]) for c in range(4)]
    load_picks = load(6, picks_hbm, picks)
    load_store = [load(7 + c, store_hbm.at[:, c, :], store.at[c]) for c in range(4)]
    load_rest = [
        load(11, metric_hbm, metric),
        load(12, normals_hbm, normals),
        load(13, scale_hbm, scale),
        load(14, damping_hbm, damping),
        load(15, mask_hbm, mask),
        load(16, level_hbm, level),
        load(17, deriv_hbm, deriv),
        load(18, lift_hbm, lift),
    ]
    def peer(k):
        other = s + k
        return jnp.where(other >= ns, other - ns, other)

    def peer_grp(k):
        other = g + k
        return jnp.where(other >= ng, other - ng, other)

    grp_in[...] = jnp.zeros_like(grp_in)

    order = sorted(range(1, ns), key=lambda k: -min(k, ns - k))

    barrier = pltpu.get_barrier_semaphore()
    for k in order:
        pl.semaphore_signal(barrier, inc=1, device_id=(g, peer(k)), device_id_type=MESH)
    for k in range(1, ng):
        pl.semaphore_signal(barrier, inc=1, device_id=(peer_grp(k), s), device_id_type=MESH)

    for copy in [load_source, load_orient, *load_fields, load_picks, *load_rest, *load_store]:
        copy.start()

    load_source.wait()
    codes = jnp.concatenate([source[f : f + 1, :] for f in range(4)], axis=1)
    slot = codes - FACES
    block = slot >> 5
    rank = slot & 31
    delta = block - s
    delta = jnp.where(delta < 0, delta + ns, delta)
    in_sub = block < ns
    after = in_sub & (delta <= NEAR)
    before = in_sub & (delta >= ns - NEAR)
    apart = in_sub & (delta > NEAR) & (delta < ns - NEAR)
    box = jnp.where(after, (delta - 1) * 16, jnp.where(before, (delta - ns + 8) * 16, grp_at + (block - ns) * 16))
    row = jnp.where(apart, far_at + (delta - NEAR - 1) * 4 + (rank & 3), box + (rank & 15))
    row = row + half * jnp.where(apart, (rank >> 2) & 1, rank >> 4)
    row = jnp.where(codes >= FACES, row, -1)

    def build_place(i, carry):
        at = lax.broadcasted_iota(jnp.int32, (32, FACES), 0) + i * 32
        place[pl.ds(i * 32, 32), :] = jnp.where(at == row, 1.0, 0.0).astype(BF16)
        return carry

    lax.fori_loop(0, 2 * half // 32, build_place, 0)

    stacked[...] = jnp.zeros_like(stacked)
    load_orient.wait()
    load_picks.wait()
    for c in range(4):
        load_fields[c].wait()
        high, low = split(fields[c])
        stacked[c, 0:NODES, :] = high
        stacked[c, 48 : 48 + NODES, :] = low
    for f in range(4):
        option_of = orient[f : f + 1, :]
        at = slice(f * ELEMS, (f + 1) * ELEMS)
        for c in range(4):
            found = jnp.dot(picks[f], stacked[c], preferred_element_type=F32)
            inner[c * 16 : (c + 1) * 16, at] = found[0:16]
            chosen = found[0:16]
            for option in range(1, 6):
                chosen = jnp.where(option_of == option, found[option * 16 : (option + 1) * 16], chosen)
            high, low = split(chosen)
            turned[c * 16 : (c + 1) * 16, at] = high
            turned[64 + c * 16 : 64 + (c + 1) * 16, at] = low

    across = (((1,), (1,)), ((), ()))
    left = lax.dot_general(place[:half, :], turned[...], across, preferred_element_type=F32)
    right = lax.dot_general(place[half:, :], turned[...], across, preferred_element_type=F32)
    left = left + pltpu.roll(left, 64, 1)
    right = right + pltpu.roll(right, 64, 1)
    lane = lax.broadcasted_iota(jnp.int32, (half, 128), 1)
    out = jnp.where(lane < 64, left, right)
    near_box[...] = out[:grp_at].reshape(8, 16, 128)
    for b in range(ns - 9):
        far_box[b] = out[far_at + 4 * b : far_at + 4 * b + 4]
    grp_box[...] = out[grp_at:far_at].reshape(2, 16, 128)

    pl.semaphore_wait(barrier, ns - 1 + ng - 1)

    def near_at(k):
        return k - 1 if k <= NEAR else k - ns + 8

    def sub_copy(k):
        if NEAR < k < ns - NEAR:
            src, dst, sems = far_box.at[k - NEAR - 1], far_in.at[ns - k - NEAR - 1], far_sems
        else:
            src, dst, sems = near_box.at[near_at(k)], near_in.at[near_at(ns - k)], near_sems
        return pltpu.make_async_remote_copy(
            src_ref=src,
            dst_ref=dst,
            send_sem=sems.at[0],
            recv_sem=sems.at[1],
            device_id=(g, peer(k)),
            device_id_type=MESH,
        )

    def grp_copy(up):
        return pltpu.make_async_remote_copy(
            src_ref=grp_box.at[up],
            dst_ref=grp_in.at[1 - up],
            send_sem=grp_send.at[up],
            recv_sem=grp_recv.at[1 - up],
            device_id=(g + 2 * up - 1, s),
            device_id_type=MESH,
        )

    for k in order:
        sub_copy(k).start()

    @pl.when(g < ng - 1)
    def _():
        grp_copy(1).start()

    @pl.when(g > 0)
    def _():
        grp_copy(0).start()

    for copy in [*load_rest, *load_store]:
        copy.wait()
    growth = jnp.exp2(level[...].astype(F32))
    absorb = damping[...] * mask[...].astype(F32)

    def build_local(i, carry):
        at = lax.broadcasted_iota(jnp.int32, (32, FACES), 0) + i * 32
        local[pl.ds(i * 32, 32), :] = jnp.where(at == codes, 1.0, 0.0).astype(BF16)
        return carry

    lax.fori_loop(0, FACES // 32, build_local, 0)
    outer_own = jnp.dot(turned[...], local[...], preferred_element_type=F32)

    lifts[...] = jnp.zeros_like(lifts)
    for f in range(4):
        lifts[0:NODES, f * 16 : f * 16 + 15] = lift[:, f * 15 : (f + 1) * 15]
    lift_high, lift_low = split(lifts[...])
    lift_cat = jnp.concatenate([lift_high, lift_high, lift_low], axis=1)

    deriv_pad[...] = jnp.zeros_like(deriv_pad)
    for d in range(3):
        deriv_pad[48 * d : 48 * d + NODES, 0:NODES] = deriv[d]
    deriv_high, deriv_low = split(deriv_pad[...])
    deriv_cat[:, 0:48] = deriv_high
    deriv_cat[:, 48:96] = deriv_high
    found = [
        jnp.dot(deriv_cat[...], stacked[c], preferred_element_type=F32)
        + jnp.dot(deriv_low, stacked[c, 0:48, :], preferred_element_type=F32)
        for c in range(4)
    ]
    slopes = [[found[c][48 * d : 48 * d + NODES] for c in range(4)] for d in range(3)]

    def physical(x, c):
        total = metric[3 * x : 3 * x + 1, :] * slopes[0][c]
        for y in range(1, 3):
            total = total + metric[3 * x + y : 3 * x + y + 1, :] * slopes[y][c]
        return growth * total

    volume = [-(physical(0, 1) + physical(1, 2) + physical(2, 3))]
    volume += [-physical(x, 0) for x in range(3)]
    for c in range(4):
        base[c] = RUNGE_CARRY * store[c] + TIME_STEP * (volume[c] - absorb * fields[c])

    known = []
    norms = []
    shares = []
    for f in range(4):
        at = slice(f * ELEMS, (f + 1) * ELEMS)
        wall = source[f : f + 1, :] < 0
        norm = [normals[x, f : f + 1, :] for x in range(3)]
        press_in = inner[0:16, at]
        veloc_in = [inner[(1 + x) * 16 : (2 + x) * 16, at] for x in range(3)]
        along = norm[0] * veloc_in[0] + norm[1] * veloc_in[1] + norm[2] * veloc_in[2]
        square = norm[0] * norm[0] + norm[1] * norm[1] + norm[2] * norm[2]
        weight = 0.5 * scale[f : f + 1, :] * growth
        known.append(weight * jnp.where(wall, 2.0 * square * along, along - press_in))
        share = jnp.where(wall, 0.0, weight)
        norms.append(norm)
        shares.append([share] + [-share * norm[x] for x in range(3)])

    def weighed(part, f):
        at = slice(f * ELEMS, (f + 1) * ELEMS)
        total = 0.0
        for c in range(4):
            outer = part[c * 16 : (c + 1) * 16, at] + part[64 + c * 16 : 64 + (c + 1) * 16, at]
            total = total + shares[f][c] * outer
        return total

    def arrival(ref, sems):
        return pltpu.make_async_copy(ref, ref, sems.at[1])

    def picked(stage, at):
        came = stage[...].T
        high, low = split(came)
        deep = stage.shape[0]
        left = jnp.concatenate([high[0:64], low[0:64]], axis=0)
        right = jnp.concatenate([high[64:128], low[64:128]], axis=0)
        return jnp.dot(left, place[at : at + deep, :], preferred_element_type=F32) + jnp.dot(
            right, place[half + at : half + at + deep, :], preferred_element_type=F32
        )

    far_stage[...] = jnp.zeros_like(far_stage)
    arrival(near_in, near_sems).wait()

    @pl.when(g > 0)
    def _():
        pltpu.make_async_copy(grp_in.at[0], grp_in.at[0], grp_recv.at[0]).wait()

    @pl.when(g < ng - 1)
    def _():
        pltpu.make_async_copy(grp_in.at[1], grp_in.at[1], grp_recv.at[1]).wait()

    near_stage[0:grp_at, :] = near_in[...].reshape(grp_at, 128)
    near_stage[grp_at:far_at, :] = grp_in[...].reshape(32, 128)
    outer_near = outer_own + picked(near_stage, 0)

    known = [known[f] + weighed(outer_near, f) for f in range(4)]

    arrival(far_in, far_sems).wait()
    for b in range(ns - 9):
        far_stage[4 * b : 4 * b + 4, :] = far_in[b]
    arrived = picked(far_stage, far_at)
    flux = [[None] * 4 for _ in range(4)]
    for f in range(4):
        flux[0][f] = known[f] + weighed(arrived, f)
        for x in range(3):
            flux[1 + x][f] = -norms[f][x] * flux[0][f]

    energy = jnp.zeros((1, ELEMS), F32)
    for c in range(4):
        high, low = split(jnp.concatenate(flux[c], axis=0))
        lifted = jnp.dot(lift_cat, jnp.concatenate([high, low, high], axis=0), preferred_element_type=F32)
        store_next = base[c] + TIME_STEP * lifted[0:NODES]
        fields_next = fields[c] + RUNGE_ADVANCE * store_next
        store_new[c] = store_next
        fields_new[c] = fields_next
        energy = energy + jnp.sum(fields_next * fields_next, axis=0, keepdims=True)
    energy = absorb * energy
    row_own[...] = energy[:, 0:128] + energy[:, 128:256]

    core = g % 2
    level_y = g // 2
    count_y = ng // 2
    lead = 2 * level_y + 1

    def sub_row(k, sems):
        return pltpu.make_async_remote_copy(
            src_ref=row_own,
            dst_ref=row_sub.at[2 * s + core],
            send_sem=sems.at[0],
            recv_sem=sub_sems.at[1],
            device_id=(lead, peer(k)),
            device_id_type=MESH,
        )

    many = row_sub.at[0 : 2 * ns - 1]
    rest = row_grp.at[0 : count_y - 1]

    def top_row(k):
        other = level_y + k
        return pltpu.make_async_remote_copy(
            src_ref=sum_own,
            dst_ref=row_grp.at[level_y],
            send_sem=top_sems.at[0],
            recv_sem=top_sems.at[1],
            device_id=(2 * jnp.where(other >= count_y, other - count_y, other) + 1, s),
            device_id_type=MESH,
        )

    def down_row():
        return pltpu.make_async_remote_copy(
            src_ref=total_own,
            dst_ref=total_in,
            send_sem=down_sems.at[0],
            recv_sem=down_sems.at[1],
            device_id=(2 * level_y, s),
            device_id_type=MESH,
        )

    first = (g == 1) & (s == 0)
    far_y = (level_y >= FAR_Y) & (level_y <= count_y - FAR_Y)

    def first_row():
        return pltpu.make_async_remote_copy(
            src_ref=row_own,
            dst_ref=row_first.at[level_y, 2 * s + core],
            send_sem=first_send.at[0],
            recv_sem=first_recv.at[level_y],
            device_id=(1, 0),
            device_id_type=MESH,
        )

    @pl.when(far_y)
    def _():
        first_row().start()

    for k in order:
        sub_row(k, sub_sems).start()

    @pl.when(core == 0)
    def _():
        sub_row(0, up_sems).start()

    @pl.when(core == 1)
    def _():
        row_sub[2 * s + 1] = row_own[...]
        arrival(many, sub_sems).wait()
        sum_own[...] = jnp.sum(row_sub[...], axis=0)
        for k in sorted(range(1, count_y), key=lambda k: -min(k, count_y - k)):

            @pl.when(jnp.logical_not((s == 0) & far_y & (level_y + k == count_y)))
            def _(k=k):
                top_row(k).start()

        row_grp[level_y] = sum_own[...]

    def left_here(ref, sem):
        pltpu.make_async_copy(ref, ref, sem).wait()

    left_here(near_box, near_sems.at[0])
    left_here(far_box, far_sems.at[0])
    left_here(row_sub.at[0 : ns - 1], sub_sems.at[0])

    @pl.when(g < ng - 1)
    def _():
        grp_copy(1).wait_send()

    @pl.when(g > 0)
    def _():
        grp_copy(0).wait_send()

    @pl.when(far_y)
    def _():
        first_row().wait_send()

    @pl.when(first)
    def _():
        arrival(row_grp.at[0 : 2 * FAR_Y - 2], top_sems).wait()
        for y in sorted(range(FAR_Y, count_y - FAR_Y + 1), key=lambda y: min(y, count_y - y)):
            pltpu.make_async_copy(row_first.at[y], row_first.at[y], first_recv.at[y]).wait()
            row_grp[y] = jnp.sum(row_first[y], axis=0)

    @pl.when((core == 1) & jnp.logical_not(first))
    def _():
        arrival(rest, top_sems).wait()

    @pl.when(core == 1)
    def _():
        total = jnp.sum(jnp.sum(row_grp[...], axis=0), axis=1, keepdims=True)
        total_own[...] = jnp.broadcast_to(total * (1.0 / (ELEMS * NODES * ng * ns)), (1, 128))
        down_row().start()
        energy_new[...] = total_own[...]
        down_row().wait_send()

        @pl.when((s == 0) & far_y)
        def _():
            left_here(row_grp.at[0 : count_y - 2], top_sems.at[0])

        @pl.when(jnp.logical_not((s == 0) & far_y))
        def _():
            left_here(rest, top_sems.at[0])

    @pl.when(core == 0)
    def _():
        sub_row(0, up_sems).wait_send()
        down_row().wait_recv()
        energy_new[...] = total_in[...]


def finish(fields_new, store_new, energy_new, fields_out, store_out, energy_out, single, out_sem):
    single[...] = energy_new[:, 0:1]
    outs = [pltpu.make_async_copy(fields_new.at[c], fields_out.at[:, c, :], out_sem.at[c]) for c in range(4)]
    outs += [pltpu.make_async_copy(store_new.at[c], store_out.at[:, c, :], out_sem.at[4 + c]) for c in range(4)]
    outs += [pltpu.make_async_copy(single, energy_out, out_sem.at[8])]
    for copy in outs:
        copy.start()
    for copy in outs:
        copy.wait()


def solution(mesh):
    ng, ns = mesh.shape["grp"], mesh.shape["sub"]
    rows = NEAR_ROWS + 4 * (ns - 9) + 32
    half = -(-rows // 16) * 16
    both = ("grp", "sub")
    hbm = pl.BlockSpec(memory_space=pltpu.HBM)
    vmem = pl.BlockSpec(memory_space=pltpu.VMEM)
    dma = pltpu.SemaphoreType.DMA
    volume = (4, NODES, ELEMS)
    state = jax.ShapeDtypeStruct((NODES, 4, ELEMS), F32)

    call = pl.pallas_call(
        functools.partial(kernel, ng, ns, half),
        out_shape=(
            jax.ShapeDtypeStruct(volume, F32),
            jax.ShapeDtypeStruct(volume, F32),
            jax.ShapeDtypeStruct((1, 128), F32),
        ),
        in_specs=[hbm] * 13,
        out_specs=(vmem, vmem, vmem),
        scratch_shapes=[
            pltpu.VMEM(volume, F32),
            pltpu.VMEM(volume, F32),
            pltpu.VMEM((9, ELEMS), F32),
            pltpu.VMEM((3, 4, ELEMS), F32),
            pltpu.VMEM((4, ELEMS), F32),
            pltpu.VMEM((1, ELEMS), F32),
            pltpu.VMEM((1, ELEMS), jnp.int32),
            pltpu.VMEM((1, ELEMS), jnp.int32),
            pltpu.VMEM((4, ELEMS), jnp.int32),
            pltpu.VMEM((4, ELEMS), jnp.int32),
            pltpu.VMEM((3, NODES, NODES), F32),
            pltpu.VMEM((NODES, 60), F32),
            pltpu.VMEM((4, 96, 96), BF16),
            pltpu.VMEM((4, 96, ELEMS), BF16),
            pltpu.VMEM((64, FACES), F32),
            pltpu.VMEM((128, FACES), BF16),
            pltpu.VMEM((2 * half, FACES), BF16),
            pltpu.VMEM((FACES, FACES), BF16),
            pltpu.VMEM(volume, F32),
            pltpu.VMEM((48, 64), F32),
            pltpu.VMEM((144, 48), F32),
            pltpu.VMEM((144, 96), BF16),
            pltpu.VMEM((8, 16, 128), F32),
            pltpu.VMEM((ns - 9, 4, 128), F32),
            pltpu.VMEM((2, 16, 128), F32),
            pltpu.VMEM((8, 16, 128), F32),
            pltpu.VMEM((ns - 9, 4, 128), F32),
            pltpu.VMEM((2, 16, 128), F32),
            pltpu.VMEM((NEAR_ROWS + 32, 128), F32),
            pltpu.VMEM((half - NEAR_ROWS - 32, 128), F32),
            pltpu.VMEM((1, 128), F32),
            pltpu.VMEM((2 * ns, 1, 128), F32),
            pltpu.VMEM((1, 128), F32),
            pltpu.VMEM((ng // 2, 1, 128), F32),
            pltpu.VMEM((1, 128), F32),
            pltpu.VMEM((1, 128), F32),
            pltpu.VMEM((ng // 2, 2 * ns, 1, 128), F32),
            dma((19,)),
            dma((2,)),
            dma((2,)),
            dma((2,)),
            dma((2,)),
            dma((2,)),
            dma((2,)),
            dma((1,)),
            dma((2,)),
            dma((1,)),
            dma((ng // 2,)),
        ],
        compiler_params=pltpu.CompilerParams(collective_id=0, has_side_effects=True, vmem_limit_bytes=24 << 20),
        name="section",
    )
    write = pl.pallas_call(
        finish,
        out_shape=(state, state, jax.ShapeDtypeStruct((1, 1), F32)),
        in_specs=[vmem] * 3,
        out_specs=(hbm, hbm, hbm),
        scratch_shapes=[pltpu.VMEM((1, 1), F32), dma((9,))],
        compiler_params=pltpu.CompilerParams(vmem_limit_bytes=8 << 20),
        name="finish",
    )

    def keep(x):
        return pltpu.with_memory_space_constraint(x, pltpu.HBM)

    def local(
        fields,
        section_store,
        metric_terms,
        normals,
        face_scale,
        damping,
        absorb_mask,
        refine_level,
        face_source,
        orientation,
        derivative,
        lift_matrix,
    ):
        fields_new, store_new, energy_new = call(*map(keep,(
            jnp.transpose(fields, (1, 0, 2)),
            jnp.transpose(section_store, (1, 0, 2)),
            metric_terms,
            jnp.transpose(normals, (1, 0, 2)),
            face_scale,
            damping.reshape(1, ELEMS),
            absorb_mask.reshape(1, ELEMS),
            refine_level.reshape(1, ELEMS),
            face_source,
            orientation,
            derivative,
            lift_matrix,
            jnp.asarray(pick_table(), BF16),
        )))
        fields_next, store_next, energy = write(fields_new, store_new, energy_new)
        return (
            jnp.transpose(fields_next, (1, 0, 2)),
            jnp.transpose(store_next, (1, 0, 2)),
            energy.reshape(()),
        )

    in_specs = (
        P(None, None, both),
        P(None, None, both),
        P(None, both),
        P(None, None, both),
        P(None, both),
        P(both),
        P(both),
        P(both),
        P(None, both),
        P(None, both),
        P(),
        P(),
    )
    out_specs = (P(None, None, both), P(None, None, both), P())
    return jax.shard_map(local, mesh=mesh, in_specs=in_specs, out_specs=out_specs, check_vma=False)
```

```python
import functools

import jax
import jax.numpy as jnp
import numpy as np
from jax import lax
from jax.experimental import pallas as pl
from jax.experimental.pallas import tpu as pltpu
from jax.sharding import PartitionSpec as P

MESH = pl.DeviceIdType.MESH
F32 = jnp.float32
BF16 = jnp.bfloat16

RUNGE_CARRY = -567301805773.0 / 1357537059087.0
RUNGE_ADVANCE = 5161836677717.0 / 13612068292357.0
TIME_STEP = 0.02

NODES = 35
ELEMS = 256
FACES = 4 * ELEMS
NEAR = 4
FAR_Y = 2
NEAR_ROWS = 8 * 16


def pick_table():
    volume = [(a, b, c, 4 - a - b - c) for a in range(5) for b in range(5 - a) for c in range(5 - a - b)]
    triples = [(a, b, 4 - a - b) for a in range(5) for b in range(5 - a)]
    orders = [(0, 1, 2), (1, 2, 0), (2, 0, 1), (0, 2, 1), (2, 1, 0), (1, 0, 2)]
    inverse = [0, 2, 1, 3, 4, 5]
    table = np.zeros((4, 6, 16, 2, 48), np.float32)
    for facet in range(4):
        others = [corner for corner in range(4) if corner != facet]
        for option in range(6):
            order = orders[inverse[option]]
            for node in range(15):
                triple = triples[node]
                turned = tuple(triple[q] for q in order)
                corners = [0, 0, 0, 0]
                for place in range(3):
                    corners[others[place]] = turned[place]
                table[facet, option, node, :, volume.index(tuple(corners))] = 1.0
    return table.reshape(4, 96, 96)


def split(value):
    high = value.astype(BF16)
    low = (value - high.astype(F32)).astype(BF16)
    return high, low


def kernel(
    ng,
    ns,
    half,
    fields_hbm,
    store_hbm,
    metric_hbm,
    normals_hbm,
    scale_hbm,
    damping_hbm,
    mask_hbm,
    level_hbm,
    source_hbm,
    orient_hbm,
    deriv_hbm,
    lift_hbm,
    picks_hbm,
    fields_new,
    store_new,
    energy_new,
    fields,
    store,
    metric,
    normals,
    scale,
    damping,
    mask,
    level,
    source,
    orient,
    deriv,
    lift,
    picks,
    stacked,
    inner,
    turned,
    place,
    local,
    base,
    lifts,
    deriv_pad,
    deriv_cat,
    near_box,
    far_box,
    grp_box,
    near_in,
    far_in,
    grp_in,
    near_stage,
    far_stage,
    row_own,
    row_sub,
    sum_own,
    row_grp,
    total_own,
    total_in,
    row_first,
    load_sem,
    near_sems,
    far_sems,
    grp_send,
    grp_recv,
    sub_sems,
    top_sems,
    up_sems,
    down_sems,
    first_send,
    first_recv,
):
    g = lax.axis_index("grp")
    s = lax.axis_index("sub")
    grp_at = NEAR_ROWS
    far_at = NEAR_ROWS + 32
    rows = far_at + 4 * (ns - 9)

    def load(at, src, dst):
        return pltpu.make_async_copy(src, dst, load_sem.at[at])

    load_source = load(0, source_hbm, source)
    load_orient = load(1, orient_hbm, orient)
    load_fields = [load(2 + c, fields_hbm.at[:, c, :], fields.at[c]) for c in range(4)]
    load_picks = load(6, picks_hbm, picks)
    load_store = [load(7 + c, store_hbm.at[:, c, :], store.at[c]) for c in range(4)]
    load_rest = [
        load(11, metric_hbm, metric),
        load(12, normals_hbm, normals),
        load(13, scale_hbm, scale),
        load(14, damping_hbm, damping),
        load(15, mask_hbm, mask),
        load(16, level_hbm, level),
        load(17, deriv_hbm, deriv),
        load(18, lift_hbm, lift),
    ]
    def peer(k):
        other = s + k
        return jnp.where(other >= ns, other - ns, other)

    def peer_grp(k):
        other = g + k
        return jnp.where(other >= ng, other - ng, other)

    grp_in[...] = jnp.zeros_like(grp_in)

    order = sorted(range(1, ns), key=lambda k: -min(k, ns - k))

    barrier = pltpu.get_barrier_semaphore()
    for k in order:
        pl.semaphore_signal(barrier, inc=1, device_id=(g, peer(k)), device_id_type=MESH)
    core = g % 2

    def greet_grp(ks):
        for k in ks:
            pl.semaphore_signal(barrier, inc=1, device_id=(peer_grp(k), s), device_id_type=MESH)

    @pl.when((core == 1) | (s == 0))
    def _():
        greet_grp(sorted(range(2, ng, 2), key=lambda k: -min(k, ng - k)))

    @pl.when(s == 0)
    def _():
        greet_grp(range(3, ng - 1, 2))

    greet_grp((1, ng - 1))
    expected = ns + 1 + jnp.where((core == 1) | (s == 0), ng // 2 - 1, 0) + jnp.where(s == 0, ng // 2 - 2, 0)

    for copy in [load_source, load_orient, *load_fields, load_picks, *load_rest, *load_store]:
        copy.start()

    load_source.wait()
    codes = jnp.concatenate([source[f : f + 1, :] for f in range(4)], axis=1)
    slot = codes - FACES
    block = slot >> 5
    rank = slot & 31
    delta = block - s
    delta = jnp.where(delta < 0, delta + ns, delta)
    in_sub = block < ns
    after = in_sub & (delta <= NEAR)
    before = in_sub & (delta >= ns - NEAR)
    apart = in_sub & (delta > NEAR) & (delta < ns - NEAR)
    box = jnp.where(after, (delta - 1) * 16, jnp.where(before, (delta - ns + 8) * 16, grp_at + (block - ns) * 16))
    row = jnp.where(apart, far_at + (delta - NEAR - 1) * 4 + (rank & 3), box + (rank & 15))
    row = row + half * jnp.where(apart, (rank >> 2) & 1, rank >> 4)
    row = jnp.where(codes >= FACES, row, -1)

    def build_place(i, carry):
        at = lax.broadcasted_iota(jnp.int32, (32, FACES), 0) + i * 32
        place[pl.ds(i * 32, 32), :] = jnp.where(at == row, 1.0, 0.0).astype(BF16)
        return carry

    lax.fori_loop(0, 2 * half // 32, build_place, 0)

    stacked[...] = jnp.zeros_like(stacked)
    load_orient.wait()
    load_picks.wait()
    for c in range(4):
        load_fields[c].wait()
        high, low = split(fields[c])
        stacked[c, 0:NODES, :] = high
        stacked[c, 48 : 48 + NODES, :] = low
    for f in range(4):
        option_of = orient[f : f + 1, :]
        at = slice(f * ELEMS, (f + 1) * ELEMS)
        for c in range(4):
            found = jnp.dot(picks[f], stacked[c], preferred_element_type=F32)
            inner[c * 16 : (c + 1) * 16, at] = found[0:16]
            chosen = found[0:16]
            for option in range(1, 6):
                chosen = jnp.where(option_of == option, found[option * 16 : (option + 1) * 16], chosen)
            high, low = split(chosen)
            turned[c * 16 : (c + 1) * 16, at] = high
            turned[64 + c * 16 : 64 + (c + 1) * 16, at] = low

    across = (((1,), (1,)), ((), ()))
    left = lax.dot_general(place[:half, :], turned[...], across, preferred_element_type=F32)
    right = lax.dot_general(place[half:, :], turned[...], across, preferred_element_type=F32)
    left = left + pltpu.roll(left, 64, 1)
    right = right + pltpu.roll(right, 64, 1)
    lane = lax.broadcasted_iota(jnp.int32, (half, 128), 1)
    out = jnp.where(lane < 64, left, right)
    near_box[...] = out[:grp_at].reshape(8, 16, 128)
    for b in range(ns - 9):
        far_box[b] = out[far_at + 4 * b : far_at + 4 * b + 4]
    grp_box[...] = out[grp_at:far_at].reshape(2, 16, 128)

    pl.semaphore_wait(barrier, expected)

    def near_at(k):
        return k - 1 if k <= NEAR else k - ns + 8

    def sub_copy(k):
        if NEAR < k < ns - NEAR:
            src, dst, sems = far_box.at[k - NEAR - 1], far_in.at[ns - k - NEAR - 1], far_sems
        else:
            src, dst, sems = near_box.at[near_at(k)], near_in.at[near_at(ns - k)], near_sems
        return pltpu.make_async_remote_copy(
            src_ref=src,
            dst_ref=dst,
            send_sem=sems.at[0],
            recv_sem=sems.at[1],
            device_id=(g, peer(k)),
            device_id_type=MESH,
        )

    def grp_copy(up):
        return pltpu.make_async_remote_copy(
            src_ref=grp_box.at[up],
            dst_ref=grp_in.at[1 - up],
            send_sem=grp_send.at[up],
            recv_sem=grp_recv.at[1 - up],
            device_id=(g + 2 * up - 1, s),
            device_id_type=MESH,
        )

    for k in order:
        sub_copy(k).start()

    @pl.when(g < ng - 1)
    def _():
        grp_copy(1).start()

    @pl.when(g > 0)
    def _():
        grp_copy(0).start()

    for copy in [*load_rest, *load_store]:
        copy.wait()
    growth = jnp.exp2(level[...].astype(F32))
    absorb = damping[...] * mask[...].astype(F32)

    def build_local(i, carry):
        at = lax.broadcasted_iota(jnp.int32, (32, FACES), 0) + i * 32
        local[pl.ds(i * 32, 32), :] = jnp.where(at == codes, 1.0, 0.0).astype(BF16)
        return carry

    lax.fori_loop(0, FACES // 32, build_local, 0)
    outer_own = jnp.dot(turned[...], local[...], preferred_element_type=F32)

    lifts[...] = jnp.zeros_like(lifts)
    for f in range(4):
        lifts[0:NODES, f * 16 : f * 16 + 15] = lift[:, f * 15 : (f + 1) * 15]
    lift_high, lift_low = split(lifts[...])
    lift_cat = jnp.concatenate([lift_high, lift_high, lift_low], axis=1)

    deriv_pad[...] = jnp.zeros_like(deriv_pad)
    for d in range(3):
        deriv_pad[48 * d : 48 * d + NODES, 0:NODES] = deriv[d]
    deriv_high, deriv_low = split(deriv_pad[...])
    deriv_cat[:, 0:48] = deriv_high
    deriv_cat[:, 48:96] = deriv_high
    found = [
        jnp.dot(deriv_cat[...], stacked[c], preferred_element_type=F32)
        + jnp.dot(deriv_low, stacked[c, 0:48, :], preferred_element_type=F32)
        for c in range(4)
    ]
    slopes = [[found[c][48 * d : 48 * d + NODES] for c in range(4)] for d in range(3)]

    def physical(x, c):
        total = metric[3 * x : 3 * x + 1, :] * slopes[0][c]
        for y in range(1, 3):
            total = total + metric[3 * x + y : 3 * x + y + 1, :] * slopes[y][c]
        return growth * total

    volume = [-(physical(0, 1) + physical(1, 2) + physical(2, 3))]
    volume += [-physical(x, 0) for x in range(3)]
    for c in range(4):
        base[c] = RUNGE_CARRY * store[c] + TIME_STEP * (volume[c] - absorb * fields[c])

    known = []
    norms = []
    shares = []
    for f in range(4):
        at = slice(f * ELEMS, (f + 1) * ELEMS)
        wall = source[f : f + 1, :] < 0
        norm = [normals[x, f : f + 1, :] for x in range(3)]
        press_in = inner[0:16, at]
        veloc_in = [inner[(1 + x) * 16 : (2 + x) * 16, at] for x in range(3)]
        along = norm[0] * veloc_in[0] + norm[1] * veloc_in[1] + norm[2] * veloc_in[2]
        square = norm[0] * norm[0] + norm[1] * norm[1] + norm[2] * norm[2]
        weight = 0.5 * scale[f : f + 1, :] * growth
        known.append(weight * jnp.where(wall, 2.0 * square * along, along - press_in))
        share = jnp.where(wall, 0.0, weight)
        norms.append(norm)
        shares.append([share] + [-share * norm[x] for x in range(3)])

    def weighed(part, f):
        at = slice(f * ELEMS, (f + 1) * ELEMS)
        total = 0.0
        for c in range(4):
            outer = part[c * 16 : (c + 1) * 16, at] + part[64 + c * 16 : 64 + (c + 1) * 16, at]
            total = total + shares[f][c] * outer
        return total

    def arrival(ref, sems):
        return pltpu.make_async_copy(ref, ref, sems.at[1])

    def picked(stage, at):
        came = stage[...].T
        high, low = split(came)
        deep = stage.shape[0]
        left = jnp.concatenate([high[0:64], low[0:64]], axis=0)
        right = jnp.concatenate([high[64:128], low[64:128]], axis=0)
        return jnp.dot(left, place[at : at + deep, :], preferred_element_type=F32) + jnp.dot(
            right, place[half + at : half + at + deep, :], preferred_element_type=F32
        )

    far_stage[...] = jnp.zeros_like(far_stage)
    arrival(near_in, near_sems).wait()

    @pl.when(g > 0)
    def _():
        pltpu.make_async_copy(grp_in.at[0], grp_in.at[0], grp_recv.at[0]).wait()

    @pl.when(g < ng - 1)
    def _():
        pltpu.make_async_copy(grp_in.at[1], grp_in.at[1], grp_recv.at[1]).wait()

    near_stage[0:grp_at, :] = near_in[...].reshape(grp_at, 128)
    near_stage[grp_at:far_at, :] = grp_in[...].reshape(32, 128)
    outer_near = outer_own + picked(near_stage, 0)

    known = [known[f] + weighed(outer_near, f) for f in range(4)]

    arrival(far_in, far_sems).wait()
    for b in range(ns - 9):
        far_stage[4 * b : 4 * b + 4, :] = far_in[b]
    arrived = picked(far_stage, far_at)
    flux = [[None] * 4 for _ in range(4)]
    for f in range(4):
        flux[0][f] = known[f] + weighed(arrived, f)
        for x in range(3):
            flux[1 + x][f] = -norms[f][x] * flux[0][f]

    energy = jnp.zeros((1, ELEMS), F32)
    for c in range(4):
        high, low = split(jnp.concatenate(flux[c], axis=0))
        lifted = jnp.dot(lift_cat, jnp.concatenate([high, low, high], axis=0), preferred_element_type=F32)
        store_next = base[c] + TIME_STEP * lifted[0:NODES]
        fields_next = fields[c] + RUNGE_ADVANCE * store_next
        store_new[c] = store_next
        fields_new[c] = fields_next
        energy = energy + jnp.sum(fields_next * fields_next, axis=0, keepdims=True)
    energy = absorb * energy
    row_own[...] = energy[:, 0:128] + energy[:, 128:256]

    level_y = g // 2
    count_y = ng // 2
    lead = 2 * level_y + 1

    def sub_row(k, sems):
        return pltpu.make_async_remote_copy(
            src_ref=row_own,
            dst_ref=row_sub.at[2 * s + core],
            send_sem=sems.at[0],
            recv_sem=sub_sems.at[1],
            device_id=(lead, peer(k)),
            device_id_type=MESH,
        )

    many = row_sub.at[0 : 2 * ns - 1]
    rest = row_grp.at[0 : count_y - 1]

    def top_row(k):
        other = level_y + k
        return pltpu.make_async_remote_copy(
            src_ref=sum_own,
            dst_ref=row_grp.at[level_y],
            send_sem=top_sems.at[0],
            recv_sem=top_sems.at[1],
            device_id=(2 * jnp.where(other >= count_y, other - count_y, other) + 1, s),
            device_id_type=MESH,
        )

    def down_row():
        return pltpu.make_async_remote_copy(
            src_ref=total_own,
            dst_ref=total_in,
            send_sem=down_sems.at[0],
            recv_sem=down_sems.at[1],
            device_id=(2 * level_y, s),
            device_id_type=MESH,
        )

    first = (g == 1) & (s == 0)
    far_y = (level_y >= FAR_Y) & (level_y <= count_y - FAR_Y)

    def first_row():
        return pltpu.make_async_remote_copy(
            src_ref=row_own,
            dst_ref=row_first.at[level_y, 2 * s + core],
            send_sem=first_send.at[0],
            recv_sem=first_recv.at[level_y],
            device_id=(1, 0),
            device_id_type=MESH,
        )

    @pl.when(far_y)
    def _():
        first_row().start()

    for k in order:
        sub_row(k, sub_sems).start()

    @pl.when(core == 0)
    def _():
        sub_row(0, up_sems).start()

    @pl.when(core == 1)
    def _():
        row_sub[2 * s + 1] = row_own[...]
        arrival(many, sub_sems).wait()
        sum_own[...] = jnp.sum(row_sub[...], axis=0)
        for k in sorted(range(1, count_y), key=lambda k: -min(k, count_y - k)):

            @pl.when(jnp.logical_not((s == 0) & far_y & (level_y + k == count_y)))
            def _(k=k):
                top_row(k).start()

        row_grp[level_y] = sum_own[...]

    def left_here(ref, sem):
        pltpu.make_async_copy(ref, ref, sem).wait()

    left_here(near_box, near_sems.at[0])
    left_here(far_box, far_sems.at[0])
    left_here(row_sub.at[0 : ns - 1], sub_sems.at[0])

    @pl.when(g < ng - 1)
    def _():
        grp_copy(1).wait_send()

    @pl.when(g > 0)
    def _():
        grp_copy(0).wait_send()

    @pl.when(far_y)
    def _():
        first_row().wait_send()

    @pl.when(first)
    def _():
        arrival(row_grp.at[0 : 2 * FAR_Y - 2], top_sems).wait()
        for y in sorted(range(FAR_Y, count_y - FAR_Y + 1), key=lambda y: min(y, count_y - y)):
            pltpu.make_async_copy(row_first.at[y], row_first.at[y], first_recv.at[y]).wait()
            row_grp[y] = jnp.sum(row_first[y], axis=0)

    @pl.when((core == 1) & jnp.logical_not(first))
    def _():
        arrival(rest, top_sems).wait()

    @pl.when(core == 1)
    def _():
        total = jnp.sum(jnp.sum(row_grp[...], axis=0), axis=1, keepdims=True)
        total_own[...] = jnp.broadcast_to(total * (1.0 / (ELEMS * NODES * ng * ns)), (1, 128))
        down_row().start()
        energy_new[...] = total_own[...]
        down_row().wait_send()

        @pl.when((s == 0) & far_y)
        def _():
            left_here(row_grp.at[0 : count_y - 2], top_sems.at[0])

        @pl.when(jnp.logical_not((s == 0) & far_y))
        def _():
            left_here(rest, top_sems.at[0])

    @pl.when(core == 0)
    def _():
        sub_row(0, up_sems).wait_send()
        down_row().wait_recv()
        energy_new[...] = total_in[...]


def finish(fields_new, store_new, energy_new, fields_out, store_out, energy_out, single, out_sem):
    single[...] = energy_new[:, 0:1]
    outs = [pltpu.make_async_copy(fields_new.at[c], fields_out.at[:, c, :], out_sem.at[c]) for c in range(4)]
    outs += [pltpu.make_async_copy(store_new.at[c], store_out.at[:, c, :], out_sem.at[4 + c]) for c in range(4)]
    outs += [pltpu.make_async_copy(single, energy_out, out_sem.at[8])]
    for copy in outs:
        copy.start()
    for copy in outs:
        copy.wait()


def solution(mesh):
    ng, ns = mesh.shape["grp"], mesh.shape["sub"]
    rows = NEAR_ROWS + 4 * (ns - 9) + 32
    half = -(-rows // 16) * 16
    both = ("grp", "sub")
    hbm = pl.BlockSpec(memory_space=pltpu.HBM)
    vmem = pl.BlockSpec(memory_space=pltpu.VMEM)
    dma = pltpu.SemaphoreType.DMA
    volume = (4, NODES, ELEMS)
    state = jax.ShapeDtypeStruct((NODES, 4, ELEMS), F32)

    call = pl.pallas_call(
        functools.partial(kernel, ng, ns, half),
        out_shape=(
            jax.ShapeDtypeStruct(volume, F32),
            jax.ShapeDtypeStruct(volume, F32),
            jax.ShapeDtypeStruct((1, 128), F32),
        ),
        in_specs=[hbm] * 13,
        out_specs=(vmem, vmem, vmem),
        scratch_shapes=[
            pltpu.VMEM(volume, F32),
            pltpu.VMEM(volume, F32),
            pltpu.VMEM((9, ELEMS), F32),
            pltpu.VMEM((3, 4, ELEMS), F32),
            pltpu.VMEM((4, ELEMS), F32),
            pltpu.VMEM((1, ELEMS), F32),
            pltpu.VMEM((1, ELEMS), jnp.int32),
            pltpu.VMEM((1, ELEMS), jnp.int32),
            pltpu.VMEM((4, ELEMS), jnp.int32),
            pltpu.VMEM((4, ELEMS), jnp.int32),
            pltpu.VMEM((3, NODES, NODES), F32),
            pltpu.VMEM((NODES, 60), F32),
            pltpu.VMEM((4, 96, 96), BF16),
            pltpu.VMEM((4, 96, ELEMS), BF16),
            pltpu.VMEM((64, FACES), F32),
            pltpu.VMEM((128, FACES), BF16),
            pltpu.VMEM((2 * half, FACES), BF16),
            pltpu.VMEM((FACES, FACES), BF16),
            pltpu.VMEM(volume, F32),
            pltpu.VMEM((48, 64), F32),
            pltpu.VMEM((144, 48), F32),
            pltpu.VMEM((144, 96), BF16),
            pltpu.VMEM((8, 16, 128), F32),
            pltpu.VMEM((ns - 9, 4, 128), F32),
            pltpu.VMEM((2, 16, 128), F32),
            pltpu.VMEM((8, 16, 128), F32),
            pltpu.VMEM((ns - 9, 4, 128), F32),
            pltpu.VMEM((2, 16, 128), F32),
            pltpu.VMEM((NEAR_ROWS + 32, 128), F32),
            pltpu.VMEM((half - NEAR_ROWS - 32, 128), F32),
            pltpu.VMEM((1, 128), F32),
            pltpu.VMEM((2 * ns, 1, 128), F32),
            pltpu.VMEM((1, 128), F32),
            pltpu.VMEM((ng // 2, 1, 128), F32),
            pltpu.VMEM((1, 128), F32),
            pltpu.VMEM((1, 128), F32),
            pltpu.VMEM((ng // 2, 2 * ns, 1, 128), F32),
            dma((19,)),
            dma((2,)),
            dma((2,)),
            dma((2,)),
            dma((2,)),
            dma((2,)),
            dma((2,)),
            dma((1,)),
            dma((2,)),
            dma((1,)),
            dma((ng // 2,)),
        ],
        compiler_params=pltpu.CompilerParams(collective_id=0, has_side_effects=True, vmem_limit_bytes=24 << 20),
        name="section",
    )
    write = pl.pallas_call(
        finish,
        out_shape=(state, state, jax.ShapeDtypeStruct((1, 1), F32)),
        in_specs=[vmem] * 3,
        out_specs=(hbm, hbm, hbm),
        scratch_shapes=[pltpu.VMEM((1, 1), F32), dma((9,))],
        compiler_params=pltpu.CompilerParams(vmem_limit_bytes=8 << 20),
        name="finish",
    )

    def keep(x):
        return pltpu.with_memory_space_constraint(x, pltpu.HBM)

    def local(
        fields,
        section_store,
        metric_terms,
        normals,
        face_scale,
        damping,
        absorb_mask,
        refine_level,
        face_source,
        orientation,
        derivative,
        lift_matrix,
    ):
        fields_new, store_new, energy_new = call(*map(keep,(
            jnp.transpose(fields, (1, 0, 2)),
            jnp.transpose(section_store, (1, 0, 2)),
            metric_terms,
            jnp.transpose(normals, (1, 0, 2)),
            face_scale,
            damping.reshape(1, ELEMS),
            absorb_mask.reshape(1, ELEMS),
            refine_level.reshape(1, ELEMS),
            face_source,
            orientation,
            derivative,
            lift_matrix,
            jnp.asarray(pick_table(), BF16),
        )))
        fields_next, store_next, energy = write(fields_new, store_new, energy_new)
        return (
            jnp.transpose(fields_next, (1, 0, 2)),
            jnp.transpose(store_next, (1, 0, 2)),
            energy.reshape(()),
        )

    in_specs = (
        P(None, None, both),
        P(None, None, both),
        P(None, both),
        P(None, None, both),
        P(None, both),
        P(both),
        P(both),
        P(both),
        P(None, both),
        P(None, both),
        P(),
        P(),
    )
    out_specs = (P(None, None, both), P(None, None, both), P())
    return jax.shard_map(local, mesh=mesh, in_specs=in_specs, out_specs=out_specs, check_vma=False)
```
